32 devices in a mesh: heads: 2 (over x), seq: 16 (over z, y, core).
Axes of the slice: x: 2, y: 2, z: 4, core: 2. Of those that a mesh axis runs over, the one named last changes fastest.
Arguments:
- query_nope: bfloat16 [1, 4, 128, 128], P(None, None, 'heads'), may hold values from -6 to 6
- query_rope: bfloat16 [1, 4, 128, 64], P(None, None, 'heads'), may hold values from -8 to 8
- latent_cache: bfloat16 [1, 8192, 512], P(None, 'seq'), may hold values from -6 to 6
- rope_keys: bfloat16 [1, 64, 8192], P(None, None, 'seq'), may hold values from -8 to 8
- lengths: int32 [1], replicated, may hold values from 2 to 8189, as said below
- key_quant: bfloat16 [128, 512, 128], P('heads', 'seq'), may hold values from -127 to 127, as said below
- key_scale: float32 [128, 4], P('heads'), may hold values from 0.0006 to 0.0024
- value_quant: bfloat16 [128, 512, 128], P('heads', 'seq'), may hold values from -127 to 127, as said below
- value_scale: float32 [128, 4], P('heads'), may hold values from 0.0003 to 0.0012
- out_weight: bfloat16 [16384, 7168], P('heads', 'seq'), may hold values from -0.375 to 0.375
Outputs:
- attn_out: bfloat16 [1, 4, 7168], P(None, None, 'seq')
The draws below stay inside these ranges and needn't reach their ends.
Inputs may be any that keep to these rules, and one draw needn't show every extreme that they name: `key_quant`: whole numbers. `value_quant`: whole numbers. `lengths`: one sequence has the largest allowed length, so that its last draft token sees all 8192 positions.
All inputs are finite; a program needn't handle non-finite values.
Results may differ from the reference program's by a relative error of at most 0.019.
Values may be sent and summed in bfloat16 or wider, within the bound.
A program may use at most 64 MiB of HBM per device.

```python
import math
import jax
import jax.numpy as jnp
from jax import lax

H = 128
C = 512
R = 64
NOPE = 128
V = 128
D = 7168
QB = 128
B = 1
QT = 4
CTX_DEV = 512
CONTEXT = 8192
N_SEQ = 16


def rope_pair(key):
    base_key = jax.random.fold_in(key, 911)
    key_query, key_cache = jax.random.split(base_key, 2)
    queries = jnp.clip(jax.random.normal(key_query, (B, QT, H, R), jnp.float32), -8.0, 8.0)
    keys_out = jnp.clip(jax.random.normal(key_cache, (B, R, CONTEXT), jnp.float32), -8.0, 8.0)
    return (queries, keys_out)


def draw_query_rope(key, part):
    return rope_pair(key)[0].astype(jnp.bfloat16)


def draw_rope_keys(key, part):
    return rope_pair(key)[1].astype(jnp.bfloat16)


def draw_lengths(key, part):
    values = jax.random.randint(jax.random.fold_in(key, 3), (B,), 2, CONTEXT - QT + 2)
    longest = jax.random.randint(jax.random.fold_in(key, 5), (), 0, B)
    return jnp.where(jnp.arange(B) == longest, CONTEXT - QT + 1, values).astype(jnp.int32)


def draw_key_quant(key, part):
    values = jax.random.randint(jax.random.fold_in(key, 7), (H, C, NOPE), -127, 128)
    return values.astype(jnp.float32).astype(jnp.bfloat16)


def draw_value_quant(key, part):
    values = jax.random.randint(jax.random.fold_in(key, 11), (H, C, V), -127, 128)
    return values.astype(jnp.float32).astype(jnp.bfloat16)


def steps_of(own_key, dims, cuts, least, high):
    factor_of = 1.0
    for dim, shards_of in cuts:
        draws = jax.random.uniform(jax.random.fold_in(jax.random.fold_in(own_key, 6), dim), (shards_of,), jnp.float32, least / len(cuts), high / len(cuts))
        factor_of = factor_of * jnp.repeat(jnp.exp(draws), dims[dim] // shards_of).reshape((-1,) + (1,) * (len(dims) - 1 - dim))
    return factor_of


def normal_values(own_key, shape, spread, limit, cuts=(), held_as=jnp.bfloat16):
    drawn = spread * jax.random.normal(own_key, shape, jnp.float32)
    if cuts:
        drawn = drawn * steps_of(own_key, shape, cuts, -0.22, 0.18)
    return jnp.clip(drawn, -limit, limit).astype(held_as)


def setup_inputs(seed: int = 0) -> dict:
    seeds = jax.random.split(jax.random.key(seed), 11)
    return {
        "query_nope": normal_values(seeds[0], (B, QT, H, NOPE), 1.0, 6.0, ((2, 2),)),
        "query_rope": draw_query_rope(jax.random.fold_in(seeds[10], 71), 0),
        "latent_cache": normal_values(seeds[2], (B, CONTEXT, C), 1.0, 6.0, ((1, 16),)),
        "rope_keys": draw_rope_keys(jax.random.fold_in(seeds[10], 71), 0),
        "lengths": draw_lengths(jax.random.fold_in(seeds[10], 71), 0),
        "key_quant": draw_key_quant(jax.random.fold_in(seeds[10], 71), 0),
        "key_scale": jnp.clip(jnp.exp(math.log(0.0024) - 1.3862944 * jax.random.uniform(seeds[6], (H, C // QB), jnp.float32) ** steps_of(seeds[6], (H, C // QB), ((0, 2),), -0.2, 0.2)), 0.0006, 0.0024),
        "value_quant": draw_value_quant(jax.random.fold_in(seeds[10], 71), 0),
        "value_scale": jnp.clip(jnp.exp(math.log(0.0012) - 1.3862944 * jax.random.uniform(seeds[8], (H, C // QB), jnp.float32) ** steps_of(seeds[8], (H, C // QB), ((0, 2),), -0.2, 0.2)), 0.0003, 0.0012),
        "out_weight": normal_values(seeds[9], (H * V, D), (H * V // 64) ** -0.5, 0.375, ((0, 2), (1, 16))),
    }


neg_large = -1.0e30


def expand_scales(block_scale, offset, count):
    row_ids = (offset + jnp.arange(count, dtype=jnp.int32)) // QB
    onehot = (row_ids[:, None] == jnp.arange(block_scale.shape[1], dtype=jnp.int32)[None, :]).astype(block_scale.dtype)
    return jnp.sum(block_scale[:, None, :] * onehot[None, :, :], axis=2)


def dequantize(quantized, block_scale, offset):
    factors = expand_scales(block_scale, offset, quantized.shape[1])
    return (quantized.astype(jnp.float32) * factors[:, :, None]).astype(jnp.bfloat16)


def combine(earlier, later):
    max_a, sum_a, out_a = earlier
    max_b, sum_b, out_b = later
    joint = jnp.maximum(max_a, max_b)
    fac_a = jnp.exp(max_a - joint)
    fac_b = jnp.exp(max_b - joint)
    return joint, sum_a * fac_a + sum_b * fac_b, out_a * fac_a[..., None] + out_b * fac_b[..., None]


def reference(query_nope, query_rope, latent_cache, rope_keys, lengths, key_quant, key_scale, value_quant, value_scale, out_weight):
    key_weight = dequantize(key_quant, key_scale, 0)
    value_weight = dequantize(value_quant, value_scale, 0)
    query_latent = jnp.einsum("btkn,kcn->btkc", query_nope.astype(jnp.float32), key_weight.astype(jnp.float32)).astype(jnp.bfloat16)
    factor = (NOPE + R) ** -0.5
    horizon = lengths[:, None] + jnp.arange(QT, dtype=jnp.int32)[None, :]
    lat_f = query_latent.astype(jnp.float32)
    rope_f = query_rope.astype(jnp.float32)

    def one_block(state_acc, block_idx):
        offset = (block_idx * CTX_DEV).astype(jnp.int32)
        cache_blk = lax.dynamic_slice_in_dim(latent_cache, offset, CTX_DEV, 1).astype(jnp.float32)
        rope_blk = lax.dynamic_slice_in_dim(rope_keys, offset, CTX_DEV, 2).astype(jnp.float32)
        scores = (jnp.einsum("btkc,bsc->btks", lat_f, cache_blk) + jnp.einsum("btkr,brs->btks", rope_f, rope_blk)) * factor
        position = offset + jnp.arange(CTX_DEV, dtype=jnp.int32)
        visible = (position[None, None, :] < horizon[:, :, None])[:, :, None, :]
        block_max = jnp.max(jnp.where(visible, scores, neg_large), axis=3)
        probs = jnp.where(visible, jnp.exp(scores - block_max[..., None]), 0.0)
        block_sum = jnp.sum(probs, axis=3)
        probs_bf = probs.astype(jnp.bfloat16)
        block_out = jnp.einsum("btks,bsc->btkc", probs_bf.astype(jnp.float32), cache_blk)
        return combine(state_acc, (block_max, block_sum, block_out)), None

    start_state = (jnp.full((B, QT, H), neg_large, jnp.float32), jnp.zeros((B, QT, H), jnp.float32), jnp.zeros((B, QT, H, C), jnp.float32))
    final_state, _ = lax.scan(one_block, start_state, jnp.arange(N_SEQ, dtype=jnp.int32))
    out_latent = (final_state[2] / final_state[1][..., None]).astype(jnp.bfloat16)
    head_output = jnp.einsum("btkc,kcv->btkv", out_latent.astype(jnp.float32), value_weight.astype(jnp.float32)).astype(jnp.bfloat16)
    summed = jnp.dot(head_output.reshape(B * QT, H * V), out_weight, preferred_element_type=jnp.float32)
    return summed.astype(jnp.bfloat16).reshape(B, QT, D)
```

```python
import functools

import jax
import jax.numpy as jnp
from jax import lax
from jax.experimental import pallas as pl
from jax.experimental.pallas import tpu as pltpu
from jax.sharding import PartitionSpec as P

QB = 128
MESH = pl.DeviceIdType.MESH
neg_large = -1e30
F32 = jnp.float32
BF16 = jnp.bfloat16


def scale_row(scale_ref, block, rows, heads):
    scales = scale_ref[...]
    line = jnp.sum(
        jnp.where(lax.broadcasted_iota(jnp.int32, scales.shape, 0) == block, scales, 0.0),
        axis=0,
        keepdims=True,
    )
    square = (heads, heads)
    diagonal = lax.broadcasted_iota(jnp.int32, square, 0) == lax.broadcasted_iota(jnp.int32, square, 1)
    column = jnp.sum(jnp.where(diagonal, line, 0.0), axis=1, keepdims=True)
    lane_head = lax.broadcasted_iota(jnp.int32, (heads, rows), 1) % heads
    own_head = lax.broadcasted_iota(jnp.int32, (heads, rows), 0)
    return jnp.sum(jnp.where(lane_head == own_head, column, 0.0), axis=0, keepdims=True)


def kernel(
    n,
    groups,
    heads,
    drafts,
    q_hbm,
    qr_hbm,
    cache_hbm,
    rope_hbm,
    len_ref,
    kq_hbm,
    ks_ref,
    vq_hbm,
    vs_ref,
    w_hbm,
    out_ref,
    q,
    qr,
    cache,
    rope,
    kq,
    vq,
    w,
    cache_t,
    vq_t,
    base,
    lat_all,
    stats,
    out_send,
    out_recv,
    part_send,
    part_recv,
    share_all,
    flat,
    heads_out,
    final,
    in_sem,
    lat_send,
    lat_recv,
    pass_send,
    st_send,
    st_recv,
    o_send,
    o_recv,
    p_send,
    p_recv,
    s_send,
    s_recv,
    f_send,
    f_recv,
):
    me = lax.axis_index("seq")
    group = lax.axis_index("heads")
    rows = q.shape[0]
    cols = lat_all.shape[1]
    width = vq.shape[1]
    positions = cache.shape[0]
    factor = (q.shape[1] + qr.shape[1]) ** (-0.5)

    loads = []
    for i, (src, dst) in enumerate(
        ((kq_hbm, kq), (q_hbm, q), (qr_hbm, qr), (rope_hbm, rope), (cache_hbm, cache), (vq_hbm, vq), (w_hbm, w))
    ):
        copy = pltpu.make_async_copy(src, dst, in_sem.at[i])
        if dst is not w:
            copy.start()
        loads.append(copy)
    kq_load, q_load, qr_load, rope_load, cache_load, vq_load, w_load = loads

    barrier = pltpu.get_barrier_semaphore()

    def greet_seq(j, c):
        pl.semaphore_signal(barrier, inc=1, device_id=(group, lax.rem(me + j, n)), device_id_type=MESH)
        return c

    def greet_heads(j, c):
        pl.semaphore_signal(barrier, inc=1, device_id=(lax.rem(group + j, groups), me), device_id_type=MESH)
        return c

    lax.fori_loop(1, n, greet_seq, 0)
    lax.fori_loop(1, groups, greet_heads, 0)

    def spread(src_of, dst, send, recv):
        def make(j):
            peer = lax.rem(me + j, n)
            return pltpu.make_async_remote_copy(
                src_ref=src_of(peer),
                dst_ref=dst.at[me],
                send_sem=send.at[peer],
                recv_sem=recv.at[me],
                device_id=(group, peer),
                device_id_type=MESH,
            )

        def go(j, c):
            make(j).start()
            return c

        lax.fori_loop(1, n, go, 0)

    def arrive(src_of, dst, send, recv):
        def wait(j, c):
            peer = lax.rem(me + j, n)
            pltpu.make_async_remote_copy(
                src_ref=src_of(peer),
                dst_ref=dst.at[peer],
                send_sem=send.at[peer],
                recv_sem=recv.at[peer],
                device_id=(group, peer),
                device_id_type=MESH,
            ).wait_recv()
            return c

        lax.fori_loop(1, n, wait, 0)

    def drain(src_of, dst, send, recv):
        def wait(j, c):
            peer = lax.rem(me + j, n)
            pltpu.make_async_remote_copy(
                src_ref=src_of(peer),
                dst_ref=dst.at[me],
                send_sem=send.at[peer],
                recv_sem=recv.at[me],
                device_id=(group, peer),
                device_id_type=MESH,
            ).wait_send()
            return c

        lax.fori_loop(1, n, wait, 0)

    block = (me * cols) // QB
    lane_head = lax.broadcasted_iota(jnp.int32, (1, rows), 1) % heads
    key_row = scale_row(ks_ref, block, rows, heads)
    value_row = scale_row(vs_ref, block, rows, heads)

    kq_load.wait()
    q_load.wait()
    every = lax.dot_general(kq[...], q[...], (((1,), (1,)), ((), ())), preferred_element_type=F32)
    every = every.reshape(heads, cols, rows)
    own = lax.broadcasted_iota(jnp.int32, (heads, 1, rows), 0) == lane_head[None]
    piece = jnp.sum(jnp.where(own, every, 0.0), axis=0) * key_row
    lat_all[me] = piece.astype(BF16)

    pl.semaphore_wait(barrier, n - 1 + groups - 1)

    partner = me + 1 - 2 * lax.rem(me, 2)

    def lat_copy(slot, peer, send):
        return pltpu.make_async_remote_copy(
            src_ref=lat_all.at[slot],
            dst_ref=lat_all.at[slot],
            send_sem=send,
            recv_sem=lat_recv.at[slot],
            device_id=(group, peer),
            device_id_type=MESH,
        )

    def like(j):
        return lax.rem(me + 2 * j, n)

    def lat_go(j, c):
        lat_copy(me, like(j), lat_send.at[like(j)]).start()
        return c

    def lat_pass(j, c):
        lat_copy(like(j), partner, pass_send.at[like(j)]).wait_recv()
        lat_copy(like(j), partner, pass_send.at[like(j)]).start()
        return c

    def lat_rest(j, c):
        other = lax.rem(partner + 2 * j, n)
        lat_copy(other, partner, pass_send.at[other]).wait_recv()
        return c

    def lat_drain(j, c):
        lat_copy(me, like(j), lat_send.at[like(j)]).wait_send()
        lat_copy(like(j), partner, pass_send.at[like(j)]).wait_send()
        return c

    lax.fori_loop(1, n // 2, lat_go, 0)
    lat_copy(me, partner, lat_send.at[partner]).start()
    w_load.start()

    qr_load.wait()
    rope_load.wait()
    base[...] = lax.dot_general(
        rope[...].T, qr[...], (((1,), (1,)), ((), ())), preferred_element_type=F32
    )
    cache_load.wait()
    cache_t[...] = cache[...].T
    lax.fori_loop(1, n // 2, lat_pass, 0)
    position = me * positions + lax.broadcasted_iota(jnp.int32, (positions, rows), 0)
    horizon = len_ref[0] + lax.broadcasted_iota(jnp.int32, (positions, rows), 1) // heads
    visible = position < horizon

    lax.fori_loop(0, n // 2, lat_rest, 0)
    query_latent = lat_all[...].reshape(n * cols, rows)
    scores = (jnp.dot(cache[...], query_latent, preferred_element_type=F32) + base[...]) * factor
    block_max = jnp.max(jnp.where(visible, scores, neg_large), axis=0, keepdims=True)
    probs = jnp.where(visible, jnp.exp(scores - block_max), 0.0)
    block_sum = jnp.sum(probs, axis=0, keepdims=True)
    stats[me, 0:1, :] = block_max
    stats[me, 1:2, :] = block_sum
    st = (lambda peer: stats.at[me], stats, st_send, st_recv)
    spread(*st)
    block_out = jnp.dot(cache_t[...], probs.astype(BF16), preferred_element_type=F32)
    out_send[...] = block_out.astype(BF16).reshape(n, cols, rows)
    o = (lambda peer: out_send.at[peer], out_recv, o_send, o_recv)
    spread(*o)
    out_recv[me] = out_send[me]
    vq_load.wait()
    vq_t[...] = vq[...].T

    arrive(*st)
    all_max = stats[:, 0:1, :]
    top = jnp.max(all_max, axis=0, keepdims=True)
    weight = jnp.exp(all_max - top)
    total = jnp.sum(weight * stats[:, 1:2, :], axis=0)
    arrive(*o)
    merged = jnp.sum(out_recv[...].astype(F32) * weight, axis=0) / total
    latent = jnp.where(own, merged[None], 0.0).astype(BF16).reshape(heads * cols, rows)
    partial = jnp.dot(vq_t[...], latent, preferred_element_type=F32) * value_row
    step = width // n
    for d in range(n):
        part_send[d] = partial[d * step : (d + 1) * step].astype(part_send.dtype)
    p = (lambda peer: part_send.at[peer], part_recv, p_send, p_recv)
    spread(*p)
    part_recv[me] = part_send[me]
    arrive(*p)
    share_all[me] = jnp.sum(part_recv[...].astype(F32), axis=0).astype(BF16)
    s = (lambda peer: share_all.at[me], share_all, s_send, s_recv)
    spread(*s)
    arrive(*s)
    head_t = jnp.concatenate([share_all[d].astype(F32) for d in range(n)], axis=0)
    heads_out[...] = head_t.T.reshape(drafts, heads, width)
    for k in range(heads):
        flat[:, k * width : (k + 1) * width] = heads_out[:, k, :].astype(BF16)
    w_load.wait()
    final[group] = lax.dot_general(
        flat[...], w[...], (((1,), (1,)), ((), ())), preferred_element_type=F32
    )

    def pair(j, at):
        peer = lax.rem(group + j, groups)
        return pltpu.make_async_remote_copy(
            src_ref=final.at[group],
            dst_ref=final.at[group if at else peer],
            send_sem=f_send.at[peer],
            recv_sem=f_recv.at[group if at else peer],
            device_id=(peer, me),
            device_id_type=MESH,
        )

    for j in range(1, groups):
        pair(j, True).start()
    for j in range(1, groups):
        pair(j, False).wait_recv()
    out_ref[...] = jnp.sum(final[...], axis=0).astype(BF16)
    for each in (st, o, p, s):
        drain(*each)
    lax.fori_loop(1, n // 2, lat_drain, 0)
    lat_copy(me, partner, lat_send.at[partner]).wait_send()
    for j in range(1, groups):
        pair(j, True).wait_send()


def chip_peer(chip, chips, k):
    out = 0
    bit = 1
    while bit < chips:
        own = lax.rem(chip // bit, 2)
        out = out + bit * ((1 - own) if k & bit else own)
        bit *= 2
    return out


def pair_kernel(
    n,
    groups,
    heads,
    drafts,
    q_hbm,
    qr_hbm,
    cache_hbm,
    rope_hbm,
    len_ref,
    kq_hbm,
    ks_ref,
    vq_hbm,
    vs_ref,
    w_hbm,
    out_ref,
    q,
    qr,
    cache,
    rope,
    kq,
    vq,
    w,
    q_rows,
    qr_rows,
    cache_t,
    base,
    lat_send,
    lat_all,
    st_send,
    st_all,
    out_send,
    out_recv,
    part_send,
    part_recv,
    share_send,
    share_recv,
    fin_send,
    fin_recv,
    in_sem,
    swap_s,
    swap_r,
    lat_s,
    lat_ps,
    lat_r,
    st_s,
    st_r,
    o_s,
    o_r,
    p_s,
    p_r,
    s_s,
    s_r,
    f_s,
    f_r,
):
    me = lax.axis_index("seq")
    group = lax.axis_index("heads")
    core = lax.rem(me, 2)
    other = 1 - core
    chip = me // 2
    chips = n // 2
    half = heads // 2
    rows = half * drafts
    cols = lat_all.shape[1]
    wide = 2 * cols
    latent = cache.shape[2]
    positions = cache.shape[1]
    width = vq.shape[2]
    span = half * width
    share = rows // chips
    per = share // drafts
    factor = (q.shape[2] + qr.shape[2]) ** (-0.5)
    far_first = range(chips - 1, -1, -1)
    peers = [chip_peer(chip, chips, k) for k in range(chips)]
    partner = 2 * chip + other

    barrier = pltpu.get_barrier_semaphore()
    for k in far_first:
        for b in range(2):
            if k:
                pl.semaphore_signal(barrier, inc=1, device_id=(group, 2 * peers[k] + b), device_id_type=MESH)
    pl.semaphore_signal(barrier, inc=1, device_id=(group, partner), device_id_type=MESH)
    for j in range(1, groups):
        for b in range(2):
            pl.semaphore_signal(
                barrier, inc=1, device_id=(lax.rem(group + j, groups), 2 * chip + b), device_id_type=MESH
            )

    def local(i, src, dst):
        copy = pltpu.make_async_copy(src, dst, in_sem.at[i])
        copy.start()
        return copy

    q_load = local(0, q_hbm, q)
    kq_loads = [local(1 + b, kq_hbm.at[pl.ds(b * half, half)], kq.at[pl.ds(b * half, half)]) for b in range(2)]
    qr_load = local(3, qr_hbm.at[:, pl.ds(core * half, half)], qr)
    rope_load = local(4, rope_hbm, rope.at[core])
    cache_load = local(5, cache_hbm, cache.at[core])

    def remote(src, dst, send, recv, peer_group, peer):
        return pltpu.make_async_remote_copy(
            src_ref=src,
            dst_ref=dst,
            send_sem=send,
            recv_sem=recv,
            device_id=(peer_group, peer),
            device_id_type=MESH,
        )

    lane = lax.broadcasted_iota(jnp.int32, (1, rows), 1)
    block = (me * cols) // QB

    def scale_line(scale_ref, index):
        scales = scale_ref[...]
        at = lax.broadcasted_iota(jnp.int32, scales.shape, 0) == index
        return jnp.sum(jnp.where(at, scales, 0.0), axis=0, keepdims=True)

    def scale_column(line, count, first, step):
        shape = (count, heads)
        pick = lax.broadcasted_iota(jnp.int32, shape, 1) == lax.broadcasted_iota(jnp.int32, shape, 0) // step + first
        return jnp.sum(jnp.where(pick, line, 0.0), axis=1, keepdims=True)

    key_column = scale_column(scale_line(ks_ref, block), heads, 0, 1)
    own_head = lax.broadcasted_iota(jnp.int32, (half, rows), 0) == lane // drafts
    key_rows = [
        jnp.sum(jnp.where(own_head, key_column[b * half : (b + 1) * half], 0.0), axis=0, keepdims=True)
        for b in range(2)
    ]
    value_column = scale_column(scale_line(vs_ref, block), rows, other * half, drafts)

    q_load.wait()
    for b in range(2):
        for t in range(drafts):
            q_rows[b, pl.ds(t, half, stride=drafts), :] = q[t, b * half : (b + 1) * half, :].astype(F32)

    own = lax.broadcasted_iota(jnp.int32, (half, 1, rows), 0) == lane[None] // drafts
    for b in range(2):
        kq_loads[b].wait()
        every = lax.dot_general(
            kq[b * half : (b + 1) * half].reshape(half * cols, kq.shape[2]),
            q_rows[b].astype(BF16),
            (((1,), (1,)), ((), ())),
            preferred_element_type=F32,
        ).reshape(half, cols, rows)
        lat_send[b] = (jnp.sum(jnp.where(own, every, 0.0), axis=0) * key_rows[b]).astype(BF16)
        if b == 0:
            pl.semaphore_wait(barrier, n - 1 + 2 * (groups - 1))
        for k in far_first:
            if k:
                remote(
                    lat_send.at[b], lat_all.at[me], lat_s.at[b, k], lat_r.at[me], group, 2 * peers[k] + b
                ).start()
    lat_pair = remote(lat_send.at[other], lat_all.at[me], lat_ps, lat_r.at[me], group, partner)
    lat_pair.start()
    lat_all[me] = lat_send[core]

    swaps = [
        remote(src, dst, swap_s.at[i], swap_r.at[i], group, partner)
        for i, (src, dst) in enumerate(
            (
                (rope_hbm, rope.at[core]),
                (cache_hbm, cache.at[core]),
                (vq_hbm.at[pl.ds(core * half, half)], vq.at[:, pl.ds(core * cols, cols)]),
                (w_hbm.at[:, pl.ds(core * span, span)], w.at[core]),
            )
        )
    ]
    swap_arrive = [
        remote(src, dst, swap_s.at[i], swap_r.at[i], group, partner)
        for i, (src, dst) in enumerate(
            (
                (rope_hbm, rope.at[other]),
                (cache_hbm, cache.at[other]),
                (vq_hbm.at[pl.ds(core * half, half)], vq.at[:, pl.ds(other * cols, cols)]),
                (w_hbm.at[:, pl.ds(core * span, span)], w.at[other]),
            )
        )
    ]
    for each in swaps:
        each.start()
    vq_load = local(6, vq_hbm.at[pl.ds(other * half, half)], vq.at[:, pl.ds(core * cols, cols)])
    w_load = local(7, w_hbm.at[:, pl.ds(other * span, span)], w.at[core])

    qr_load.wait()
    for t in range(drafts):
        qr_rows[pl.ds(t, half, stride=drafts), :] = qr[t].astype(F32)
    query_rope = qr_rows[...].astype(BF16)

    def prepare(j):
        turned = lax.dot_general(
            rope[j].T, query_rope, (((1,), (1,)), ((), ())), preferred_element_type=F32
        )
        position = (2 * chip + j) * positions + lax.broadcasted_iota(jnp.int32, (positions, rows), 0)
        horizon = len_ref[0] + lax.rem(lax.broadcasted_iota(jnp.int32, (positions, rows), 1), drafts)
        base[j] = jnp.where(position < horizon, turned * factor, neg_large)
        cache_t[j] = cache[j].T

    rope_load.wait()
    cache_load.wait()
    prepare(core)
    swap_arrive[0].wait_recv()
    swap_arrive[1].wait_recv()
    prepare(other)

    def lat_wait(k):
        for b in range(2):
            src = 2 * peers[k] + b
            remote(lat_send.at[b], lat_all.at[src], lat_s.at[b, k], lat_r.at[src], group, src).wait_recv()

    quarter = chips // 2
    near = chip // quarter
    remote(lat_send.at[other], lat_all.at[partner], lat_ps, lat_r.at[partner], group, partner).wait_recv()
    for k in range(1, quarter):
        lat_wait(k)

    def part_scores(side):
        begin = pl.multiple_of(side * (latent // 2), latent // 2)
        query = lat_all[pl.ds(side * chips, chips)].reshape(latent // 2, rows)
        return [
            jnp.dot(cache[j, :, pl.ds(begin, latent // 2)], query, preferred_element_type=F32) * factor + base[j]
            for j in range(2)
        ]

    for j, each in enumerate(part_scores(near)):
        base[j] = each
    for k in range(quarter, chips):
        lat_wait(k)
    scores = part_scores(1 - near)
    block_max = jnp.maximum(
        jnp.max(scores[0], axis=0, keepdims=True), jnp.max(scores[1], axis=0, keepdims=True)
    )
    probs = [jnp.exp(each - block_max) for each in scores]
    st_send[0:1, :] = block_max
    st_send[1:2, :] = jnp.sum(probs[0], axis=0, keepdims=True) + jnp.sum(probs[1], axis=0, keepdims=True)

    def exchange(src_of, dst, send, recv, ks):
        for k in ks:
            remote(src_of(k), dst.at[k], send.at[k], recv.at[k], group, 2 * peers[k] + other).start()

    def arrive(src_of, dst, send, recv, k):
        remote(src_of(k), dst.at[k], send.at[k], recv.at[k], group, 2 * peers[k] + other).wait_recv()

    st = (lambda k: st_send, st_all, st_s, st_r)
    exchange(*st, far_first)
    probs = [each.astype(BF16) for each in probs]
    o = (lambda k: out_send.at[peers[k]], out_recv, o_s, o_r)
    for side, ks in ((1 - near, range(chips - 1, quarter - 1, -1)), (near, range(quarter - 1, -1, -1))):
        begin = pl.multiple_of(side * (latent // 2), latent // 2)
        block_out = sum(
            jnp.dot(cache_t[j, pl.ds(begin, latent // 2), :], probs[j], preferred_element_type=F32)
            for j in range(2)
        )
        out_send[pl.ds(side * quarter, quarter)] = block_out.astype(BF16).reshape(quarter, wide, rows)
        exchange(*o, ks)

    vq_load.wait()
    swap_arrive[2].wait_recv()

    for k in range(chips):
        arrive(*st, k)
    all_max = [st_all[k, 0:1, :] for k in range(chips)]
    top = functools.reduce(jnp.maximum, all_max)
    weight = [jnp.exp(each - top) for each in all_max]
    total = sum(weight[k] * st_all[k, 1:2, :] for k in range(chips))
    merged = jnp.zeros((wide, rows), F32)
    for k in range(chips):
        arrive(*o, k)
        merged = merged + out_recv[k].astype(F32) * weight[k]
    merged = (merged / total).astype(BF16).astype(F32).T
    tile = per * wide
    spread = jnp.concatenate([merged] * per, axis=1)
    keep = (
        lax.broadcasted_iota(jnp.int32, (rows, tile), 1) // wide
        == lax.rem(lax.broadcasted_iota(jnp.int32, (rows, tile), 0) // drafts, per)
    )
    spread = jnp.where(keep, spread, 0.0).astype(BF16)
    for e in range(chips):
        part = jnp.dot(
            spread[e * share : (e + 1) * share],
            vq[e * per : (e + 1) * per].reshape(tile, width),
            preferred_element_type=F32,
        )
        part_send[e] = (part * value_column[e * share : (e + 1) * share]).astype(BF16)
    p = (lambda k: part_send.at[peers[k]], part_recv, p_s, p_r)
    exchange(*p, far_first)
    summed = jnp.zeros((share, width), F32)
    for k in range(chips):
        arrive(*p, k)
        summed = summed + part_recv[k].astype(F32)
    for h in range(per):
        share_send[:, h * width : (h + 1) * width] = summed[h * drafts : (h + 1) * drafts].astype(BF16)
    s = (lambda k: share_send, share_recv, s_s, s_r)
    exchange(*s, far_first)

    w_load.wait()
    swap_arrive[3].wait_recv()
    model = w.shape[1]
    final = [jnp.zeros((drafts, model), F32) for j in range(2)]
    for k in range(chips):
        arrive(*s, k)
        begin = pl.multiple_of(peers[k] * (per * width), per * width)
        for j in range(2):
            final[j] = final[j] + lax.dot_general(
                share_recv[k],
                w[j, :, pl.ds(begin, per * width)],
                (((1,), (1,)), ((), ())),
                preferred_element_type=F32,
            )
    for j in range(2):
        fin_send[j] = final[j]

    def last(i, j, b):
        peer_group = lax.rem(group + j, groups)
        side = core if b == 0 else other
        return remote(fin_send.at[side], fin_recv.at[i], f_s.at[i], f_r.at[i], peer_group, 2 * chip + side)

    lasts = [last(i, j, b) for i, (j, b) in enumerate((j, b) for j in range(groups) for b in range(2) if j or b)]
    for each in lasts[::-1]:
        each.start()
    result = fin_send[core]
    back = [((-j) % groups, b) for j in range(groups) for b in range(2) if j or b]
    for i in range(len(lasts)):
        lasts[i].wait_recv()
        result = result + fin_recv[i]
    out_ref[...] = result.astype(BF16)

    for src_of, dst, send, recv in (st, o, p, s):
        for k in range(chips):
            remote(src_of(k), dst.at[k], send.at[k], recv.at[k], group, 2 * peers[k] + other).wait_send()
    for b in range(2):
        for k in range(1, chips):
            remote(
                lat_send.at[b], lat_all.at[me], lat_s.at[b, k], lat_r.at[me], group, 2 * peers[k] + b
            ).wait_send()
    lat_pair.wait_send()
    for each in swaps:
        each.wait_send()
    for each in lasts:
        each.wait_send()


def solution(mesh):
    n = mesh.shape["seq"]
    groups = mesh.shape["heads"]

    def paired(query_nope, query_rope, latent_cache, rope_keys, lengths, key_quant, key_scale, value_quant, value_scale, out_weight):
        drafts, heads, nope = query_nope.shape[1:]
        rope = query_rope.shape[-1]
        positions, latent = latent_cache.shape[1:]
        cols = key_quant.shape[1]
        width = value_quant.shape[2]
        model = out_weight.shape[1]
        chips = n // 2
        half = heads // 2
        rows = half * drafts
        share = rows // chips
        wide = 2 * cols
        hbm = pl.BlockSpec(memory_space=pltpu.HBM)
        vmem = pl.BlockSpec(memory_space=pltpu.VMEM)
        smem = pl.BlockSpec(memory_space=pltpu.SMEM)
        dma = pltpu.SemaphoreType.DMA
        lasts = 2 * groups - 1
        result = pl.pallas_call(
            functools.partial(pair_kernel, n, groups, heads, drafts),
            out_shape=jax.ShapeDtypeStruct((drafts, model), BF16),
            in_specs=[hbm, hbm, hbm, hbm, smem, hbm, vmem, hbm, vmem, hbm],
            out_specs=vmem,
            scratch_shapes=[
                pltpu.VMEM((drafts, heads, nope), BF16),
                pltpu.VMEM((drafts, half, rope), BF16),
                pltpu.VMEM((2, positions, latent), BF16),
                pltpu.VMEM((2, rope, positions), BF16),
                pltpu.VMEM((heads, cols, nope), BF16),
                pltpu.VMEM((half, wide, width), BF16),
                pltpu.VMEM((2, model, half * width), BF16),
                pltpu.VMEM((2, rows, nope), F32),
                pltpu.VMEM((rows, rope), F32),
                pltpu.VMEM((2, latent, positions), BF16),
                pltpu.VMEM((2, positions, rows), F32),
                pltpu.VMEM((2, cols, rows), BF16),
                pltpu.VMEM((n, cols, rows), BF16),
                pltpu.VMEM((2, rows), F32),
                pltpu.VMEM((chips, 2, rows), F32),
                pltpu.VMEM((chips, wide, rows), BF16),
                pltpu.VMEM((chips, wide, rows), BF16),
                pltpu.VMEM((chips, share, width), BF16),
                pltpu.VMEM((chips, share, width), BF16),
                pltpu.VMEM((drafts, share // drafts * width), BF16),
                pltpu.VMEM((chips, drafts, share // drafts * width), BF16),
                pltpu.VMEM((2, drafts, model), F32),
                pltpu.VMEM((lasts, drafts, model), F32),
                dma((8,)),
                dma((4,)),
                dma((4,)),
                dma((2, chips)),
                dma,
                dma((n,)),
            ]
            + [dma((chips,))] * 8
            + [dma((lasts,))] * 2,
            compiler_params=pltpu.CompilerParams(
                collective_id=0, has_side_effects=True, vmem_limit_bytes=63 * 1024 * 1024
            ),
        )(
            query_nope.reshape(drafts, heads, nope),
            query_rope.reshape(drafts, heads, rope),
            latent_cache.reshape(positions, latent),
            rope_keys.reshape(rope, positions),
            lengths,
            key_quant,
            key_scale.T,
            value_quant,
            value_scale.T,
            out_weight.T,
        )
        return result.reshape(1, drafts, model)

    def per_device(*args):
        drafts, heads = args[0].shape[1:3]
        chips = n // 2
        rows = heads // 2 * drafts
        paired_fits = (
            n % 2 == 0
            and chips & (chips - 1) == 0
            and chips >= 2
            and heads % (2 * chips) == 0
            and rows % 128 == 0
            and args[5].shape[1] % 16 == 0
            and QB % (2 * args[5].shape[1]) == 0
        )
        return (paired if paired_fits else spread_out)(*args)

    def spread_out(
        query_nope,
        query_rope,
        latent_cache,
        rope_keys,
        lengths,
        key_quant,
        key_scale,
        value_quant,
        value_scale,
        out_weight,
    ):
        batch, drafts, heads, nope = query_nope.shape
        rows = batch * drafts * heads
        rope = query_rope.shape[-1]
        positions, latent = latent_cache.shape[1:]
        cols = key_quant.shape[1]
        width = value_quant.shape[2]
        model = out_weight.shape[1]
        hbm = pl.BlockSpec(memory_space=pltpu.HBM)
        vmem = pl.BlockSpec(memory_space=pltpu.VMEM)
        smem = pl.BlockSpec(memory_space=pltpu.SMEM)
        dma = pltpu.SemaphoreType.DMA
        result = pl.pallas_call(
            functools.partial(kernel, n, groups, heads, drafts),
            out_shape=jax.ShapeDtypeStruct((drafts, model), BF16),
            in_specs=[hbm, hbm, hbm, hbm, smem, hbm, vmem, hbm, vmem, hbm],
            out_specs=vmem,
            scratch_shapes=[
                pltpu.VMEM((rows, nope), BF16),
                pltpu.VMEM((rows, rope), BF16),
                pltpu.VMEM((positions, latent), BF16),
                pltpu.VMEM((rope, positions), BF16),
                pltpu.VMEM((heads * cols, nope), BF16),
                pltpu.VMEM((heads * cols, width), BF16),
                pltpu.VMEM(out_weight.shape[::-1], BF16),
                pltpu.VMEM((latent, positions), BF16),
                pltpu.VMEM((width, heads * cols), BF16),
                pltpu.VMEM((positions, rows), F32),
                pltpu.VMEM((n, cols, rows), BF16),
                pltpu.VMEM((n, 2, rows), F32),
                pltpu.VMEM((n, cols, rows), BF16),
                pltpu.VMEM((n, cols, rows), BF16),
                pltpu.VMEM((n, width // n, rows), BF16),
                pltpu.VMEM((n, width // n, rows), BF16),
                pltpu.VMEM((n, width // n, rows), BF16),
                pltpu.VMEM((drafts, heads * width), BF16),
                pltpu.VMEM((drafts, heads, width), F32),
                pltpu.VMEM((groups, drafts, model), F32),
                dma((7,)),
            ]
            + [dma((n,))] * 11
            + [dma((groups,))] * 2,
            compiler_params=pltpu.CompilerParams(
                collective_id=0, has_side_effects=True, vmem_limit_bytes=63 * 1024 * 1024
            ),
        )(
            query_nope.reshape(rows, nope),
            query_rope.reshape(rows, rope),
            latent_cache.reshape(positions, latent),
            rope_keys.reshape(rope, positions),
            lengths,
            key_quant.reshape(heads * cols, nope),
            key_scale.T,
            value_quant.reshape(heads * cols, width),
            value_scale.T,
            out_weight.T,
        )
        return result.reshape(batch, drafts, model)

    in_specs = (
        P(None, None, "heads", None),
        P(None, None, "heads", None),
        P(None, "seq", None),
        P(None, None, "seq"),
        P(),
        P("heads", "seq", None),
        P("heads", None),
        P("heads", "seq", None),
        P("heads", None),
        P("heads", "seq"),
    )
    return jax.shard_map(
        per_device, mesh=mesh, in_specs=in_specs, out_specs=P(None, None, "seq"), check_vma=False
    )
```

```python
import functools

import jax
import jax.numpy as jnp
from jax import lax
from jax.experimental import pallas as pl
from jax.experimental.pallas import tpu as pltpu
from jax.sharding import PartitionSpec as P

QB = 128
VMEM_LIMIT = 67043328 - 32768
MESH = pl.DeviceIdType.MESH
neg_large = -1e30
F32 = jnp.float32
BF16 = jnp.bfloat16


def scale_row(scale_ref, block, rows, heads):
    scales = scale_ref[...]
    line = jnp.sum(
        jnp.where(lax.broadcasted_iota(jnp.int32, scales.shape, 0) == block, scales, 0.0),
        axis=0,
        keepdims=True,
    )
    square = (heads, heads)
    diagonal = lax.broadcasted_iota(jnp.int32, square, 0) == lax.broadcasted_iota(jnp.int32, square, 1)
    column = jnp.sum(jnp.where(diagonal, line, 0.0), axis=1, keepdims=True)
    lane_head = lax.broadcasted_iota(jnp.int32, (heads, rows), 1) % heads
    own_head = lax.broadcasted_iota(jnp.int32, (heads, rows), 0)
    return jnp.sum(jnp.where(lane_head == own_head, column, 0.0), axis=0, keepdims=True)


def kernel(
    n,
    groups,
    heads,
    drafts,
    q_hbm,
    qr_hbm,
    cache_hbm,
    rope_hbm,
    len_ref,
    kq_hbm,
    ks_ref,
    vq_hbm,
    vs_ref,
    w_hbm,
    out_ref,
    q,
    qr,
    cache,
    rope,
    kq,
    vq,
    w,
    cache_t,
    vq_t,
    base,
    lat_all,
    stats,
    out_send,
    out_recv,
    part_send,
    part_recv,
    share_all,
    flat,
    heads_out,
    final,
    in_sem,
    lat_send,
    lat_recv,
    pass_send,
    st_send,
    st_recv,
    o_send,
    o_recv,
    p_send,
    p_recv,
    s_send,
    s_recv,
    f_send,
    f_recv,
):
    me = lax.axis_index("seq")
    group = lax.axis_index("heads")
    rows = q.shape[0]
    cols = lat_all.shape[1]
    width = vq.shape[1]
    positions = cache.shape[0]
    factor = (q.shape[1] + qr.shape[1]) ** (-0.5)

    loads = []
    for i, (src, dst) in enumerate(
        ((kq_hbm, kq), (q_hbm, q), (qr_hbm, qr), (rope_hbm, rope), (cache_hbm, cache), (vq_hbm, vq), (w_hbm, w))
    ):
        copy = pltpu.make_async_copy(src, dst, in_sem.at[i])
        if dst is not w:
            copy.start()
        loads.append(copy)
    kq_load, q_load, qr_load, rope_load, cache_load, vq_load, w_load = loads

    barrier = pltpu.get_barrier_semaphore()

    def greet_seq(j, c):
        pl.semaphore_signal(barrier, inc=1, device_id=(group, lax.rem(me + j, n)), device_id_type=MESH)
        return c

    def greet_heads(j, c):
        pl.semaphore_signal(barrier, inc=1, device_id=(lax.rem(group + j, groups), me), device_id_type=MESH)
        return c

    lax.fori_loop(1, n, greet_seq, 0)
    lax.fori_loop(1, groups, greet_heads, 0)

    def spread(src_of, dst, send, recv):
        def make(j):
            peer = lax.rem(me + j, n)
            return pltpu.make_async_remote_copy(
                src_ref=src_of(peer),
                dst_ref=dst.at[me],
                send_sem=send.at[peer],
                recv_sem=recv.at[me],
                device_id=(group, peer),
                device_id_type=MESH,
            )

        def go(j, c):
            make(j).start()
            return c

        lax.fori_loop(1, n, go, 0)

    def arrive(src_of, dst, send, recv):
        def wait(j, c):
            peer = lax.rem(me + j, n)
            pltpu.make_async_remote_copy(
                src_ref=src_of(peer),
                dst_ref=dst.at[peer],
                send_sem=send.at[peer],
                recv_sem=recv.at[peer],
                device_id=(group, peer),
                device_id_type=MESH,
            ).wait_recv()
            return c

        lax.fori_loop(1, n, wait, 0)

    def drain(src_of, dst, send, recv):
        def wait(j, c):
            peer = lax.rem(me + j, n)
            pltpu.make_async_remote_copy(
                src_ref=src_of(peer),
                dst_ref=dst.at[me],
                send_sem=send.at[peer],
                recv_sem=recv.at[me],
                device_id=(group, peer),
                device_id_type=MESH,
            ).wait_send()
            return c

        lax.fori_loop(1, n, wait, 0)

    block = (me * cols) // QB
    lane_head = lax.broadcasted_iota(jnp.int32, (1, rows), 1) % heads
    key_row = scale_row(ks_ref, block, rows, heads)
    value_row = scale_row(vs_ref, block, rows, heads)

    kq_load.wait()
    q_load.wait()
    every = lax.dot_general(kq[...], q[...], (((1,), (1,)), ((), ())), preferred_element_type=F32)
    every = every.reshape(heads, cols, rows)
    own = lax.broadcasted_iota(jnp.int32, (heads, 1, rows), 0) == lane_head[None]
    piece = jnp.sum(jnp.where(own, every, 0.0), axis=0) * key_row
    lat_all[me] = piece.astype(BF16)

    pl.semaphore_wait(barrier, n - 1 + groups - 1)

    partner = me + 1 - 2 * lax.rem(me, 2)

    def lat_copy(slot, peer, send):
        return pltpu.make_async_remote_copy(
            src_ref=lat_all.at[slot],
            dst_ref=lat_all.at[slot],
            send_sem=send,
            recv_sem=lat_recv.at[slot],
            device_id=(group, peer),
            device_id_type=MESH,
        )

    def like(j):
        return lax.rem(me + 2 * j, n)

    def lat_go(j, c):
        lat_copy(me, like(j), lat_send.at[like(j)]).start()
        return c

    def lat_pass(j, c):
        lat_copy(like(j), partner, pass_send.at[like(j)]).wait_recv()
        lat_copy(like(j), partner, pass_send.at[like(j)]).start()
        return c

    def lat_rest(j, c):
        other = lax.rem(partner + 2 * j, n)
        lat_copy(other, partner, pass_send.at[other]).wait_recv()
        return c

    def lat_drain(j, c):
        lat_copy(me, like(j), lat_send.at[like(j)]).wait_send()
        lat_copy(like(j), partner, pass_send.at[like(j)]).wait_send()
        return c

    lax.fori_loop(1, n // 2, lat_go, 0)
    lat_copy(me, partner, lat_send.at[partner]).start()
    w_load.start()

    qr_load.wait()
    rope_load.wait()
    base[...] = lax.dot_general(
        rope[...].T, qr[...], (((1,), (1,)), ((), ())), preferred_element_type=F32
    )
    cache_load.wait()
    cache_t[...] = cache[...].T
    lax.fori_loop(1, n // 2, lat_pass, 0)
    position = me * positions + lax.broadcasted_iota(jnp.int32, (positions, rows), 0)
    horizon = len_ref[0] + lax.broadcasted_iota(jnp.int32, (positions, rows), 1) // heads
    visible = position < horizon

    lax.fori_loop(0, n // 2, lat_rest, 0)
    query_latent = lat_all[...].reshape(n * cols, rows)
    scores = (jnp.dot(cache[...], query_latent, preferred_element_type=F32) + base[...]) * factor
    block_max = jnp.max(jnp.where(visible, scores, neg_large), axis=0, keepdims=True)
    probs = jnp.where(visible, jnp.exp(scores - block_max), 0.0)
    block_sum = jnp.sum(probs, axis=0, keepdims=True)
    stats[me, 0:1, :] = block_max
    stats[me, 1:2, :] = block_sum
    st = (lambda peer: stats.at[me], stats, st_send, st_recv)
    spread(*st)
    block_out = jnp.dot(cache_t[...], probs.astype(BF16), preferred_element_type=F32)
    out_send[...] = block_out.astype(BF16).reshape(n, cols, rows)
    o = (lambda peer: out_send.at[peer], out_recv, o_send, o_recv)
    spread(*o)
    out_recv[me] = out_send[me]
    vq_load.wait()
    vq_t[...] = vq[...].T

    arrive(*st)
    all_max = stats[:, 0:1, :]
    top = jnp.max(all_max, axis=0, keepdims=True)
    weight = jnp.exp(all_max - top)
    total = jnp.sum(weight * stats[:, 1:2, :], axis=0)
    arrive(*o)
    merged = jnp.sum(out_recv[...].astype(F32) * weight, axis=0) / total
    latent = jnp.where(own, merged[None], 0.0).astype(BF16).reshape(heads * cols, rows)
    partial = jnp.dot(vq_t[...], latent, preferred_element_type=F32) * value_row
    step = width // n
    for d in range(n):
        part_send[d] = partial[d * step : (d + 1) * step].astype(part_send.dtype)
    p = (lambda peer: part_send.at[peer], part_recv, p_send, p_recv)
    spread(*p)
    part_recv[me] = part_send[me]
    arrive(*p)
    share_all[me] = jnp.sum(part_recv[...].astype(F32), axis=0).astype(BF16)
    s = (lambda peer: share_all.at[me], share_all, s_send, s_recv)
    spread(*s)
    arrive(*s)
    head_t = jnp.concatenate([share_all[d].astype(F32) for d in range(n)], axis=0)
    heads_out[...] = head_t.T.reshape(drafts, heads, width)
    for k in range(heads):
        flat[:, k * width : (k + 1) * width] = heads_out[:, k, :].astype(BF16)
    w_load.wait()
    final[group] = lax.dot_general(
        flat[...], w[...], (((1,), (1,)), ((), ())), preferred_element_type=F32
    )

    def pair(j, at):
        peer = lax.rem(group + j, groups)
        return pltpu.make_async_remote_copy(
            src_ref=final.at[group],
            dst_ref=final.at[group if at else peer],
            send_sem=f_send.at[peer],
            recv_sem=f_recv.at[group if at else peer],
            device_id=(peer, me),
            device_id_type=MESH,
        )

    for j in range(1, groups):
        pair(j, True).start()
    for j in range(1, groups):
        pair(j, False).wait_recv()
    out_ref[...] = jnp.sum(final[...], axis=0).astype(BF16)
    for each in (st, o, p, s):
        drain(*each)
    lax.fori_loop(1, n // 2, lat_drain, 0)
    lat_copy(me, partner, lat_send.at[partner]).wait_send()
    for j in range(1, groups):
        pair(j, True).wait_send()


def chip_peer(chip, chips, k):
    out = 0
    bit = 1
    while bit < chips:
        own = lax.rem(chip // bit, 2)
        out = out + bit * ((1 - own) if k & bit else own)
        bit *= 2
    return out


def pair_kernel(
    n,
    groups,
    heads,
    drafts,
    q_hbm,
    qr_hbm,
    cache_hbm,
    rope_hbm,
    len_hbm,
    kq_hbm,
    ks_hbm,
    vq_hbm,
    vs_hbm,
    w_hbm,
    out_ref,
    len_ref,
    ks_ref,
    vs_ref,
    q,
    qr,
    cache,
    rope,
    kq,
    vq,
    w,
    q_rows,
    qr_rows,
    cache_t,
    base,
    lat_send,
    lat_all,
    st_send,
    st_all,
    out_send,
    out_recv,
    part_send,
    part_recv,
    share_send,
    share_recv,
    fin_send,
    fin_recv,
    in_sem,
    swap_s,
    swap_r,
    lat_s,
    lat_ps,
    lat_r,
    st_s,
    st_r,
    o_s,
    o_r,
    p_s,
    p_r,
    s_s,
    s_r,
    f_s,
    f_r,
):
    me = lax.axis_index("seq")
    group = lax.axis_index("heads")
    core = lax.rem(me, 2)
    other = 1 - core
    chip = me // 2
    chips = n // 2
    half = heads // 2
    rows = half * drafts
    cols = lat_all.shape[1]
    wide = 2 * cols
    latent = cache.shape[2]
    positions = cache.shape[1]
    width = vq.shape[2]
    span = half * width
    share = rows // chips
    per = share // drafts
    factor = (q.shape[2] + qr.shape[2]) ** (-0.5)
    far_first = range(chips - 1, -1, -1)
    peers = [chip_peer(chip, chips, k) for k in range(chips)]
    partner = 2 * chip + other

    barrier = pltpu.get_barrier_semaphore()
    for k in far_first:
        for b in range(2):
            if k:
                pl.semaphore_signal(barrier, inc=1, device_id=(group, 2 * peers[k] + b), device_id_type=MESH)
    pl.semaphore_signal(barrier, inc=1, device_id=(group, partner), device_id_type=MESH)
    for j in range(1, groups):
        for b in range(2):
            pl.semaphore_signal(
                barrier, inc=1, device_id=(lax.rem(group + j, groups), 2 * chip + b), device_id_type=MESH
            )

    def local(i, src, dst):
        copy = pltpu.make_async_copy(src, dst, in_sem.at[i])
        copy.start()
        return copy

    ks_load = local(8, ks_hbm, ks_ref)
    q_load = local(0, q_hbm, q)
    kq_loads = [local(1 + b, kq_hbm.at[pl.ds(b * half, half)], kq.at[pl.ds(b * half, half)]) for b in range(2)]
    qr_load = local(3, qr_hbm.at[:, pl.ds(core * half, half)], qr)
    rope_load = local(4, rope_hbm, rope.at[core])
    cache_load = local(5, cache_hbm, cache.at[core])
    vs_load = local(9, vs_hbm, vs_ref)
    len_load = local(10, len_hbm, len_ref)

    def remote(src, dst, send, recv, peer_group, peer):
        return pltpu.make_async_remote_copy(
            src_ref=src,
            dst_ref=dst,
            send_sem=send,
            recv_sem=recv,
            device_id=(peer_group, peer),
            device_id_type=MESH,
        )

    lane = lax.broadcasted_iota(jnp.int32, (1, rows), 1)
    block = (me * cols) // QB

    def scale_line(scale_ref, index):
        scales = scale_ref[...]
        at = lax.broadcasted_iota(jnp.int32, scales.shape, 0) == index
        return jnp.sum(jnp.where(at, scales, 0.0), axis=0, keepdims=True)

    def scale_column(line, count, first, step):
        shape = (count, heads)
        pick = lax.broadcasted_iota(jnp.int32, shape, 1) == lax.broadcasted_iota(jnp.int32, shape, 0) // step + first
        return jnp.sum(jnp.where(pick, line, 0.0), axis=1, keepdims=True)

    ks_load.wait()
    key_column = scale_column(scale_line(ks_ref, block), heads, 0, 1)
    own_head = lax.broadcasted_iota(jnp.int32, (half, rows), 0) == lane // drafts
    key_rows = [
        jnp.sum(jnp.where(own_head, key_column[b * half : (b + 1) * half], 0.0), axis=0, keepdims=True)
        for b in range(2)
    ]

    q_load.wait()
    for b in range(2):
        for t in range(drafts):
            q_rows[b, pl.ds(t, half, stride=drafts), :] = q[t, b * half : (b + 1) * half, :].astype(F32)

    own = lax.broadcasted_iota(jnp.int32, (half, 1, rows), 0) == lane[None] // drafts
    for b in range(2):
        kq_loads[b].wait()
        every = lax.dot_general(
            kq[b * half : (b + 1) * half].reshape(half * cols, kq.shape[2]),
            q_rows[b].astype(BF16),
            (((1,), (1,)), ((), ())),
            preferred_element_type=F32,
        ).reshape(half, cols, rows)
        lat_send[b] = (jnp.sum(jnp.where(own, every, 0.0), axis=0) * key_rows[b]).astype(BF16)
        if b == 0:
            pl.semaphore_wait(barrier, n - 1 + 2 * (groups - 1))
        for k in far_first:
            if k:
                remote(
                    lat_send.at[b], lat_all.at[me], lat_s.at[b, k], lat_r.at[me], group, 2 * peers[k] + b
                ).start()
    lat_pair = remote(lat_send.at[other], lat_all.at[me], lat_ps, lat_r.at[me], group, partner)
    lat_pair.start()
    lat_all[me] = lat_send[core]

    swaps = [
        remote(src, dst, swap_s.at[i], swap_r.at[i], group, partner)
        for i, (src, dst) in enumerate(
            (
                (rope_hbm, rope.at[core]),
                (cache_hbm, cache.at[core]),
                (vq_hbm.at[pl.ds(core * half, half)], vq.at[:, pl.ds(core * cols, cols)]),
                (w_hbm.at[:, pl.ds(core * span, span)], w.at[core]),
            )
        )
    ]
    swap_arrive = [
        remote(src, dst, swap_s.at[i], swap_r.at[i], group, partner)
        for i, (src, dst) in enumerate(
            (
                (rope_hbm, rope.at[other]),
                (cache_hbm, cache.at[other]),
                (vq_hbm.at[pl.ds(core * half, half)], vq.at[:, pl.ds(other * cols, cols)]),
                (w_hbm.at[:, pl.ds(core * span, span)], w.at[other]),
            )
        )
    ]
    for each in swaps:
        each.start()
    vq_load = local(6, vq_hbm.at[pl.ds(other * half, half)], vq.at[:, pl.ds(core * cols, cols)])
    w_load = local(7, w_hbm.at[:, pl.ds(other * span, span)], w.at[core])

    qr_load.wait()
    for t in range(drafts):
        qr_rows[pl.ds(t, half, stride=drafts), :] = qr[t].astype(F32)
    query_rope = qr_rows[...].astype(BF16)

    def prepare(j):
        turned = lax.dot_general(
            rope[j].T, query_rope, (((1,), (1,)), ((), ())), preferred_element_type=F32
        )
        position = (2 * chip + j) * positions + lax.broadcasted_iota(jnp.int32, (positions, rows), 0)
        horizon = len_ref[0] + lax.rem(lax.broadcasted_iota(jnp.int32, (positions, rows), 1), drafts)
        base[j] = jnp.where(position < horizon, turned * factor, neg_large)
        cache_t[j] = cache[j].T

    vs_load.wait()
    value_column = scale_column(scale_line(vs_ref, block), rows, other * half, drafts)
    len_load.wait()
    rope_load.wait()
    cache_load.wait()
    prepare(core)
    swap_arrive[0].wait_recv()
    swap_arrive[1].wait_recv()
    prepare(other)

    def lat_wait(k):
        for b in range(2):
            src = 2 * peers[k] + b
            remote(lat_send.at[b], lat_all.at[src], lat_s.at[b, k], lat_r.at[src], group, src).wait_recv()

    quarter = chips // 2
    near = chip // quarter
    remote(lat_send.at[other], lat_all.at[partner], lat_ps, lat_r.at[partner], group, partner).wait_recv()
    for k in range(1, quarter):
        lat_wait(k)

    def part_scores(side):
        begin = pl.multiple_of(side * (latent // 2), latent // 2)
        query = lat_all[pl.ds(side * chips, chips)].reshape(latent // 2, rows)
        return [
            jnp.dot(cache[j, :, pl.ds(begin, latent // 2)], query, preferred_element_type=F32) * factor + base[j]
            for j in range(2)
        ]

    for j, each in enumerate(part_scores(near)):
        base[j] = each
    for k in range(quarter, chips):
        lat_wait(k)
    scores = part_scores(1 - near)
    block_max = jnp.maximum(
        jnp.max(scores[0], axis=0, keepdims=True), jnp.max(scores[1], axis=0, keepdims=True)
    )
    probs = [jnp.exp(each - block_max) for each in scores]
    st_send[0:1, :] = block_max
    st_send[1:2, :] = jnp.sum(probs[0], axis=0, keepdims=True) + jnp.sum(probs[1], axis=0, keepdims=True)

    def exchange(src_of, dst, send, recv, ks):
        for k in ks:
            remote(src_of(k), dst.at[k], send.at[k], recv.at[k], group, 2 * peers[k] + other).start()

    def arrive(src_of, dst, send, recv, k):
        remote(src_of(k), dst.at[k], send.at[k], recv.at[k], group, 2 * peers[k] + other).wait_recv()

    st = (lambda k: st_send, st_all, st_s, st_r)
    exchange(*st, far_first)
    probs = [each.astype(BF16) for each in probs]
    o = (lambda k: out_send.at[peers[k]], out_recv, o_s, o_r)
    for side, ks in ((1 - near, range(chips - 1, quarter - 1, -1)), (near, range(quarter - 1, -1, -1))):
        begin = pl.multiple_of(side * (latent // 2), latent // 2)
        block_out = sum(
            jnp.dot(cache_t[j, pl.ds(begin, latent // 2), :], probs[j], preferred_element_type=F32)
            for j in range(2)
        )
        out_send[pl.ds(side * quarter, quarter)] = block_out.astype(BF16).reshape(quarter, wide, rows)
        exchange(*o, ks)

    vq_load.wait()
    swap_arrive[2].wait_recv()

    for k in range(chips):
        arrive(*st, k)
    all_max = [st_all[k, 0:1, :] for k in range(chips)]
    top = functools.reduce(jnp.maximum, all_max)
    weight = [jnp.exp(each - top) for each in all_max]
    total = sum(weight[k] * st_all[k, 1:2, :] for k in range(chips))
    merged = jnp.zeros((wide, rows), F32)
    for k in range(chips):
        arrive(*o, k)
        merged = merged + out_recv[k].astype(F32) * weight[k]
    merged = (merged / total).astype(BF16).astype(F32).T
    tile = per * wide
    spread = jnp.concatenate([merged] * per, axis=1)
    keep = (
        lax.broadcasted_iota(jnp.int32, (rows, tile), 1) // wide
        == lax.rem(lax.broadcasted_iota(jnp.int32, (rows, tile), 0) // drafts, per)
    )
    spread = jnp.where(keep, spread, 0.0).astype(BF16)
    for e in range(chips):
        part = jnp.dot(
            spread[e * share : (e + 1) * share],
            vq[e * per : (e + 1) * per].reshape(tile, width),
            preferred_element_type=F32,
        )
        part_send[e] = (part * value_column[e * share : (e + 1) * share]).astype(BF16)
    p = (lambda k: part_send.at[peers[k]], part_recv, p_s, p_r)
    exchange(*p, far_first)
    summed = jnp.zeros((share, width), F32)
    for k in range(chips):
        arrive(*p, k)
        summed = summed + part_recv[k].astype(F32)
    for h in range(per):
        share_send[:, h * width : (h + 1) * width] = summed[h * drafts : (h + 1) * drafts].astype(BF16)
    s = (lambda k: share_send, share_recv, s_s, s_r)
    exchange(*s, far_first)

    w_load.wait()
    swap_arrive[3].wait_recv()
    model = w.shape[1]
    final = [jnp.zeros((drafts, model), F32) for j in range(2)]
    for k in range(chips):
        arrive(*s, k)
        begin = pl.multiple_of(peers[k] * (per * width), per * width)
        for j in range(2):
            final[j] = final[j] + lax.dot_general(
                share_recv[k],
                w[j, :, pl.ds(begin, per * width)],
                (((1,), (1,)), ((), ())),
                preferred_element_type=F32,
            )
    for j in range(2):
        fin_send[j] = final[j]

    def last(i, j, b):
        peer_group = lax.rem(group + j, groups)
        side = core if b == 0 else other
        return remote(fin_send.at[side], fin_recv.at[i], f_s.at[i], f_r.at[i], peer_group, 2 * chip + side)

    lasts = [last(i, j, b) for i, (j, b) in enumerate((j, b) for j in range(groups) for b in range(2) if j or b)]
    for each in lasts[::-1]:
        each.start()
    result = fin_send[core]
    back = [((-j) % groups, b) for j in range(groups) for b in range(2) if j or b]
    for i in range(len(lasts)):
        lasts[i].wait_recv()
        result = result + fin_recv[i]
    out_ref[...] = result.astype(BF16)

    for src_of, dst, send, recv in (st, o, p, s):
        for k in range(chips):
            remote(src_of(k), dst.at[k], send.at[k], recv.at[k], group, 2 * peers[k] + other).wait_send()
    for b in range(2):
        for k in range(1, chips):
            remote(
                lat_send.at[b], lat_all.at[me], lat_s.at[b, k], lat_r.at[me], group, 2 * peers[k] + b
            ).wait_send()
    lat_pair.wait_send()
    for each in swaps:
        each.wait_send()
    for each in lasts:
        each.wait_send()


def solution(mesh):
    n = mesh.shape["seq"]
    groups = mesh.shape["heads"]

    def paired(query_nope, query_rope, latent_cache, rope_keys, lengths, key_quant, key_scale, value_quant, value_scale, out_weight):
        drafts, heads, nope = query_nope.shape[1:]
        rope = query_rope.shape[-1]
        positions, latent = latent_cache.shape[1:]
        cols = key_quant.shape[1]
        width = value_quant.shape[2]
        model = out_weight.shape[1]
        chips = n // 2
        half = heads // 2
        rows = half * drafts
        share = rows // chips
        wide = 2 * cols
        hbm = pl.BlockSpec(memory_space=pltpu.HBM)
        vmem = pl.BlockSpec(memory_space=pltpu.VMEM)
        dma = pltpu.SemaphoreType.DMA
        lasts = 2 * groups - 1
        result = pl.pallas_call(
            functools.partial(pair_kernel, n, groups, heads, drafts),
            out_shape=pltpu.VMEM((drafts, model), BF16),
            in_specs=[hbm] * 10,
            out_specs=vmem,
            scratch_shapes=[
                pltpu.SMEM(lengths.shape, jnp.int32),
                pltpu.VMEM(key_scale.shape[::-1], F32),
                pltpu.VMEM(value_scale.shape[::-1], F32),
                pltpu.VMEM((drafts, heads, nope), BF16),
                pltpu.VMEM((drafts, half, rope), BF16),
                pltpu.VMEM((2, positions, latent), BF16),
                pltpu.VMEM((2, rope, positions), BF16),
                pltpu.VMEM((heads, cols, nope), BF16),
                pltpu.VMEM((half, wide, width), BF16),
                pltpu.VMEM((2, model, half * width), BF16),
                pltpu.VMEM((2, rows, nope), F32),
                pltpu.VMEM((rows, rope), F32),
                pltpu.VMEM((2, latent, positions), BF16),
                pltpu.VMEM((2, positions, rows), F32),
                pltpu.VMEM((2, cols, rows), BF16),
                pltpu.VMEM((n, cols, rows), BF16),
                pltpu.VMEM((2, rows), F32),
                pltpu.VMEM((chips, 2, rows), F32),
                pltpu.VMEM((chips, wide, rows), BF16),
                pltpu.VMEM((chips, wide, rows), BF16),
                pltpu.VMEM((chips, share, width), BF16),
                pltpu.VMEM((chips, share, width), BF16),
                pltpu.VMEM((drafts, share // drafts * width), BF16),
                pltpu.VMEM((chips, drafts, share // drafts * width), BF16),
                pltpu.VMEM((2, drafts, model), F32),
                pltpu.VMEM((lasts, drafts, model), F32),
                dma((11,)),
                dma((4,)),
                dma((4,)),
                dma((2, chips)),
                dma,
                dma((n,)),
            ]
            + [dma((chips,))] * 8
            + [dma((lasts,))] * 2,
            compiler_params=pltpu.CompilerParams(
                collective_id=0, has_side_effects=True, vmem_limit_bytes=VMEM_LIMIT
            ),
        )(
            query_nope.reshape(drafts, heads, nope),
            query_rope.reshape(drafts, heads, rope),
            latent_cache.reshape(positions, latent),
            rope_keys.reshape(rope, positions),
            lengths,
            key_quant,
            key_scale.T,
            value_quant,
            value_scale.T,
            out_weight.T,
        )
        return result.reshape(1, drafts, model)

    def per_device(*args):
        drafts, heads = args[0].shape[1:3]
        chips = n // 2
        rows = heads // 2 * drafts
        paired_fits = (
            n % 2 == 0
            and chips & (chips - 1) == 0
            and chips >= 2
            and heads % (2 * chips) == 0
            and rows % 128 == 0
            and args[5].shape[1] % 16 == 0
            and QB % (2 * args[5].shape[1]) == 0
        )
        return (paired if paired_fits else spread_out)(*args)

    def spread_out(
        query_nope,
        query_rope,
        latent_cache,
        rope_keys,
        lengths,
        key_quant,
        key_scale,
        value_quant,
        value_scale,
        out_weight,
    ):
        batch, drafts, heads, nope = query_nope.shape
        rows = batch * drafts * heads
        rope = query_rope.shape[-1]
        positions, latent = latent_cache.shape[1:]
        cols = key_quant.shape[1]
        width = value_quant.shape[2]
        model = out_weight.shape[1]
        hbm = pl.BlockSpec(memory_space=pltpu.HBM)
        vmem = pl.BlockSpec(memory_space=pltpu.VMEM)
        smem = pl.BlockSpec(memory_space=pltpu.SMEM)
        dma = pltpu.SemaphoreType.DMA
        result = pl.pallas_call(
            functools.partial(kernel, n, groups, heads, drafts),
            out_shape=jax.ShapeDtypeStruct((drafts, model), BF16),
            in_specs=[hbm, hbm, hbm, hbm, smem, hbm, vmem, hbm, vmem, hbm],
            out_specs=vmem,
            scratch_shapes=[
                pltpu.VMEM((rows, nope), BF16),
                pltpu.VMEM((rows, rope), BF16),
                pltpu.VMEM((positions, latent), BF16),
                pltpu.VMEM((rope, positions), BF16),
                pltpu.VMEM((heads * cols, nope), BF16),
                pltpu.VMEM((heads * cols, width), BF16),
                pltpu.VMEM(out_weight.shape[::-1], BF16),
                pltpu.VMEM((latent, positions), BF16),
                pltpu.VMEM((width, heads * cols), BF16),
                pltpu.VMEM((positions, rows), F32),
                pltpu.VMEM((n, cols, rows), BF16),
                pltpu.VMEM((n, 2, rows), F32),
                pltpu.VMEM((n, cols, rows), BF16),
                pltpu.VMEM((n, cols, rows), BF16),
                pltpu.VMEM((n, width // n, rows), BF16),
                pltpu.VMEM((n, width // n, rows), BF16),
                pltpu.VMEM((n, width // n, rows), BF16),
                pltpu.VMEM((drafts, heads * width), BF16),
                pltpu.VMEM((drafts, heads, width), F32),
                pltpu.VMEM((groups, drafts, model), F32),
                dma((7,)),
            ]
            + [dma((n,))] * 11
            + [dma((groups,))] * 2,
            compiler_params=pltpu.CompilerParams(
                collective_id=0, has_side_effects=True, vmem_limit_bytes=63 * 1024 * 1024
            ),
        )(
            query_nope.reshape(rows, nope),
            query_rope.reshape(rows, rope),
            latent_cache.reshape(positions, latent),
            rope_keys.reshape(rope, positions),
            lengths,
            key_quant.reshape(heads * cols, nope),
            key_scale.T,
            value_quant.reshape(heads * cols, width),
            value_scale.T,
            out_weight.T,
        )
        return result.reshape(batch, drafts, model)

    in_specs = (
        P(None, None, "heads", None),
        P(None, None, "heads", None),
        P(None, "seq", None),
        P(None, None, "seq"),
        P(),
        P("heads", "seq", None),
        P("heads", None),
        P("heads", "seq", None),
        P("heads", None),
        P("heads", "seq"),
    )
    return jax.shard_map(
        per_device, mesh=mesh, in_specs=in_specs, out_specs=P(None, None, "seq"), check_vma=False
    )
```

```python
import functools

import jax
import jax.numpy as jnp
from jax import lax
from jax.experimental import pallas as pl
from jax.experimental.pallas import tpu as pltpu
from jax.sharding import PartitionSpec as P

QB = 128
VMEM_LIMIT = 67043328 - 32768
MESH = pl.DeviceIdType.MESH
neg_large = -1e30
F32 = jnp.float32
BF16 = jnp.bfloat16


def scale_row(scale_ref, block, rows, heads):
    scales = scale_ref[...]
    line = jnp.sum(
        jnp.where(lax.broadcasted_iota(jnp.int32, scales.shape, 0) == block, scales, 0.0),
        axis=0,
        keepdims=True,
    )
    square = (heads, heads)
    diagonal = lax.broadcasted_iota(jnp.int32, square, 0) == lax.broadcasted_iota(jnp.int32, square, 1)
    column = jnp.sum(jnp.where(diagonal, line, 0.0), axis=1, keepdims=True)
    lane_head = lax.broadcasted_iota(jnp.int32, (heads, rows), 1) % heads
    own_head = lax.broadcasted_iota(jnp.int32, (heads, rows), 0)
    return jnp.sum(jnp.where(lane_head == own_head, column, 0.0), axis=0, keepdims=True)


def kernel(
    n,
    groups,
    heads,
    drafts,
    q_hbm,
    qr_hbm,
    cache_hbm,
    rope_hbm,
    len_ref,
    kq_hbm,
    ks_ref,
    vq_hbm,
    vs_ref,
    w_hbm,
    out_ref,
    q,
    qr,
    cache,
    rope,
    kq,
    vq,
    w,
    cache_t,
    vq_t,
    base,
    lat_all,
    stats,
    out_send,
    out_recv,
    part_send,
    part_recv,
    share_all,
    flat,
    heads_out,
    final,
    in_sem,
    lat_send,
    lat_recv,
    pass_send,
    st_send,
    st_recv,
    o_send,
    o_recv,
    p_send,
    p_recv,
    s_send,
    s_recv,
    f_send,
    f_recv,
):
    me = lax.axis_index("seq")
    group = lax.axis_index("heads")
    rows = q.shape[0]
    cols = lat_all.shape[1]
    width = vq.shape[1]
    positions = cache.shape[0]
    factor = (q.shape[1] + qr.shape[1]) ** (-0.5)

    loads = []
    for i, (src, dst) in enumerate(
        ((kq_hbm, kq), (q_hbm, q), (qr_hbm, qr), (rope_hbm, rope), (cache_hbm, cache), (vq_hbm, vq), (w_hbm, w))
    ):
        copy = pltpu.make_async_copy(src, dst, in_sem.at[i])
        if dst is not w:
            copy.start()
        loads.append(copy)
    kq_load, q_load, qr_load, rope_load, cache_load, vq_load, w_load = loads

    barrier = pltpu.get_barrier_semaphore()

    def greet_seq(j, c):
        pl.semaphore_signal(barrier, inc=1, device_id=(group, lax.rem(me + j, n)), device_id_type=MESH)
        return c

    def greet_heads(j, c):
        pl.semaphore_signal(barrier, inc=1, device_id=(lax.rem(group + j, groups), me), device_id_type=MESH)
        return c

    lax.fori_loop(1, n, greet_seq, 0)
    lax.fori_loop(1, groups, greet_heads, 0)

    def spread(src_of, dst, send, recv):
        def make(j):
            peer = lax.rem(me + j, n)
            return pltpu.make_async_remote_copy(
                src_ref=src_of(peer),
                dst_ref=dst.at[me],
                send_sem=send.at[peer],
                recv_sem=recv.at[me],
                device_id=(group, peer),
                device_id_type=MESH,
            )

        def go(j, c):
            make(j).start()
            return c

        lax.fori_loop(1, n, go, 0)

    def arrive(src_of, dst, send, recv):
        def wait(j, c):
            peer = lax.rem(me + j, n)
            pltpu.make_async_remote_copy(
                src_ref=src_of(peer),
                dst_ref=dst.at[peer],
                send_sem=send.at[peer],
                recv_sem=recv.at[peer],
                device_id=(group, peer),
                device_id_type=MESH,
            ).wait_recv()
            return c

        lax.fori_loop(1, n, wait, 0)

    def drain(src_of, dst, send, recv):
        def wait(j, c):
            peer = lax.rem(me + j, n)
            pltpu.make_async_remote_copy(
                src_ref=src_of(peer),
                dst_ref=dst.at[me],
                send_sem=send.at[peer],
                recv_sem=recv.at[me],
                device_id=(group, peer),
                device_id_type=MESH,
            ).wait_send()
            return c

        lax.fori_loop(1, n, wait, 0)

    block = (me * cols) // QB
    lane_head = lax.broadcasted_iota(jnp.int32, (1, rows), 1) % heads
    key_row = scale_row(ks_ref, block, rows, heads)
    value_row = scale_row(vs_ref, block, rows, heads)

    kq_load.wait()
    q_load.wait()
    every = lax.dot_general(kq[...], q[...], (((1,), (1,)), ((), ())), preferred_element_type=F32)
    every = every.reshape(heads, cols, rows)
    own = lax.broadcasted_iota(jnp.int32, (heads, 1, rows), 0) == lane_head[None]
    piece = jnp.sum(jnp.where(own, every, 0.0), axis=0) * key_row
    lat_all[me] = piece.astype(BF16)

    pl.semaphore_wait(barrier, n - 1 + groups - 1)

    partner = me + 1 - 2 * lax.rem(me, 2)

    def lat_copy(slot, peer, send):
        return pltpu.make_async_remote_copy(
            src_ref=lat_all.at[slot],
            dst_ref=lat_all.at[slot],
            send_sem=send,
            recv_sem=lat_recv.at[slot],
            device_id=(group, peer),
            device_id_type=MESH,
        )

    def like(j):
        return lax.rem(me + 2 * j, n)

    def lat_go(j, c):
        lat_copy(me, like(j), lat_send.at[like(j)]).start()
        return c

    def lat_pass(j, c):
        lat_copy(like(j), partner, pass_send.at[like(j)]).wait_recv()
        lat_copy(like(j), partner, pass_send.at[like(j)]).start()
        return c

    def lat_rest(j, c):
        other = lax.rem(partner + 2 * j, n)
        lat_copy(other, partner, pass_send.at[other]).wait_recv()
        return c

    def lat_drain(j, c):
        lat_copy(me, like(j), lat_send.at[like(j)]).wait_send()
        lat_copy(like(j), partner, pass_send.at[like(j)]).wait_send()
        return c

    lax.fori_loop(1, n // 2, lat_go, 0)
    lat_copy(me, partner, lat_send.at[partner]).start()
    w_load.start()

    qr_load.wait()
    rope_load.wait()
    base[...] = lax.dot_general(
        rope[...].T, qr[...], (((1,), (1,)), ((), ())), preferred_element_type=F32
    )
    cache_load.wait()
    cache_t[...] = cache[...].T
    lax.fori_loop(1, n // 2, lat_pass, 0)
    position = me * positions + lax.broadcasted_iota(jnp.int32, (positions, rows), 0)
    horizon = len_ref[0] + lax.broadcasted_iota(jnp.int32, (positions, rows), 1) // heads
    visible = position < horizon

    lax.fori_loop(0, n // 2, lat_rest, 0)
    query_latent = lat_all[...].reshape(n * cols, rows)
    scores = (jnp.dot(cache[...], query_latent, preferred_element_type=F32) + base[...]) * factor
    block_max = jnp.max(jnp.where(visible, scores, neg_large), axis=0, keepdims=True)
    probs = jnp.where(visible, jnp.exp(scores - block_max), 0.0)
    block_sum = jnp.sum(probs, axis=0, keepdims=True)
    stats[me, 0:1, :] = block_max
    stats[me, 1:2, :] = block_sum
    st = (lambda peer: stats.at[me], stats, st_send, st_recv)
    spread(*st)
    block_out = jnp.dot(cache_t[...], probs.astype(BF16), preferred_element_type=F32)
    out_send[...] = block_out.astype(BF16).reshape(n, cols, rows)
    o = (lambda peer: out_send.at[peer], out_recv, o_send, o_recv)
    spread(*o)
    out_recv[me] = out_send[me]
    vq_load.wait()
    vq_t[...] = vq[...].T

    arrive(*st)
    all_max = stats[:, 0:1, :]
    top = jnp.max(all_max, axis=0, keepdims=True)
    weight = jnp.exp(all_max - top)
    total = jnp.sum(weight * stats[:, 1:2, :], axis=0)
    arrive(*o)
    merged = jnp.sum(out_recv[...].astype(F32) * weight, axis=0) / total
    latent = jnp.where(own, merged[None], 0.0).astype(BF16).reshape(heads * cols, rows)
    partial = jnp.dot(vq_t[...], latent, preferred_element_type=F32) * value_row
    step = width // n
    for d in range(n):
        part_send[d] = partial[d * step : (d + 1) * step].astype(part_send.dtype)
    p = (lambda peer: part_send.at[peer], part_recv, p_send, p_recv)
    spread(*p)
    part_recv[me] = part_send[me]
    arrive(*p)
    share_all[me] = jnp.sum(part_recv[...].astype(F32), axis=0).astype(BF16)
    s = (lambda peer: share_all.at[me], share_all, s_send, s_recv)
    spread(*s)
    arrive(*s)
    head_t = jnp.concatenate([share_all[d].astype(F32) for d in range(n)], axis=0)
    heads_out[...] = head_t.T.reshape(drafts, heads, width)
    for k in range(heads):
        flat[:, k * width : (k + 1) * width] = heads_out[:, k, :].astype(BF16)
    w_load.wait()
    final[group] = lax.dot_general(
        flat[...], w[...], (((1,), (1,)), ((), ())), preferred_element_type=F32
    )

    def pair(j, at):
        peer = lax.rem(group + j, groups)
        return pltpu.make_async_remote_copy(
            src_ref=final.at[group],
            dst_ref=final.at[group if at else peer],
            send_sem=f_send.at[peer],
            recv_sem=f_recv.at[group if at else peer],
            device_id=(peer, me),
            device_id_type=MESH,
        )

    for j in range(1, groups):
        pair(j, True).start()
    for j in range(1, groups):
        pair(j, False).wait_recv()
    out_ref[...] = jnp.sum(final[...], axis=0).astype(BF16)
    for each in (st, o, p, s):
        drain(*each)
    lax.fori_loop(1, n // 2, lat_drain, 0)
    lat_copy(me, partner, lat_send.at[partner]).wait_send()
    for j in range(1, groups):
        pair(j, True).wait_send()


def chip_peer(chip, chips, k):
    out = 0
    bit = 1
    while bit < chips:
        own = lax.rem(chip // bit, 2)
        out = out + bit * ((1 - own) if k & bit else own)
        bit *= 2
    return out


def pair_kernel(
    n,
    groups,
    heads,
    drafts,
    q_hbm,
    qr_hbm,
    cache_hbm,
    rope_hbm,
    len_hbm,
    kq_hbm,
    ks_hbm,
    vq_hbm,
    vs_hbm,
    w_hbm,
    out_ref,
    len_ref,
    ks_ref,
    vs_ref,
    q,
    qr,
    cache,
    rope,
    kq,
    vq,
    w,
    q_rows,
    qr_rows,
    cache_t,
    base,
    lat_send,
    lat_all,
    st_send,
    st_all,
    out_send,
    out_recv,
    part_send,
    part_recv,
    share_send,
    share_recv,
    fin_send,
    fin_recv,
    in_sem,
    swap_s,
    swap_r,
    lat_s,
    lat_r,
    st_s,
    st_r,
    o_s,
    o_r,
    p_s,
    p_r,
    s_s,
    s_r,
    f_s,
    f_r,
):
    me = lax.axis_index("seq")
    group = lax.axis_index("heads")
    core = lax.rem(me, 2)
    other = 1 - core
    chip = me // 2
    chips = n // 2
    half = heads // 2
    rows = half * drafts
    cols = lat_all.shape[1]
    wide = 2 * cols
    latent = cache.shape[2]
    positions = cache.shape[1]
    width = vq.shape[2]
    span = half * width
    share = rows // chips
    per = share // drafts
    factor = (q.shape[2] + qr.shape[2]) ** (-0.5)
    far_first = range(chips - 1, -1, -1)
    peers = [chip_peer(chip, chips, k) for k in range(chips)]
    partner = 2 * chip + other
    quarter = chips // 2
    near = chip // quarter

    def local(i, src, dst):
        copy = pltpu.make_async_copy(src, dst, in_sem.at[i])
        copy.start()
        return copy

    q_load = local(0, q_hbm, q)
    kq_loads = [local(1 + b, kq_hbm.at[pl.ds(b * half, half)], kq.at[pl.ds(b * half, half)]) for b in range(2)]

    barrier = pltpu.get_barrier_semaphore()
    for k in far_first:
        for b in range(2):
            if k:
                pl.semaphore_signal(barrier, inc=1, device_id=(group, 2 * peers[k] + b), device_id_type=MESH)
    pl.semaphore_signal(barrier, inc=1, device_id=(group, partner), device_id_type=MESH)
    for j in range(1, groups):
        for b in range(2):
            pl.semaphore_signal(
                barrier, inc=1, device_id=(lax.rem(group + j, groups), 2 * chip + b), device_id_type=MESH
            )

    ks_load = local(8, ks_hbm, ks_ref)
    qr_load = local(3, qr_hbm.at[:, pl.ds(core * half, half)], qr)
    rope_load = local(4, rope_hbm, rope.at[core])
    cache_load = local(5, cache_hbm, cache.at[core])
    vs_load = local(9, vs_hbm, vs_ref)
    len_load = local(10, len_hbm, len_ref)

    def remote(src, dst, send, recv, peer_group, peer):
        return pltpu.make_async_remote_copy(
            src_ref=src,
            dst_ref=dst,
            send_sem=send,
            recv_sem=recv,
            device_id=(peer_group, peer),
            device_id_type=MESH,
        )

    lane = lax.broadcasted_iota(jnp.int32, (1, rows), 1)
    block = (me * cols) // QB

    def scale_line(scale_ref, index):
        scales = scale_ref[...]
        at = lax.broadcasted_iota(jnp.int32, scales.shape, 0) == index
        return jnp.sum(jnp.where(at, scales, 0.0), axis=0, keepdims=True)

    def scale_column(line, count, first, step):
        shape = (count, heads)
        pick = lax.broadcasted_iota(jnp.int32, shape, 1) == lax.broadcasted_iota(jnp.int32, shape, 0) // step + first
        return jnp.sum(jnp.where(pick, line, 0.0), axis=1, keepdims=True)

    ks_load.wait()
    key_column = scale_column(scale_line(ks_ref, block), heads, 0, 1)
    own_head = lax.broadcasted_iota(jnp.int32, (half, rows), 0) == lane // drafts
    key_rows = [
        jnp.sum(jnp.where(own_head, key_column[b * half : (b + 1) * half], 0.0), axis=0, keepdims=True)
        for b in range(2)
    ]

    q_load.wait()
    for b in range(2):
        for t in range(drafts):
            q_rows[b, pl.ds(t, half, stride=drafts), :] = q[t, b * half : (b + 1) * half, :].astype(F32)

    own = lax.broadcasted_iota(jnp.int32, (half, 1, rows), 0) == lane[None] // drafts
    for b in range(2):
        kq_loads[b].wait()
        every = lax.dot_general(
            kq[b * half : (b + 1) * half].reshape(half * cols, kq.shape[2]),
            q_rows[b].astype(BF16),
            (((1,), (1,)), ((), ())),
            preferred_element_type=F32,
        ).reshape(half, cols, rows)
        lat_send[b] = (jnp.sum(jnp.where(own, every, 0.0), axis=0) * key_rows[b]).astype(BF16)
        if b == 0:
            pl.semaphore_wait(barrier, n - 1 + 2 * (groups - 1))
        for k in far_first:
            if k:
                remote(
                    lat_send.at[b], lat_all.at[me], lat_s, lat_r.at[k // quarter], group, 2 * peers[k] + b
                ).start()
    remote(lat_send.at[other], lat_all.at[me], lat_s, lat_r.at[0], group, partner).start()
    lat_all[me] = lat_send[core]

    swaps = [
        remote(src, dst, swap_s.at[i], swap_r.at[i], group, partner)
        for i, (src, dst) in enumerate(
            (
                (rope_hbm, rope.at[core]),
                (cache_hbm, cache.at[core]),
                (vq_hbm.at[pl.ds(core * half, half)], vq.at[:, pl.ds(core * cols, cols)]),
                (w_hbm.at[:, pl.ds(core * span, span)], w.at[core]),
            )
        )
    ]
    swap_arrive = [
        remote(src, dst, swap_s.at[i], swap_r.at[i], group, partner)
        for i, (src, dst) in enumerate(
            (
                (rope_hbm, rope.at[other]),
                (cache_hbm, cache.at[other]),
                (vq_hbm.at[pl.ds(core * half, half)], vq.at[:, pl.ds(other * cols, cols)]),
                (w_hbm.at[:, pl.ds(core * span, span)], w.at[other]),
            )
        )
    ]
    for each in swaps:
        each.start()
    vq_load = local(6, vq_hbm.at[pl.ds(other * half, half)], vq.at[:, pl.ds(core * cols, cols)])
    w_load = local(7, w_hbm.at[:, pl.ds(other * span, span)], w.at[core])

    qr_load.wait()
    for t in range(drafts):
        qr_rows[pl.ds(t, half, stride=drafts), :] = qr[t].astype(F32)
    query_rope = qr_rows[...].astype(BF16)

    def prepare(j):
        turned = lax.dot_general(
            rope[j].T, query_rope, (((1,), (1,)), ((), ())), preferred_element_type=F32
        )
        position = (2 * chip + j) * positions + lax.broadcasted_iota(jnp.int32, (positions, rows), 0)
        horizon = len_ref[0] + lax.rem(lax.broadcasted_iota(jnp.int32, (positions, rows), 1), drafts)
        base[j] = jnp.where(position < horizon, turned * factor, neg_large)
        cache_t[j] = cache[j].T

    vs_load.wait()
    value_column = scale_column(scale_line(vs_ref, block), rows, other * half, drafts)
    len_load.wait()
    rope_load.wait()
    cache_load.wait()
    prepare(core)
    swap_arrive[0].wait_recv()
    swap_arrive[1].wait_recv()
    prepare(other)

    def pieces(ref, count, send, recv):
        some = ref.at[pl.ds(0, count)]
        return remote(some, some, send, recv, group, partner)

    pieces(lat_all, 2 * quarter - 1, lat_s, lat_r.at[0]).wait_recv()

    def part_scores(side):
        begin = pl.multiple_of(side * (latent // 2), latent // 2)
        query = lat_all[pl.ds(side * chips, chips)].reshape(latent // 2, rows)
        return [
            jnp.dot(cache[j, :, pl.ds(begin, latent // 2)], query, preferred_element_type=F32) * factor + base[j]
            for j in range(2)
        ]

    for j, each in enumerate(part_scores(near)):
        base[j] = each
    pieces(lat_all, 2 * quarter, lat_s, lat_r.at[1]).wait_recv()
    scores = part_scores(1 - near)
    block_max = jnp.maximum(
        jnp.max(scores[0], axis=0, keepdims=True), jnp.max(scores[1], axis=0, keepdims=True)
    )
    probs = [jnp.exp(each - block_max) for each in scores]
    st_send[0:1, :] = block_max
    st_send[1:2, :] = jnp.sum(probs[0], axis=0, keepdims=True) + jnp.sum(probs[1], axis=0, keepdims=True)

    def exchange(src_of, dst, send, recv, ks):
        for k in ks:
            remote(src_of(k), dst.at[k], send, recv(k), group, 2 * peers[k] + other).start()

    st = (lambda k: st_send, st_all, st_s, lambda k: st_r)
    exchange(*st, far_first)
    probs = [each.astype(BF16) for each in probs]
    o = (lambda k: out_send.at[peers[k]], out_recv, o_s, lambda k: o_r.at[k // quarter])
    for side, ks in ((1 - near, range(chips - 1, quarter - 1, -1)), (near, range(quarter - 1, -1, -1))):
        begin = pl.multiple_of(side * (latent // 2), latent // 2)
        block_out = sum(
            jnp.dot(cache_t[j, pl.ds(begin, latent // 2), :], probs[j], preferred_element_type=F32)
            for j in range(2)
        )
        out_send[pl.ds(side * quarter, quarter)] = block_out.astype(BF16).reshape(quarter, wide, rows)
        exchange(*o, ks)

    vq_load.wait()
    swap_arrive[2].wait_recv()

    pieces(st_all, chips, st_s, st_r).wait_recv()
    all_max = [st_all[k, 0:1, :] for k in range(chips)]
    top = functools.reduce(jnp.maximum, all_max)
    weight = [jnp.exp(each - top) for each in all_max]
    total = sum(weight[k] * st_all[k, 1:2, :] for k in range(chips))
    merged = jnp.zeros((wide, rows), F32)
    for k in range(chips):
        if k % quarter == 0:
            pieces(out_recv, quarter, o_s, o_r.at[k // quarter]).wait_recv()
        merged = merged + out_recv[k].astype(F32) * weight[k]
    merged = (merged / total).astype(BF16).astype(F32).T
    tile = per * wide
    spread = jnp.concatenate([merged] * per, axis=1)
    keep = (
        lax.broadcasted_iota(jnp.int32, (rows, tile), 1) // wide
        == lax.rem(lax.broadcasted_iota(jnp.int32, (rows, tile), 0) // drafts, per)
    )
    spread = jnp.where(keep, spread, 0.0).astype(BF16)
    for e in range(chips):
        part = jnp.dot(
            spread[e * share : (e + 1) * share],
            vq[e * per : (e + 1) * per].reshape(tile, width),
            preferred_element_type=F32,
        )
        part_send[e] = (part * value_column[e * share : (e + 1) * share]).astype(BF16)
    p = (lambda k: part_send.at[peers[k]], part_recv, p_s, lambda k: p_r)
    exchange(*p, far_first)
    summed = jnp.zeros((share, width), F32)
    pieces(part_recv, chips, p_s, p_r).wait_recv()
    for k in range(chips):
        summed = summed + part_recv[k].astype(F32)
    for h in range(per):
        share_send[:, h * width : (h + 1) * width] = summed[h * drafts : (h + 1) * drafts].astype(BF16)
    s = (lambda k: share_send, share_recv, s_s, lambda k: s_r.at[k])
    exchange(*s, far_first)

    w_load.wait()
    swap_arrive[3].wait_recv()
    model = w.shape[1]
    final = [jnp.zeros((drafts, model), F32) for j in range(2)]
    for k in range(chips):
        pieces(share_recv, 1, s_s, s_r.at[k]).wait_recv()
        begin = pl.multiple_of(peers[k] * (per * width), per * width)
        for j in range(2):
            final[j] = final[j] + lax.dot_general(
                share_recv[k],
                w[j, :, pl.ds(begin, per * width)],
                (((1,), (1,)), ((), ())),
                preferred_element_type=F32,
            )
    for j in range(2):
        fin_send[j] = final[j]

    def last(i, j, b):
        peer_group = lax.rem(group + j, groups)
        side = core if b == 0 else other
        return remote(fin_send.at[side], fin_recv.at[i], f_s, f_r, peer_group, 2 * chip + side)

    lasts = [last(i, j, b) for i, (j, b) in enumerate((j, b) for j in range(groups) for b in range(2) if j or b)]
    for each in lasts[::-1]:
        each.start()
    result = fin_send[core]
    pieces(fin_recv, len(lasts), f_s, f_r).wait_recv()
    for i in range(len(lasts)):
        result = result + fin_recv[i]
    out_ref[...] = result.astype(BF16)

    pieces(lat_all, n - 1, lat_s, lat_r.at[0]).wait_send()
    for ref, send, recv in (
        (st_all, st_s, st_r),
        (out_send, o_s, o_r.at[0]),
        (part_send, p_s, p_r),
        (share_recv, s_s, s_r.at[0]),
        (fin_recv, f_s, f_r),
    ):
        pieces(ref, ref.shape[0], send, recv).wait_send()
    for each in swaps:
        each.wait_send()


def solution(mesh):
    n = mesh.shape["seq"]
    groups = mesh.shape["heads"]

    def paired(query_nope, query_rope, latent_cache, rope_keys, lengths, key_quant, key_scale, value_quant, value_scale, out_weight):
        drafts, heads, nope = query_nope.shape[1:]
        rope = query_rope.shape[-1]
        positions, latent = latent_cache.shape[1:]
        cols = key_quant.shape[1]
        width = value_quant.shape[2]
        model = out_weight.shape[1]
        chips = n // 2
        half = heads // 2
        rows = half * drafts
        share = rows // chips
        wide = 2 * cols
        hbm = pl.BlockSpec(memory_space=pltpu.HBM)
        vmem = pl.BlockSpec(memory_space=pltpu.VMEM)
        dma = pltpu.SemaphoreType.DMA
        lasts = 2 * groups - 1
        result = pl.pallas_call(
            functools.partial(pair_kernel, n, groups, heads, drafts),
            out_shape=pltpu.VMEM((drafts, model), BF16),
            in_specs=[hbm] * 10,
            out_specs=vmem,
            scratch_shapes=[
                pltpu.SMEM(lengths.shape, jnp.int32),
                pltpu.VMEM(key_scale.shape[::-1], F32),
                pltpu.VMEM(value_scale.shape[::-1], F32),
                pltpu.VMEM((drafts, heads, nope), BF16),
                pltpu.VMEM((drafts, half, rope), BF16),
                pltpu.VMEM((2, positions, latent), BF16),
                pltpu.VMEM((2, rope, positions), BF16),
                pltpu.VMEM((heads, cols, nope), BF16),
                pltpu.VMEM((half, wide, width), BF16),
                pltpu.VMEM((2, model, half * width), BF16),
                pltpu.VMEM((2, rows, nope), F32),
                pltpu.VMEM((rows, rope), F32),
                pltpu.VMEM((2, latent, positions), BF16),
                pltpu.VMEM((2, positions, rows), F32),
                pltpu.VMEM((2, cols, rows), BF16),
                pltpu.VMEM((n, cols, rows), BF16),
                pltpu.VMEM((2, rows), F32),
                pltpu.VMEM((chips, 2, rows), F32),
                pltpu.VMEM((chips, wide, rows), BF16),
                pltpu.VMEM((chips, wide, rows), BF16),
                pltpu.VMEM((chips, share, width), BF16),
                pltpu.VMEM((chips, share, width), BF16),
                pltpu.VMEM((drafts, share // drafts * width), BF16),
                pltpu.VMEM((chips, drafts, share // drafts * width), BF16),
                pltpu.VMEM((2, drafts, model), F32),
                pltpu.VMEM((lasts, drafts, model), F32),
                dma((11,)),
                dma((4,)),
                dma((4,)),
                dma,
                dma((2,)),
                dma,
                dma,
                dma,
                dma((2,)),
                dma,
                dma,
                dma,
                dma((chips,)),
                dma,
                dma,
            ],
            compiler_params=pltpu.CompilerParams(
                collective_id=0, has_side_effects=True, vmem_limit_bytes=VMEM_LIMIT
            ),
        )(
            query_nope.reshape(drafts, heads, nope),
            query_rope.reshape(drafts, heads, rope),
            latent_cache.reshape(positions, latent),
            rope_keys.reshape(rope, positions),
            lengths,
            key_quant,
            key_scale.T,
            value_quant,
            value_scale.T,
            out_weight.T,
        )
        return result.reshape(1, drafts, model)

    def per_device(*args):
        drafts, heads = args[0].shape[1:3]
        chips = n // 2
        rows = heads // 2 * drafts
        paired_fits = (
            n % 2 == 0
            and chips & (chips - 1) == 0
            and chips >= 2
            and heads % (2 * chips) == 0
            and rows % 128 == 0
            and args[5].shape[1] % 16 == 0
            and QB % (2 * args[5].shape[1]) == 0
        )
        return (paired if paired_fits else spread_out)(*args)

    def spread_out(
        query_nope,
        query_rope,
        latent_cache,
        rope_keys,
        lengths,
        key_quant,
        key_scale,
        value_quant,
        value_scale,
        out_weight,
    ):
        batch, drafts, heads, nope = query_nope.shape
        rows = batch * drafts * heads
        rope = query_rope.shape[-1]
        positions, latent = latent_cache.shape[1:]
        cols = key_quant.shape[1]
        width = value_quant.shape[2]
        model = out_weight.shape[1]
        hbm = pl.BlockSpec(memory_space=pltpu.HBM)
        vmem = pl.BlockSpec(memory_space=pltpu.VMEM)
        smem = pl.BlockSpec(memory_space=pltpu.SMEM)
        dma = pltpu.SemaphoreType.DMA
        result = pl.pallas_call(
            functools.partial(kernel, n, groups, heads, drafts),
            out_shape=jax.ShapeDtypeStruct((drafts, model), BF16),
            in_specs=[hbm, hbm, hbm, hbm, smem, hbm, vmem, hbm, vmem, hbm],
            out_specs=vmem,
            scratch_shapes=[
                pltpu.VMEM((rows, nope), BF16),
                pltpu.VMEM((rows, rope), BF16),
                pltpu.VMEM((positions, latent), BF16),
                pltpu.VMEM((rope, positions), BF16),
                pltpu.VMEM((heads * cols, nope), BF16),
                pltpu.VMEM((heads * cols, width), BF16),
                pltpu.VMEM(out_weight.shape[::-1], BF16),
                pltpu.VMEM((latent, positions), BF16),
                pltpu.VMEM((width, heads * cols), BF16),
                pltpu.VMEM((positions, rows), F32),
                pltpu.VMEM((n, cols, rows), BF16),
                pltpu.VMEM((n, 2, rows), F32),
                pltpu.VMEM((n, cols, rows), BF16),
                pltpu.VMEM((n, cols, rows), BF16),
                pltpu.VMEM((n, width // n, rows), BF16),
                pltpu.VMEM((n, width // n, rows), BF16),
                pltpu.VMEM((n, width // n, rows), BF16),
                pltpu.VMEM((drafts, heads * width), BF16),
                pltpu.VMEM((drafts, heads, width), F32),
                pltpu.VMEM((groups, drafts, model), F32),
                dma((7,)),
            ]
            + [dma((n,))] * 11
            + [dma((groups,))] * 2,
            compiler_params=pltpu.CompilerParams(
                collective_id=0, has_side_effects=True, vmem_limit_bytes=63 * 1024 * 1024
            ),
        )(
            query_nope.reshape(rows, nope),
            query_rope.reshape(rows, rope),
            latent_cache.reshape(positions, latent),
            rope_keys.reshape(rope, positions),
            lengths,
            key_quant.reshape(heads * cols, nope),
            key_scale.T,
            value_quant.reshape(heads * cols, width),
            value_scale.T,
            out_weight.T,
        )
        return result.reshape(batch, drafts, model)

    in_specs = (
        P(None, None, "heads", None),
        P(None, None, "heads", None),
        P(None, "seq", None),
        P(None, None, "seq"),
        P(),
        P("heads", "seq", None),
        P("heads", None),
        P("heads", "seq", None),
        P("heads", None),
        P("heads", "seq"),
    )
    return jax.shard_map(
        per_device, mesh=mesh, in_specs=in_specs, out_specs=P(None, None, "seq"), check_vma=False
    )
```

```python
import functools

import jax
import jax.numpy as jnp
from jax import lax
from jax.experimental import pallas as pl
from jax.experimental.pallas import tpu as pltpu
from jax.sharding import PartitionSpec as P

QB = 128
VMEM_LIMIT = 67043328 - 32768
MESH = pl.DeviceIdType.MESH
neg_large = -1e30
F32 = jnp.float32
BF16 = jnp.bfloat16


def scale_row(scale_ref, block, rows, heads):
    scales = scale_ref[...]
    line = jnp.sum(
        jnp.where(lax.broadcasted_iota(jnp.int32, scales.shape, 0) == block, scales, 0.0),
        axis=0,
        keepdims=True,
    )
    square = (heads, heads)
    diagonal = lax.broadcasted_iota(jnp.int32, square, 0) == lax.broadcasted_iota(jnp.int32, square, 1)
    column = jnp.sum(jnp.where(diagonal, line, 0.0), axis=1, keepdims=True)
    lane_head = lax.broadcasted_iota(jnp.int32, (heads, rows), 1) % heads
    own_head = lax.broadcasted_iota(jnp.int32, (heads, rows), 0)
    return jnp.sum(jnp.where(lane_head == own_head, column, 0.0), axis=0, keepdims=True)


def kernel(
    n,
    groups,
    heads,
    drafts,
    q_hbm,
    qr_hbm,
    cache_hbm,
    rope_hbm,
    len_ref,
    kq_hbm,
    ks_ref,
    vq_hbm,
    vs_ref,
    w_hbm,
    out_ref,
    q,
    qr,
    cache,
    rope,
    kq,
    vq,
    w,
    cache_t,
    vq_t,
    base,
    lat_all,
    stats,
    out_send,
    out_recv,
    part_send,
    part_recv,
    share_all,
    flat,
    heads_out,
    final,
    in_sem,
    lat_send,
    lat_recv,
    pass_send,
    st_send,
    st_recv,
    o_send,
    o_recv,
    p_send,
    p_recv,
    s_send,
    s_recv,
    f_send,
    f_recv,
):
    me = lax.axis_index("seq")
    group = lax.axis_index("heads")
    rows = q.shape[0]
    cols = lat_all.shape[1]
    width = vq.shape[1]
    positions = cache.shape[0]
    factor = (q.shape[1] + qr.shape[1]) ** (-0.5)

    loads = []
    for i, (src, dst) in enumerate(
        ((kq_hbm, kq), (q_hbm, q), (qr_hbm, qr), (rope_hbm, rope), (cache_hbm, cache), (vq_hbm, vq), (w_hbm, w))
    ):
        copy = pltpu.make_async_copy(src, dst, in_sem.at[i])
        if dst is not w:
            copy.start()
        loads.append(copy)
    kq_load, q_load, qr_load, rope_load, cache_load, vq_load, w_load = loads

    barrier = pltpu.get_barrier_semaphore()

    def greet_seq(j, c):
        pl.semaphore_signal(barrier, inc=1, device_id=(group, lax.rem(me + j, n)), device_id_type=MESH)
        return c

    def greet_heads(j, c):
        pl.semaphore_signal(barrier, inc=1, device_id=(lax.rem(group + j, groups), me), device_id_type=MESH)
        return c

    lax.fori_loop(1, n, greet_seq, 0)
    lax.fori_loop(1, groups, greet_heads, 0)

    def spread(src_of, dst, send, recv):
        def make(j):
            peer = lax.rem(me + j, n)
            return pltpu.make_async_remote_copy(
                src_ref=src_of(peer),
                dst_ref=dst.at[me],
                send_sem=send.at[peer],
                recv_sem=recv.at[me],
                device_id=(group, peer),
                device_id_type=MESH,
            )

        def go(j, c):
            make(j).start()
            return c

        lax.fori_loop(1, n, go, 0)

    def arrive(src_of, dst, send, recv):
        def wait(j, c):
            peer = lax.rem(me + j, n)
            pltpu.make_async_remote_copy(
                src_ref=src_of(peer),
                dst_ref=dst.at[peer],
                send_sem=send.at[peer],
                recv_sem=recv.at[peer],
                device_id=(group, peer),
                device_id_type=MESH,
            ).wait_recv()
            return c

        lax.fori_loop(1, n, wait, 0)

    def drain(src_of, dst, send, recv):
        def wait(j, c):
            peer = lax.rem(me + j, n)
            pltpu.make_async_remote_copy(
                src_ref=src_of(peer),
                dst_ref=dst.at[me],
                send_sem=send.at[peer],
                recv_sem=recv.at[me],
                device_id=(group, peer),
                device_id_type=MESH,
            ).wait_send()
            return c

        lax.fori_loop(1, n, wait, 0)

    block = (me * cols) // QB
    lane_head = lax.broadcasted_iota(jnp.int32, (1, rows), 1) % heads
    key_row = scale_row(ks_ref, block, rows, heads)
    value_row = scale_row(vs_ref, block, rows, heads)

    kq_load.wait()
    q_load.wait()
    every = lax.dot_general(kq[...], q[...], (((1,), (1,)), ((), ())), preferred_element_type=F32)
    every = every.reshape(heads, cols, rows)
    own = lax.broadcasted_iota(jnp.int32, (heads, 1, rows), 0) == lane_head[None]
    piece = jnp.sum(jnp.where(own, every, 0.0), axis=0) * key_row
    lat_all[me] = piece.astype(BF16)

    pl.semaphore_wait(barrier, n - 1 + groups - 1)

    partner = me + 1 - 2 * lax.rem(me, 2)

    def lat_copy(slot, peer, send):
        return pltpu.make_async_remote_copy(
            src_ref=lat_all.at[slot],
            dst_ref=lat_all.at[slot],
            send_sem=send,
            recv_sem=lat_recv.at[slot],
            device_id=(group, peer),
            device_id_type=MESH,
        )

    def like(j):
        return lax.rem(me + 2 * j, n)

    def lat_go(j, c):
        lat_copy(me, like(j), lat_send.at[like(j)]).start()
        return c

    def lat_pass(j, c):
        lat_copy(like(j), partner, pass_send.at[like(j)]).wait_recv()
        lat_copy(like(j), partner, pass_send.at[like(j)]).start()
        return c

    def lat_rest(j, c):
        other = lax.rem(partner + 2 * j, n)
        lat_copy(other, partner, pass_send.at[other]).wait_recv()
        return c

    def lat_drain(j, c):
        lat_copy(me, like(j), lat_send.at[like(j)]).wait_send()
        lat_copy(like(j), partner, pass_send.at[like(j)]).wait_send()
        return c

    lax.fori_loop(1, n // 2, lat_go, 0)
    lat_copy(me, partner, lat_send.at[partner]).start()
    w_load.start()

    qr_load.wait()
    rope_load.wait()
    base[...] = lax.dot_general(
        rope[...].T, qr[...], (((1,), (1,)), ((), ())), preferred_element_type=F32
    )
    cache_load.wait()
    cache_t[...] = cache[...].T
    lax.fori_loop(1, n // 2, lat_pass, 0)
    position = me * positions + lax.broadcasted_iota(jnp.int32, (positions, rows), 0)
    horizon = len_ref[0] + lax.broadcasted_iota(jnp.int32, (positions, rows), 1) // heads
    visible = position < horizon

    lax.fori_loop(0, n // 2, lat_rest, 0)
    query_latent = lat_all[...].reshape(n * cols, rows)
    scores = (jnp.dot(cache[...], query_latent, preferred_element_type=F32) + base[...]) * factor
    block_max = jnp.max(jnp.where(visible, scores, neg_large), axis=0, keepdims=True)
    probs = jnp.where(visible, jnp.exp(scores - block_max), 0.0)
    block_sum = jnp.sum(probs, axis=0, keepdims=True)
    stats[me, 0:1, :] = block_max
    stats[me, 1:2, :] = block_sum
    st = (lambda peer: stats.at[me], stats, st_send, st_recv)
    spread(*st)
    block_out = jnp.dot(cache_t[...], probs.astype(BF16), preferred_element_type=F32)
    out_send[...] = block_out.astype(BF16).reshape(n, cols, rows)
    o = (lambda peer: out_send.at[peer], out_recv, o_send, o_recv)
    spread(*o)
    out_recv[me] = out_send[me]
    vq_load.wait()
    vq_t[...] = vq[...].T

    arrive(*st)
    all_max = stats[:, 0:1, :]
    top = jnp.max(all_max, axis=0, keepdims=True)
    weight = jnp.exp(all_max - top)
    total = jnp.sum(weight * stats[:, 1:2, :], axis=0)
    arrive(*o)
    merged = jnp.sum(out_recv[...].astype(F32) * weight, axis=0) / total
    latent = jnp.where(own, merged[None], 0.0).astype(BF16).reshape(heads * cols, rows)
    partial = jnp.dot(vq_t[...], latent, preferred_element_type=F32) * value_row
    step = width // n
    for d in range(n):
        part_send[d] = partial[d * step : (d + 1) * step].astype(part_send.dtype)
    p = (lambda peer: part_send.at[peer], part_recv, p_send, p_recv)
    spread(*p)
    part_recv[me] = part_send[me]
    arrive(*p)
    share_all[me] = jnp.sum(part_recv[...].astype(F32), axis=0).astype(BF16)
    s = (lambda peer: share_all.at[me], share_all, s_send, s_recv)
    spread(*s)
    arrive(*s)
    head_t = jnp.concatenate([share_all[d].astype(F32) for d in range(n)], axis=0)
    heads_out[...] = head_t.T.reshape(drafts, heads, width)
    for k in range(heads):
        flat[:, k * width : (k + 1) * width] = heads_out[:, k, :].astype(BF16)
    w_load.wait()
    final[group] = lax.dot_general(
        flat[...], w[...], (((1,), (1,)), ((), ())), preferred_element_type=F32
    )

    def pair(j, at):
        peer = lax.rem(group + j, groups)
        return pltpu.make_async_remote_copy(
            src_ref=final.at[group],
            dst_ref=final.at[group if at else peer],
            send_sem=f_send.at[peer],
            recv_sem=f_recv.at[group if at else peer],
            device_id=(peer, me),
            device_id_type=MESH,
        )

    for j in range(1, groups):
        pair(j, True).start()
    for j in range(1, groups):
        pair(j, False).wait_recv()
    out_ref[...] = jnp.sum(final[...], axis=0).astype(BF16)
    for each in (st, o, p, s):
        drain(*each)
    lax.fori_loop(1, n // 2, lat_drain, 0)
    lat_copy(me, partner, lat_send.at[partner]).wait_send()
    for j in range(1, groups):
        pair(j, True).wait_send()


def chip_peer(chip, chips, k):
    out = 0
    bit = 1
    while bit < chips:
        own = lax.rem(chip // bit, 2)
        out = out + bit * ((1 - own) if k & bit else own)
        bit *= 2
    return out


def pair_kernel(
    n,
    groups,
    heads,
    drafts,
    q_hbm,
    qr_hbm,
    cache_hbm,
    rope_hbm,
    len_hbm,
    kq_hbm,
    ks_hbm,
    vq_hbm,
    vs_hbm,
    w_hbm,
    out_ref,
    len_ref,
    ks_ref,
    vs_ref,
    q,
    qr,
    cache,
    rope,
    kq,
    vq,
    w,
    q_rows,
    qr_rows,
    cache_t,
    base,
    lat_send,
    lat_all,
    st_send,
    st_all,
    out_send,
    out_recv,
    part_send,
    part_recv,
    weights,
    share_send,
    share_recv,
    fin_send,
    fin_recv,
    in_sem,
    swap_s,
    swap_r,
    lat_s,
    lat_r,
    st_s,
    st_r,
    o_s,
    o_r,
    p_s,
    p_r,
    s_s,
    s_r,
    v_s,
    v_r,
    f_s,
    f_r,
):
    me = lax.axis_index("seq")
    group = lax.axis_index("heads")
    core = lax.rem(me, 2)
    other = 1 - core
    chip = me // 2
    chips = n // 2
    half = heads // 2
    rows = half * drafts
    cols = lat_all.shape[1]
    wide = 2 * cols
    latent = cache.shape[2]
    positions = cache.shape[1]
    width = vq.shape[2]
    span = half * width
    factor = (q.shape[2] + qr.shape[2]) ** (-0.5)
    far_first = range(chips - 1, -1, -1)
    peers = [chip_peer(chip, chips, k) for k in range(chips)]
    partner = 2 * chip + other
    quarter = chips // 2
    near = chip // quarter
    place = lax.rem(chip, quarter)
    per = half // quarter
    share = per * drafts

    def local(i, src, dst):
        copy = pltpu.make_async_copy(src, dst, in_sem.at[i])
        copy.start()
        return copy

    q_load = local(0, q_hbm, q)
    kq_loads = [local(1 + b, kq_hbm.at[pl.ds(b * half, half)], kq.at[pl.ds(b * half, half)]) for b in range(2)]

    barrier = pltpu.get_barrier_semaphore()
    for k in far_first:
        for b in range(2):
            if k:
                pl.semaphore_signal(barrier, inc=1, device_id=(group, 2 * peers[k] + b), device_id_type=MESH)
    pl.semaphore_signal(barrier, inc=1, device_id=(group, partner), device_id_type=MESH)
    for j in range(1, groups):
        for b in range(2):
            pl.semaphore_signal(
                barrier, inc=1, device_id=(lax.rem(group + j, groups), 2 * chip + b), device_id_type=MESH
            )

    ks_load = local(8, ks_hbm, ks_ref)
    qr_load = local(3, qr_hbm.at[:, pl.ds(core * half, half)], qr)
    rope_load = local(4, rope_hbm, rope.at[core])
    cache_load = local(5, cache_hbm, cache.at[core])
    vs_load = local(9, vs_hbm, vs_ref)
    len_load = local(10, len_hbm, len_ref)

    def remote(src, dst, send, recv, peer_group, peer):
        return pltpu.make_async_remote_copy(
            src_ref=src,
            dst_ref=dst,
            send_sem=send,
            recv_sem=recv,
            device_id=(peer_group, peer),
            device_id_type=MESH,
        )

    lane = lax.broadcasted_iota(jnp.int32, (1, rows), 1)
    block = (me * cols) // QB

    def scale_line(scale_ref, index):
        scales = scale_ref[...]
        at = lax.broadcasted_iota(jnp.int32, scales.shape, 0) == index
        return jnp.sum(jnp.where(at, scales, 0.0), axis=0, keepdims=True)

    def scale_column(line, count, first, step):
        shape = (count, heads)
        pick = lax.broadcasted_iota(jnp.int32, shape, 1) == lax.broadcasted_iota(jnp.int32, shape, 0) // step + first
        return jnp.sum(jnp.where(pick, line, 0.0), axis=1, keepdims=True)

    ks_load.wait()
    key_column = scale_column(scale_line(ks_ref, block), heads, 0, 1)
    own_head = lax.broadcasted_iota(jnp.int32, (half, rows), 0) == lane // drafts
    key_rows = [
        jnp.sum(jnp.where(own_head, key_column[b * half : (b + 1) * half], 0.0), axis=0, keepdims=True)
        for b in range(2)
    ]

    q_load.wait()
    for b in range(2):
        for t in range(drafts):
            q_rows[b, pl.ds(t, half, stride=drafts), :] = q[t, b * half : (b + 1) * half, :].astype(F32)

    own = lax.broadcasted_iota(jnp.int32, (half, 1, rows), 0) == lane[None] // drafts
    for b in range(2):
        kq_loads[b].wait()
        every = lax.dot_general(
            kq[b * half : (b + 1) * half].reshape(half * cols, kq.shape[2]),
            q_rows[b].astype(BF16),
            (((1,), (1,)), ((), ())),
            preferred_element_type=F32,
        ).reshape(half, cols, rows)
        lat_send[b] = (jnp.sum(jnp.where(own, every, 0.0), axis=0) * key_rows[b]).astype(BF16)
        if b == 0:
            pl.semaphore_wait(barrier, n - 1 + 2 * (groups - 1))
        for k in far_first:
            if k:
                remote(
                    lat_send.at[b], lat_all.at[me], lat_s, lat_r.at[k // quarter], group, 2 * peers[k] + b
                ).start()
    remote(lat_send.at[other], lat_all.at[me], lat_s, lat_r.at[0], group, partner).start()
    lat_all[me] = lat_send[core]

    swaps = [
        remote(src, dst, swap_s.at[i], swap_r.at[i], group, partner)
        for i, (src, dst) in enumerate(
            (
                (rope_hbm, rope.at[core]),
                (cache_hbm, cache.at[core]),
                (w_hbm.at[:, pl.ds(core * span, span)], w.at[core]),
            )
        )
    ]
    swap_arrive = [
        remote(src, dst, swap_s.at[i], swap_r.at[i], group, partner)
        for i, (src, dst) in enumerate(
            (
                (rope_hbm, rope.at[other]),
                (cache_hbm, cache.at[other]),
                (w_hbm.at[:, pl.ds(core * span, span)], w.at[other]),
            )
        )
    ]
    for each in swaps:
        each.start()
    w_load = local(7, w_hbm.at[:, pl.ds(other * span, span)], w.at[core])

    qr_load.wait()
    for t in range(drafts):
        qr_rows[pl.ds(t, half, stride=drafts), :] = qr[t].astype(F32)
    query_rope = qr_rows[...].astype(BF16)

    def prepare(j):
        turned = lax.dot_general(
            rope[j].T, query_rope, (((1,), (1,)), ((), ())), preferred_element_type=F32
        )
        position = (2 * chip + j) * positions + lax.broadcasted_iota(jnp.int32, (positions, rows), 0)
        horizon = len_ref[0] + lax.rem(lax.broadcasted_iota(jnp.int32, (positions, rows), 1), drafts)
        base[j] = jnp.where(position < horizon, turned * factor, neg_large)
        cache_t[j] = cache[j].T

    vs_load.wait()
    blocks = latent // 2 // QB
    value_scale = jnp.concatenate(
        [
            jnp.broadcast_to(
                scale_column(
                    scale_line(vs_ref, near * blocks + i), share, other * half + place * per, drafts
                ),
                (share, QB),
            )
            for i in range(blocks)
        ],
        axis=1,
    )
    len_load.wait()
    vq_slot = vq.at[:, pl.ds(place * wide + core * cols, cols)]

    def vq_part(side, at):
        return vq_hbm.at[pl.ds(side * half + at * per, per)]

    vq_load = local(6, vq_part(other, place), vq_slot)
    for k in range(quarter - 1, -1, -1):
        for b in range(2) if k else (other,):
            remote(
                vq_part(1 - b, lax.rem(peers[k], quarter)), vq_slot, v_s, v_r, group, 2 * peers[k] + b
            ).start()

    rope_load.wait()
    cache_load.wait()
    prepare(core)
    swap_arrive[0].wait_recv()
    swap_arrive[1].wait_recv()
    prepare(other)

    def pieces(ref, count, send, recv):
        some = ref.at[pl.ds(0, count)]
        return remote(some, some, send, recv, group, partner)

    pieces(lat_all, 2 * quarter - 1, lat_s, lat_r.at[0]).wait_recv()

    def part_scores(side):
        begin = pl.multiple_of(side * (latent // 2), latent // 2)
        query = lat_all[pl.ds(side * chips, chips)].reshape(latent // 2, rows)
        return [
            jnp.dot(cache[j, :, pl.ds(begin, latent // 2)], query, preferred_element_type=F32) * factor + base[j]
            for j in range(2)
        ]

    for j, each in enumerate(part_scores(near)):
        base[j] = each
    pieces(lat_all, 2 * quarter, lat_s, lat_r.at[1]).wait_recv()
    scores = part_scores(1 - near)
    block_max = jnp.maximum(
        jnp.max(scores[0], axis=0, keepdims=True), jnp.max(scores[1], axis=0, keepdims=True)
    )
    probs = [jnp.exp(each - block_max) for each in scores]
    st_send[0:1, :] = block_max
    st_send[1:2, :] = jnp.sum(probs[0], axis=0, keepdims=True) + jnp.sum(probs[1], axis=0, keepdims=True)

    def exchange(src_of, dst, send, recv, ks):
        for k in ks:
            remote(src_of(k), dst.at[k], send, recv(k), group, 2 * peers[k] + other).start()

    st = (lambda k: st_send, st_all, st_s, lambda k: st_r)
    exchange(*st, far_first)
    probs = [each.astype(BF16) for each in probs]
    o = (lambda k: out_send.at[peers[k]], out_recv, o_s, lambda k: o_r.at[k // quarter])
    for side, ks in ((1 - near, range(chips - 1, quarter - 1, -1)), (near, range(quarter - 1, -1, -1))):
        begin = pl.multiple_of(side * (latent // 2), latent // 2)
        block_out = sum(
            jnp.dot(cache_t[j, pl.ds(begin, latent // 2), :], probs[j], preferred_element_type=F32)
            for j in range(2)
        )
        out_send[pl.ds(side * quarter, quarter)] = block_out.T.astype(BF16).reshape(quarter, share, latent // 2)
        exchange(*o, ks)

    vq_load.wait()
    vq_rest = vq.at[:, pl.ds(0, (2 * quarter - 1) * cols)]
    vq_swap = remote(vq_rest, vq_rest, v_s, v_r, group, partner)
    vq_swap.wait_recv()

    pieces(st_all, chips, st_s, st_r).wait_recv()
    all_max = [st_all[k, 0:1, :] for k in range(chips)]
    top = functools.reduce(jnp.maximum, all_max)
    weight = [jnp.exp(each - top) for each in all_max]
    total = sum(weight[k] * st_all[k, 1:2, :] for k in range(chips))
    weights[...] = jnp.concatenate([each / total for each in weight], axis=0).T
    weight = weights[pl.ds(place * share, share), :]
    merged = jnp.zeros((share, latent // 2), F32)
    for k in range(chips):
        if k % quarter == 0:
            pieces(out_recv, quarter, o_s, o_r.at[k // quarter]).wait_recv()
        merged = merged + out_recv[k].astype(F32) * weight[:, k : k + 1]
    merged = (merged * value_scale).astype(BF16)
    row_head = lax.broadcasted_iota(jnp.int32, (share, width), 0) // drafts
    part = jnp.zeros((share, width), F32)
    for h in range(per):
        part = jnp.where(row_head == h, jnp.dot(merged, vq[h], preferred_element_type=F32), part)
    part_send[...] = part.astype(BF16)
    for i, k in ((1, quarter), (0, 0)):
        remote(part_send, part_recv.at[i], p_s, p_r, group, 2 * peers[k] + other).start()
    pieces(part_recv, 2, p_s, p_r).wait_recv()
    summed = part_recv[0].astype(F32) + part_recv[1].astype(F32)
    for h in range(per):
        share_send[:, h * width : (h + 1) * width] = summed[h * drafts : (h + 1) * drafts].astype(BF16)
    s = (lambda k: share_send, share_recv, s_s, lambda k: s_r.at[k])
    exchange(*s, range(quarter - 1, -1, -1))

    w_load.wait()
    swap_arrive[2].wait_recv()
    model = w.shape[1]
    final = [jnp.zeros((drafts, model), F32) for j in range(2)]
    for k in range(quarter):
        pieces(share_recv, 1, s_s, s_r.at[k]).wait_recv()
        begin = pl.multiple_of(lax.rem(peers[k], quarter) * (per * width), per * width)
        for j in range(2):
            final[j] = final[j] + lax.dot_general(
                share_recv[k],
                w[j, :, pl.ds(begin, per * width)],
                (((1,), (1,)), ((), ())),
                preferred_element_type=F32,
            )
    for j in range(2):
        fin_send[j] = final[j]

    def last(i, j, b):
        peer_group = lax.rem(group + j, groups)
        side = core if b == 0 else other
        return remote(fin_send.at[side], fin_recv.at[i], f_s, f_r, peer_group, 2 * chip + side)

    lasts = [last(i, j, b) for i, (j, b) in enumerate((j, b) for j in range(groups) for b in range(2) if j or b)]
    for each in lasts[::-1]:
        each.start()
    result = fin_send[core]
    pieces(fin_recv, len(lasts), f_s, f_r).wait_recv()
    for i in range(len(lasts)):
        result = result + fin_recv[i]
    out_ref[...] = result.astype(BF16)

    pieces(lat_all, n - 1, lat_s, lat_r.at[0]).wait_send()
    for ref, send, recv in (
        (st_all, st_s, st_r),
        (out_send, o_s, o_r.at[0]),
        (part_recv, p_s, p_r),
        (share_recv, s_s, s_r.at[0]),
        (fin_recv, f_s, f_r),
    ):
        pieces(ref, ref.shape[0], send, recv).wait_send()
    vq_swap.wait_send()
    for each in swaps:
        each.wait_send()


def solution(mesh):
    n = mesh.shape["seq"]
    groups = mesh.shape["heads"]

    def paired(query_nope, query_rope, latent_cache, rope_keys, lengths, key_quant, key_scale, value_quant, value_scale, out_weight):
        drafts, heads, nope = query_nope.shape[1:]
        rope = query_rope.shape[-1]
        positions, latent = latent_cache.shape[1:]
        cols = key_quant.shape[1]
        width = value_quant.shape[2]
        model = out_weight.shape[1]
        chips = n // 2
        half = heads // 2
        rows = half * drafts
        quarter = chips // 2
        per = half // quarter
        share = per * drafts
        hbm = pl.BlockSpec(memory_space=pltpu.HBM)
        vmem = pl.BlockSpec(memory_space=pltpu.VMEM)
        dma = pltpu.SemaphoreType.DMA
        lasts = 2 * groups - 1
        result = pl.pallas_call(
            functools.partial(pair_kernel, n, groups, heads, drafts),
            out_shape=pltpu.VMEM((drafts, model), BF16),
            in_specs=[hbm] * 10,
            out_specs=vmem,
            scratch_shapes=[
                pltpu.SMEM(lengths.shape, jnp.int32),
                pltpu.VMEM(key_scale.shape[::-1], F32),
                pltpu.VMEM(value_scale.shape[::-1], F32),
                pltpu.VMEM((drafts, heads, nope), BF16),
                pltpu.VMEM((drafts, half, rope), BF16),
                pltpu.VMEM((2, positions, latent), BF16),
                pltpu.VMEM((2, rope, positions), BF16),
                pltpu.VMEM((heads, cols, nope), BF16),
                pltpu.VMEM((per, latent // 2, width), BF16),
                pltpu.VMEM((2, model, half * width), BF16),
                pltpu.VMEM((2, rows, nope), F32),
                pltpu.VMEM((rows, rope), F32),
                pltpu.VMEM((2, latent, positions), BF16),
                pltpu.VMEM((2, positions, rows), F32),
                pltpu.VMEM((2, cols, rows), BF16),
                pltpu.VMEM((n, cols, rows), BF16),
                pltpu.VMEM((2, rows), F32),
                pltpu.VMEM((chips, 2, rows), F32),
                pltpu.VMEM((chips, share, latent // 2), BF16),
                pltpu.VMEM((chips, share, latent // 2), BF16),
                pltpu.VMEM((share, width), BF16),
                pltpu.VMEM((2, share, width), BF16),
                pltpu.VMEM((rows, chips), F32),
                pltpu.VMEM((drafts, per * width), BF16),
                pltpu.VMEM((quarter, drafts, per * width), BF16),
                pltpu.VMEM((2, drafts, model), F32),
                pltpu.VMEM((lasts, drafts, model), F32),
                dma((11,)),
                dma((3,)),
                dma((3,)),
                dma,
                dma((2,)),
                dma,
                dma,
                dma,
                dma((2,)),
                dma,
                dma,
                dma,
                dma((quarter,)),
                dma,
                dma,
                dma,
                dma,
            ],
            compiler_params=pltpu.CompilerParams(
                collective_id=0, has_side_effects=True, vmem_limit_bytes=VMEM_LIMIT
            ),
        )(
            query_nope.reshape(drafts, heads, nope),
            query_rope.reshape(drafts, heads, rope),
            latent_cache.reshape(positions, latent),
            rope_keys.reshape(rope, positions),
            lengths,
            key_quant,
            key_scale.T,
            value_quant,
            value_scale.T,
            out_weight.T,
        )
        return result.reshape(1, drafts, model)

    def per_device(*args):
        drafts, heads = args[0].shape[1:3]
        chips = n // 2
        rows = heads // 2 * drafts
        paired_fits = (
            n % 2 == 0
            and chips & (chips - 1) == 0
            and chips >= 2
            and heads % chips == 0
            and heads // chips * drafts % 16 == 0
            and args[2].shape[2] % (2 * QB) == 0
            and rows % 128 == 0
            and args[5].shape[1] % 16 == 0
            and QB % args[5].shape[1] == 0
        )
        return (paired if paired_fits else spread_out)(*args)

    def spread_out(
        query_nope,
        query_rope,
        latent_cache,
        rope_keys,
        lengths,
        key_quant,
        key_scale,
        value_quant,
        value_scale,
        out_weight,
    ):
        batch, drafts, heads, nope = query_nope.shape
        rows = batch * drafts * heads
        rope = query_rope.shape[-1]
        positions, latent = latent_cache.shape[1:]
        cols = key_quant.shape[1]
        width = value_quant.shape[2]
        model = out_weight.shape[1]
        hbm = pl.BlockSpec(memory_space=pltpu.HBM)
        vmem = pl.BlockSpec(memory_space=pltpu.VMEM)
        smem = pl.BlockSpec(memory_space=pltpu.SMEM)
        dma = pltpu.SemaphoreType.DMA
        result = pl.pallas_call(
            functools.partial(kernel, n, groups, heads, drafts),
            out_shape=jax.ShapeDtypeStruct((drafts, model), BF16),
            in_specs=[hbm, hbm, hbm, hbm, smem, hbm, vmem, hbm, vmem, hbm],
            out_specs=vmem,
            scratch_shapes=[
                pltpu.VMEM((rows, nope), BF16),
                pltpu.VMEM((rows, rope), BF16),
                pltpu.VMEM((positions, latent), BF16),
                pltpu.VMEM((rope, positions), BF16),
                pltpu.VMEM((heads * cols, nope), BF16),
                pltpu.VMEM((heads * cols, width), BF16),
                pltpu.VMEM(out_weight.shape[::-1], BF16),
                pltpu.VMEM((latent, positions), BF16),
                pltpu.VMEM((width, heads * cols), BF16),
                pltpu.VMEM((positions, rows), F32),
                pltpu.VMEM((n, cols, rows), BF16),
                pltpu.VMEM((n, 2, rows), F32),
                pltpu.VMEM((n, cols, rows), BF16),
                pltpu.VMEM((n, cols, rows), BF16),
                pltpu.VMEM((n, width // n, rows), BF16),
                pltpu.VMEM((n, width // n, rows), BF16),
                pltpu.VMEM((n, width // n, rows), BF16),
                pltpu.VMEM((drafts, heads * width), BF16),
                pltpu.VMEM((drafts, heads, width), F32),
                pltpu.VMEM((groups, drafts, model), F32),
                dma((7,)),
            ]
            + [dma((n,))] * 11
            + [dma((groups,))] * 2,
            compiler_params=pltpu.CompilerParams(
                collective_id=0, has_side_effects=True, vmem_limit_bytes=63 * 1024 * 1024
            ),
        )(
            query_nope.reshape(rows, nope),
            query_rope.reshape(rows, rope),
            latent_cache.reshape(positions, latent),
            rope_keys.reshape(rope, positions),
            lengths,
            key_quant.reshape(heads * cols, nope),
            key_scale.T,
            value_quant.reshape(heads * cols, width),
            value_scale.T,
            out_weight.T,
        )
        return result.reshape(batch, drafts, model)

    in_specs = (
        P(None, None, "heads", None),
        P(None, None, "heads", None),
        P(None, "seq", None),
        P(None, None, "seq"),
        P(),
        P("heads", "seq", None),
        P("heads", None),
        P("heads", "seq", None),
        P("heads", None),
        P("heads", "seq"),
    )
    return jax.shard_map(
        per_device, mesh=mesh, in_specs=in_specs, out_specs=P(None, None, "seq"), check_vma=False
    )
```

```python
import functools

import jax
import jax.numpy as jnp
from jax import lax
from jax.experimental import pallas as pl
from jax.experimental.pallas import tpu as pltpu
from jax.sharding import PartitionSpec as P

QB = 128
VMEM_LIMIT = 67043328 - 32768
MESH = pl.DeviceIdType.MESH
neg_large = -1e30
F32 = jnp.float32
BF16 = jnp.bfloat16


def scale_row(scale_ref, block, rows, heads):
    scales = scale_ref[...]
    line = jnp.sum(
        jnp.where(lax.broadcasted_iota(jnp.int32, scales.shape, 0) == block, scales, 0.0),
        axis=0,
        keepdims=True,
    )
    square = (heads, heads)
    diagonal = lax.broadcasted_iota(jnp.int32, square, 0) == lax.broadcasted_iota(jnp.int32, square, 1)
    column = jnp.sum(jnp.where(diagonal, line, 0.0), axis=1, keepdims=True)
    lane_head = lax.broadcasted_iota(jnp.int32, (heads, rows), 1) % heads
    own_head = lax.broadcasted_iota(jnp.int32, (heads, rows), 0)
    return jnp.sum(jnp.where(lane_head == own_head, column, 0.0), axis=0, keepdims=True)


def kernel(
    n,
    groups,
    heads,
    drafts,
    q_hbm,
    qr_hbm,
    cache_hbm,
    rope_hbm,
    len_ref,
    kq_hbm,
    ks_ref,
    vq_hbm,
    vs_ref,
    w_hbm,
    out_ref,
    q,
    qr,
    cache,
    rope,
    kq,
    vq,
    w,
    cache_t,
    vq_t,
    base,
    lat_all,
    stats,
    out_send,
    out_recv,
    part_send,
    part_recv,
    share_all,
    flat,
    heads_out,
    final,
    in_sem,
    lat_send,
    lat_recv,
    pass_send,
    st_send,
    st_recv,
    o_send,
    o_recv,
    p_send,
    p_recv,
    s_send,
    s_recv,
    f_send,
    f_recv,
):
    me = lax.axis_index("seq")
    group = lax.axis_index("heads")
    rows = q.shape[0]
    cols = lat_all.shape[1]
    width = vq.shape[1]
    positions = cache.shape[0]
    factor = (q.shape[1] + qr.shape[1]) ** (-0.5)

    loads = []
    for i, (src, dst) in enumerate(
        ((kq_hbm, kq), (q_hbm, q), (qr_hbm, qr), (rope_hbm, rope), (cache_hbm, cache), (vq_hbm, vq), (w_hbm, w))
    ):
        copy = pltpu.make_async_copy(src, dst, in_sem.at[i])
        if dst is not w:
            copy.start()
        loads.append(copy)
    kq_load, q_load, qr_load, rope_load, cache_load, vq_load, w_load = loads

    barrier = pltpu.get_barrier_semaphore()

    def greet_seq(j, c):
        pl.semaphore_signal(barrier, inc=1, device_id=(group, lax.rem(me + j, n)), device_id_type=MESH)
        return c

    def greet_heads(j, c):
        pl.semaphore_signal(barrier, inc=1, device_id=(lax.rem(group + j, groups), me), device_id_type=MESH)
        return c

    lax.fori_loop(1, n, greet_seq, 0)
    lax.fori_loop(1, groups, greet_heads, 0)

    def spread(src_of, dst, send, recv):
        def make(j):
            peer = lax.rem(me + j, n)
            return pltpu.make_async_remote_copy(
                src_ref=src_of(peer),
                dst_ref=dst.at[me],
                send_sem=send.at[peer],
                recv_sem=recv.at[me],
                device_id=(group, peer),
                device_id_type=MESH,
            )

        def go(j, c):
            make(j).start()
            return c

        lax.fori_loop(1, n, go, 0)

    def arrive(src_of, dst, send, recv):
        def wait(j, c):
            peer = lax.rem(me + j, n)
            pltpu.make_async_remote_copy(
                src_ref=src_of(peer),
                dst_ref=dst.at[peer],
                send_sem=send.at[peer],
                recv_sem=recv.at[peer],
                device_id=(group, peer),
                device_id_type=MESH,
            ).wait_recv()
            return c

        lax.fori_loop(1, n, wait, 0)

    def drain(src_of, dst, send, recv):
        def wait(j, c):
            peer = lax.rem(me + j, n)
            pltpu.make_async_remote_copy(
                src_ref=src_of(peer),
                dst_ref=dst.at[me],
                send_sem=send.at[peer],
                recv_sem=recv.at[me],
                device_id=(group, peer),
                device_id_type=MESH,
            ).wait_send()
            return c

        lax.fori_loop(1, n, wait, 0)

    block = (me * cols) // QB
    lane_head = lax.broadcasted_iota(jnp.int32, (1, rows), 1) % heads
    key_row = scale_row(ks_ref, block, rows, heads)
    value_row = scale_row(vs_ref, block, rows, heads)

    kq_load.wait()
    q_load.wait()
    every = lax.dot_general(kq[...], q[...], (((1,), (1,)), ((), ())), preferred_element_type=F32)
    every = every.reshape(heads, cols, rows)
    own = lax.broadcasted_iota(jnp.int32, (heads, 1, rows), 0) == lane_head[None]
    piece = jnp.sum(jnp.where(own, every, 0.0), axis=0) * key_row
    lat_all[me] = piece.astype(BF16)

    pl.semaphore_wait(barrier, n - 1 + groups - 1)

    partner = me + 1 - 2 * lax.rem(me, 2)

    def lat_copy(slot, peer, send):
        return pltpu.make_async_remote_copy(
            src_ref=lat_all.at[slot],
            dst_ref=lat_all.at[slot],
            send_sem=send,
            recv_sem=lat_recv.at[slot],
            device_id=(group, peer),
            device_id_type=MESH,
        )

    def like(j):
        return lax.rem(me + 2 * j, n)

    def lat_go(j, c):
        lat_copy(me, like(j), lat_send.at[like(j)]).start()
        return c

    def lat_pass(j, c):
        lat_copy(like(j), partner, pass_send.at[like(j)]).wait_recv()
        lat_copy(like(j), partner, pass_send.at[like(j)]).start()
        return c

    def lat_rest(j, c):
        other = lax.rem(partner + 2 * j, n)
        lat_copy(other, partner, pass_send.at[other]).wait_recv()
        return c

    def lat_drain(j, c):
        lat_copy(me, like(j), lat_send.at[like(j)]).wait_send()
        lat_copy(like(j), partner, pass_send.at[like(j)]).wait_send()
        return c

    lax.fori_loop(1, n // 2, lat_go, 0)
    lat_copy(me, partner, lat_send.at[partner]).start()
    w_load.start()

    qr_load.wait()
    rope_load.wait()
    base[...] = lax.dot_general(
        rope[...].T, qr[...], (((1,), (1,)), ((), ())), preferred_element_type=F32
    )
    cache_load.wait()
    cache_t[...] = cache[...].T
    lax.fori_loop(1, n // 2, lat_pass, 0)
    position = me * positions + lax.broadcasted_iota(jnp.int32, (positions, rows), 0)
    horizon = len_ref[0] + lax.broadcasted_iota(jnp.int32, (positions, rows), 1) // heads
    visible = position < horizon

    lax.fori_loop(0, n // 2, lat_rest, 0)
    query_latent = lat_all[...].reshape(n * cols, rows)
    scores = (jnp.dot(cache[...], query_latent, preferred_element_type=F32) + base[...]) * factor
    block_max = jnp.max(jnp.where(visible, scores, neg_large), axis=0, keepdims=True)
    probs = jnp.where(visible, jnp.exp(scores - block_max), 0.0)
    block_sum = jnp.sum(probs, axis=0, keepdims=True)
    stats[me, 0:1, :] = block_max
    stats[me, 1:2, :] = block_sum
    st = (lambda peer: stats.at[me], stats, st_send, st_recv)
    spread(*st)
    block_out = jnp.dot(cache_t[...], probs.astype(BF16), preferred_element_type=F32)
    out_send[...] = block_out.astype(BF16).reshape(n, cols, rows)
    o = (lambda peer: out_send.at[peer], out_recv, o_send, o_recv)
    spread(*o)
    out_recv[me] = out_send[me]
    vq_load.wait()
    vq_t[...] = vq[...].T

    arrive(*st)
    all_max = stats[:, 0:1, :]
    top = jnp.max(all_max, axis=0, keepdims=True)
    weight = jnp.exp(all_max - top)
    total = jnp.sum(weight * stats[:, 1:2, :], axis=0)
    arrive(*o)
    merged = jnp.sum(out_recv[...].astype(F32) * weight, axis=0) / total
    latent = jnp.where(own, merged[None], 0.0).astype(BF16).reshape(heads * cols, rows)
    partial = jnp.dot(vq_t[...], latent, preferred_element_type=F32) * value_row
    step = width // n
    for d in range(n):
        part_send[d] = partial[d * step : (d + 1) * step].astype(part_send.dtype)
    p = (lambda peer: part_send.at[peer], part_recv, p_send, p_recv)
    spread(*p)
    part_recv[me] = part_send[me]
    arrive(*p)
    share_all[me] = jnp.sum(part_recv[...].astype(F32), axis=0).astype(BF16)
    s = (lambda peer: share_all.at[me], share_all, s_send, s_recv)
    spread(*s)
    arrive(*s)
    head_t = jnp.concatenate([share_all[d].astype(F32) for d in range(n)], axis=0)
    heads_out[...] = head_t.T.reshape(drafts, heads, width)
    for k in range(heads):
        flat[:, k * width : (k + 1) * width] = heads_out[:, k, :].astype(BF16)
    w_load.wait()
    final[group] = lax.dot_general(
        flat[...], w[...], (((1,), (1,)), ((), ())), preferred_element_type=F32
    )

    def pair(j, at):
        peer = lax.rem(group + j, groups)
        return pltpu.make_async_remote_copy(
            src_ref=final.at[group],
            dst_ref=final.at[group if at else peer],
            send_sem=f_send.at[peer],
            recv_sem=f_recv.at[group if at else peer],
            device_id=(peer, me),
            device_id_type=MESH,
        )

    for j in range(1, groups):
        pair(j, True).start()
    for j in range(1, groups):
        pair(j, False).wait_recv()
    out_ref[...] = jnp.sum(final[...], axis=0).astype(BF16)
    for each in (st, o, p, s):
        drain(*each)
    lax.fori_loop(1, n // 2, lat_drain, 0)
    lat_copy(me, partner, lat_send.at[partner]).wait_send()
    for j in range(1, groups):
        pair(j, True).wait_send()


def chip_peer(chip, chips, k):
    out = 0
    bit = 1
    while bit < chips:
        own = lax.rem(chip // bit, 2)
        out = out + bit * ((1 - own) if k & bit else own)
        bit *= 2
    return out


def pair_kernel(
    n,
    groups,
    heads,
    drafts,
    q_hbm,
    qr_hbm,
    cache_hbm,
    rope_hbm,
    len_hbm,
    kq_hbm,
    ks_hbm,
    vq_hbm,
    vs_hbm,
    w_hbm,
    out_ref,
    len_ref,
    ks_ref,
    vs_ref,
    q,
    qr,
    cache,
    rope,
    kq,
    vq,
    w,
    q_rows,
    qr_rows,
    cache_t,
    base,
    lat_send,
    lat_all,
    st_send,
    st_all,
    out_send,
    out_recv,
    part_send,
    part_recv,
    share_send,
    share_recv,
    fin_send,
    fin_recv,
    in_sem,
    swap_s,
    swap_r,
    lat_s,
    lat_r,
    st_s,
    st_r,
    o_s,
    o_r,
    p_s,
    p_r,
    s_s,
    s_r,
    f_s,
    f_r,
):
    me = lax.axis_index("seq")
    group = lax.axis_index("heads")
    core = lax.rem(me, 2)
    other = 1 - core
    chip = me // 2
    chips = n // 2
    half = heads // 2
    rows = half * drafts
    cols = lat_all.shape[1]
    wide = 2 * cols
    latent = cache.shape[2]
    positions = cache.shape[1]
    width = vq.shape[2]
    span = half * width
    share = rows // chips
    per = share // drafts
    factor = (q.shape[2] + qr.shape[2]) ** (-0.5)
    far_first = range(chips - 1, -1, -1)
    peers = [chip_peer(chip, chips, k) for k in range(chips)]
    partner = 2 * chip + other
    quarter = chips // 2
    near = chip // quarter

    def local(i, src, dst):
        copy = pltpu.make_async_copy(src, dst, in_sem.at[i])
        copy.start()
        return copy

    q_load = local(0, q_hbm, q)
    kq_loads = [local(1 + b, kq_hbm.at[pl.ds(b * half, half)], kq.at[pl.ds(b * half, half)]) for b in (1, 0)][::-1]

    barrier = pltpu.get_barrier_semaphore()
    for k in far_first:
        for b in range(2):
            if k:
                pl.semaphore_signal(barrier, inc=1, device_id=(group, 2 * peers[k] + b), device_id_type=MESH)
    pl.semaphore_signal(barrier, inc=1, device_id=(group, partner), device_id_type=MESH)
    for j in range(1, groups):
        for b in range(2):
            pl.semaphore_signal(
                barrier, inc=1, device_id=(lax.rem(group + j, groups), 2 * chip + b), device_id_type=MESH
            )

    ks_load = local(8, ks_hbm, ks_ref)
    qr_load = local(3, qr_hbm.at[:, pl.ds(core * half, half)], qr)
    rope_load = local(4, rope_hbm, rope.at[core])
    cache_load = local(5, cache_hbm, cache.at[core])
    vs_load = local(9, vs_hbm, vs_ref)
    len_load = local(10, len_hbm, len_ref)

    def remote(src, dst, send, recv, peer_group, peer):
        return pltpu.make_async_remote_copy(
            src_ref=src,
            dst_ref=dst,
            send_sem=send,
            recv_sem=recv,
            device_id=(peer_group, peer),
            device_id_type=MESH,
        )

    lane = lax.broadcasted_iota(jnp.int32, (1, rows), 1)
    block = (me * cols) // QB

    def scale_line(scale_ref, index):
        scales = scale_ref[...]
        at = lax.broadcasted_iota(jnp.int32, scales.shape, 0) == index
        return jnp.sum(jnp.where(at, scales, 0.0), axis=0, keepdims=True)

    def scale_column(line, count, first, step):
        shape = (count, heads)
        pick = lax.broadcasted_iota(jnp.int32, shape, 1) == lax.broadcasted_iota(jnp.int32, shape, 0) // step + first
        return jnp.sum(jnp.where(pick, line, 0.0), axis=1, keepdims=True)

    ks_load.wait()
    key_column = scale_column(scale_line(ks_ref, block), heads, 0, 1)
    own_head = lax.broadcasted_iota(jnp.int32, (half, rows), 0) == lane // drafts
    key_rows = [
        jnp.sum(jnp.where(own_head, key_column[b * half : (b + 1) * half], 0.0), axis=0, keepdims=True)
        for b in range(2)
    ]

    q_load.wait()
    for b in range(2):
        for t in range(drafts):
            q_rows[b, pl.ds(t, half, stride=drafts), :] = q[t, b * half : (b + 1) * half, :].astype(F32)

    own = lax.broadcasted_iota(jnp.int32, (half, 1, rows), 0) == lane[None] // drafts
    for b in (1, 0):
        kq_loads[b].wait()
        every = lax.dot_general(
            kq[b * half : (b + 1) * half].reshape(half * cols, kq.shape[2]),
            q_rows[b].astype(BF16),
            (((1,), (1,)), ((), ())),
            preferred_element_type=F32,
        ).reshape(half, cols, rows)
        lat_send[b] = (jnp.sum(jnp.where(own, every, 0.0), axis=0) * key_rows[b]).astype(BF16)
        if b == 1:
            pl.semaphore_wait(barrier, n - 1 + 2 * (groups - 1))
        for k in far_first:
            if k:
                remote(
                    lat_send.at[b], lat_all.at[me], lat_s, lat_r.at[k // quarter], group, 2 * peers[k] + b
                ).start()
    remote(lat_send.at[other], lat_all.at[me], lat_s, lat_r.at[0], group, partner).start()
    lat_all[me] = lat_send[core]

    swaps = [
        remote(src, dst, swap_s.at[i], swap_r.at[i], group, partner)
        for i, (src, dst) in enumerate(
            (
                (rope_hbm, rope.at[core]),
                (cache_hbm, cache.at[core]),
                (vq_hbm.at[pl.ds(core * half, half)], vq.at[:, pl.ds(core * cols, cols)]),
                (w_hbm.at[:, pl.ds(core * span, span)], w.at[core]),
            )
        )
    ]
    swap_arrive = [
        remote(src, dst, swap_s.at[i], swap_r.at[i], group, partner)
        for i, (src, dst) in enumerate(
            (
                (rope_hbm, rope.at[other]),
                (cache_hbm, cache.at[other]),
                (vq_hbm.at[pl.ds(core * half, half)], vq.at[:, pl.ds(other * cols, cols)]),
                (w_hbm.at[:, pl.ds(core * span, span)], w.at[other]),
            )
        )
    ]
    for each in swaps:
        each.start()
    vq_load = local(6, vq_hbm.at[pl.ds(other * half, half)], vq.at[:, pl.ds(core * cols, cols)])
    w_load = local(7, w_hbm.at[:, pl.ds(other * span, span)], w.at[core])

    qr_load.wait()
    for t in range(drafts):
        qr_rows[pl.ds(t, half, stride=drafts), :] = qr[t].astype(F32)
    query_rope = qr_rows[...].astype(BF16)

    def prepare(j):
        turned = lax.dot_general(
            rope[j].T, query_rope, (((1,), (1,)), ((), ())), preferred_element_type=F32
        )
        position = (2 * chip + j) * positions + lax.broadcasted_iota(jnp.int32, (positions, rows), 0)
        horizon = len_ref[0] + lax.rem(lax.broadcasted_iota(jnp.int32, (positions, rows), 1), drafts)
        base[j] = jnp.where(position < horizon, turned * factor, neg_large)
        cache_t[j] = cache[j].T

    vs_load.wait()
    value_column = scale_column(scale_line(vs_ref, block), rows, other * half, drafts)
    len_load.wait()
    rope_load.wait()
    cache_load.wait()
    prepare(core)
    swap_arrive[0].wait_recv()
    swap_arrive[1].wait_recv()
    prepare(other)

    def pieces(ref, count, send, recv):
        some = ref.at[pl.ds(0, count)]
        return remote(some, some, send, recv, group, partner)

    pieces(lat_all, 2 * quarter - 1, lat_s, lat_r.at[0]).wait_recv()

    def part_scores(side):
        begin = pl.multiple_of(side * (latent // 2), latent // 2)
        query = lat_all[pl.ds(side * chips, chips)].reshape(latent // 2, rows)
        return [
            jnp.dot(cache[j, :, pl.ds(begin, latent // 2)], query, preferred_element_type=F32) * factor + base[j]
            for j in range(2)
        ]

    for j, each in enumerate(part_scores(near)):
        base[j] = each
    pieces(lat_all, 2 * quarter, lat_s, lat_r.at[1]).wait_recv()
    scores = part_scores(1 - near)
    block_max = jnp.maximum(
        jnp.max(scores[0], axis=0, keepdims=True), jnp.max(scores[1], axis=0, keepdims=True)
    )
    probs = [jnp.exp(each - block_max) for each in scores]
    st_send[0:1, :] = block_max
    st_send[1:2, :] = jnp.sum(probs[0], axis=0, keepdims=True) + jnp.sum(probs[1], axis=0, keepdims=True)

    def exchange(src_of, dst, send, recv, ks):
        for k in ks:
            remote(src_of(k), dst.at[k], send, recv(k), group, 2 * peers[k] + other).start()

    st = (lambda k: st_send, st_all, st_s, lambda k: st_r)
    exchange(*st, far_first)
    probs = [each.astype(BF16) for each in probs]
    o = (lambda k: out_send.at[peers[k]], out_recv, o_s, lambda k: o_r.at[k // quarter])
    for side, ks in ((1 - near, range(chips - 1, quarter - 1, -1)), (near, range(quarter - 1, -1, -1))):
        begin = pl.multiple_of(side * (latent // 2), latent // 2)
        block_out = sum(
            jnp.dot(cache_t[j, pl.ds(begin, latent // 2), :], probs[j], preferred_element_type=F32)
            for j in range(2)
        )
        out_send[pl.ds(side * quarter, quarter)] = block_out.astype(BF16).reshape(quarter, wide, rows)
        exchange(*o, ks)

    vq_load.wait()
    swap_arrive[2].wait_recv()

    pieces(st_all, chips, st_s, st_r).wait_recv()
    all_max = [st_all[k, 0:1, :] for k in range(chips)]
    top = functools.reduce(jnp.maximum, all_max)
    weight = [jnp.exp(each - top) for each in all_max]
    total = sum(weight[k] * st_all[k, 1:2, :] for k in range(chips))
    merged = jnp.zeros((wide, rows), F32)
    for k in range(chips):
        if k % quarter == 0:
            pieces(out_recv, quarter, o_s, o_r.at[k // quarter]).wait_recv()
        merged = merged + out_recv[k].astype(F32) * weight[k]
    merged = (merged / total).astype(BF16).astype(F32).T
    tile = per * wide
    spread = jnp.concatenate([merged] * per, axis=1)
    keep = (
        lax.broadcasted_iota(jnp.int32, (rows, tile), 1) // wide
        == lax.rem(lax.broadcasted_iota(jnp.int32, (rows, tile), 0) // drafts, per)
    )
    spread = jnp.where(keep, spread, 0.0).astype(BF16)
    for e in range(chips):
        part = jnp.dot(
            spread[e * share : (e + 1) * share],
            vq[e * per : (e + 1) * per].reshape(tile, width),
            preferred_element_type=F32,
        )
        part_send[e] = (part * value_column[e * share : (e + 1) * share]).astype(BF16)
    p = (lambda k: part_send.at[peers[k]], part_recv, p_s, lambda k: p_r)
    exchange(*p, far_first)
    summed = jnp.zeros((share, width), F32)
    pieces(part_recv, chips, p_s, p_r).wait_recv()
    for k in range(chips):
        summed = summed + part_recv[k].astype(F32)
    for h in range(per):
        share_send[:, h * width : (h + 1) * width] = summed[h * drafts : (h + 1) * drafts].astype(BF16)
    s = (lambda k: share_send, share_recv, s_s, lambda k: s_r.at[k])
    exchange(*s, far_first)

    w_load.wait()
    swap_arrive[3].wait_recv()
    model = w.shape[1]
    final = [jnp.zeros((drafts, model), F32) for j in range(2)]
    for k in range(chips):
        pieces(share_recv, 1, s_s, s_r.at[k]).wait_recv()
        begin = pl.multiple_of(peers[k] * (per * width), per * width)
        for j in range(2):
            final[j] = final[j] + lax.dot_general(
                share_recv[k],
                w[j, :, pl.ds(begin, per * width)],
                (((1,), (1,)), ((), ())),
                preferred_element_type=F32,
            )
    for j in range(2):
        fin_send[j] = final[j]

    def last(i, j, b):
        peer_group = lax.rem(group + j, groups)
        side = core if b == 0 else other
        return remote(fin_send.at[side], fin_recv.at[i], f_s, f_r, peer_group, 2 * chip + side)

    lasts = [last(i, j, b) for i, (j, b) in enumerate((j, b) for j in range(groups) for b in range(2) if j or b)]
    for each in lasts[::-1]:
        each.start()
    result = fin_send[core]
    pieces(fin_recv, len(lasts), f_s, f_r).wait_recv()
    for i in range(len(lasts)):
        result = result + fin_recv[i]
    out_ref[...] = result.astype(BF16)

    pieces(lat_all, n - 1, lat_s, lat_r.at[0]).wait_send()
    for ref, send, recv in (
        (st_all, st_s, st_r),
        (out_send, o_s, o_r.at[0]),
        (part_send, p_s, p_r),
        (share_recv, s_s, s_r.at[0]),
        (fin_recv, f_s, f_r),
    ):
        pieces(ref, ref.shape[0], send, recv).wait_send()
    for each in swaps:
        each.wait_send()


def solution(mesh):
    n = mesh.shape["seq"]
    groups = mesh.shape["heads"]

    def paired(query_nope, query_rope, latent_cache, rope_keys, lengths, key_quant, key_scale, value_quant, value_scale, out_weight):
        drafts, heads, nope = query_nope.shape[1:]
        rope = query_rope.shape[-1]
        positions, latent = latent_cache.shape[1:]
        cols = key_quant.shape[1]
        width = value_quant.shape[2]
        model = out_weight.shape[1]
        chips = n // 2
        half = heads // 2
        rows = half * drafts
        share = rows // chips
        wide = 2 * cols
        hbm = pl.BlockSpec(memory_space=pltpu.HBM)
        vmem = pl.BlockSpec(memory_space=pltpu.VMEM)
        dma = pltpu.SemaphoreType.DMA
        lasts = 2 * groups - 1
        result = pl.pallas_call(
            functools.partial(pair_kernel, n, groups, heads, drafts),
            out_shape=pltpu.VMEM((drafts, model), BF16),
            in_specs=[hbm] * 10,
            out_specs=vmem,
            scratch_shapes=[
                pltpu.SMEM(lengths.shape, jnp.int32),
                pltpu.VMEM(key_scale.shape[::-1], F32),
                pltpu.VMEM(value_scale.shape[::-1], F32),
                pltpu.VMEM((drafts, heads, nope), BF16),
                pltpu.VMEM((drafts, half, rope), BF16),
                pltpu.VMEM((2, positions, latent), BF16),
                pltpu.VMEM((2, rope, positions), BF16),
                pltpu.VMEM((heads, cols, nope), BF16),
                pltpu.VMEM((half, wide, width), BF16),
                pltpu.VMEM((2, model, half * width), BF16),
                pltpu.VMEM((2, rows, nope), F32),
                pltpu.VMEM((rows, rope), F32),
                pltpu.VMEM((2, latent, positions), BF16),
                pltpu.VMEM((2, positions, rows), F32),
                pltpu.VMEM((2, cols, rows), BF16),
                pltpu.VMEM((n, cols, rows), BF16),
                pltpu.VMEM((2, rows), F32),
                pltpu.VMEM((chips, 2, rows), F32),
                pltpu.VMEM((chips, wide, rows), BF16),
                pltpu.VMEM((chips, wide, rows), BF16),
                pltpu.VMEM((chips, share, width), BF16),
                pltpu.VMEM((chips, share, width), BF16),
                pltpu.VMEM((drafts, share // drafts * width), BF16),
                pltpu.VMEM((chips, drafts, share // drafts * width), BF16),
                pltpu.VMEM((2, drafts, model), F32),
                pltpu.VMEM((lasts, drafts, model), F32),
                dma((11,)),
                dma((4,)),
                dma((4,)),
                dma,
                dma((2,)),
                dma,
                dma,
                dma,
                dma((2,)),
                dma,
                dma,
                dma,
                dma((chips,)),
                dma,
                dma,
            ],
            compiler_params=pltpu.CompilerParams(
                collective_id=0, has_side_effects=True, vmem_limit_bytes=VMEM_LIMIT
            ),
        )(
            query_nope.reshape(drafts, heads, nope),
            query_rope.reshape(drafts, heads, rope),
            latent_cache.reshape(positions, latent),
            rope_keys.reshape(rope, positions),
            lengths,
            key_quant,
            key_scale.T,
            value_quant,
            value_scale.T,
            out_weight.T,
        )
        return result.reshape(1, drafts, model)

    def per_device(*args):
        drafts, heads = args[0].shape[1:3]
        chips = n // 2
        rows = heads // 2 * drafts
        paired_fits = (
            n % 2 == 0
            and chips & (chips - 1) == 0
            and chips >= 2
            and heads % (2 * chips) == 0
            and rows % 128 == 0
            and args[5].shape[1] % 16 == 0
            and QB % (2 * args[5].shape[1]) == 0
        )
        return (paired if paired_fits else spread_out)(*args)

    def spread_out(
        query_nope,
        query_rope,
        latent_cache,
        rope_keys,
        lengths,
        key_quant,
        key_scale,
        value_quant,
        value_scale,
        out_weight,
    ):
        batch, drafts, heads, nope = query_nope.shape
        rows = batch * drafts * heads
        rope = query_rope.shape[-1]
        positions, latent = latent_cache.shape[1:]
        cols = key_quant.shape[1]
        width = value_quant.shape[2]
        model = out_weight.shape[1]
        hbm = pl.BlockSpec(memory_space=pltpu.HBM)
        vmem = pl.BlockSpec(memory_space=pltpu.VMEM)
        smem = pl.BlockSpec(memory_space=pltpu.SMEM)
        dma = pltpu.SemaphoreType.DMA
        result = pl.pallas_call(
            functools.partial(kernel, n, groups, heads, drafts),
            out_shape=jax.ShapeDtypeStruct((drafts, model), BF16),
            in_specs=[hbm, hbm, hbm, hbm, smem, hbm, vmem, hbm, vmem, hbm],
            out_specs=vmem,
            scratch_shapes=[
                pltpu.VMEM((rows, nope), BF16),
                pltpu.VMEM((rows, rope), BF16),
                pltpu.VMEM((positions, latent), BF16),
                pltpu.VMEM((rope, positions), BF16),
                pltpu.VMEM((heads * cols, nope), BF16),
                pltpu.VMEM((heads * cols, width), BF16),
                pltpu.VMEM(out_weight.shape[::-1], BF16),
                pltpu.VMEM((latent, positions), BF16),
                pltpu.VMEM((width, heads * cols), BF16),
                pltpu.VMEM((positions, rows), F32),
                pltpu.VMEM((n, cols, rows), BF16),
                pltpu.VMEM((n, 2, rows), F32),
                pltpu.VMEM((n, cols, rows), BF16),
                pltpu.VMEM((n, cols, rows), BF16),
                pltpu.VMEM((n, width // n, rows), BF16),
                pltpu.VMEM((n, width // n, rows), BF16),
                pltpu.VMEM((n, width // n, rows), BF16),
                pltpu.VMEM((drafts, heads * width), BF16),
                pltpu.VMEM((drafts, heads, width), F32),
                pltpu.VMEM((groups, drafts, model), F32),
                dma((7,)),
            ]
            + [dma((n,))] * 11
            + [dma((groups,))] * 2,
            compiler_params=pltpu.CompilerParams(
                collective_id=0, has_side_effects=True, vmem_limit_bytes=63 * 1024 * 1024
            ),
        )(
            query_nope.reshape(rows, nope),
            query_rope.reshape(rows, rope),
            latent_cache.reshape(positions, latent),
            rope_keys.reshape(rope, positions),
            lengths,
            key_quant.reshape(heads * cols, nope),
            key_scale.T,
            value_quant.reshape(heads * cols, width),
            value_scale.T,
            out_weight.T,
        )
        return result.reshape(batch, drafts, model)

    in_specs = (
        P(None, None, "heads", None),
        P(None, None, "heads", None),
        P(None, "seq", None),
        P(None, None, "seq"),
        P(),
        P("heads", "seq", None),
        P("heads", None),
        P("heads", "seq", None),
        P("heads", None),
        P("heads", "seq"),
    )
    return jax.shard_map(
        per_device, mesh=mesh, in_specs=in_specs, out_specs=P(None, None, "seq"), check_vma=False
    )
```

```python
import functools

import jax
import jax.numpy as jnp
from jax import lax
from jax.experimental import pallas as pl
from jax.experimental.pallas import tpu as pltpu
from jax.sharding import PartitionSpec as P

QB = 128
VMEM_LIMIT = 67043328 - 32768
MESH = pl.DeviceIdType.MESH
neg_large = -1e30
F32 = jnp.float32
BF16 = jnp.bfloat16


def scale_row(scale_ref, block, rows, heads):
    scales = scale_ref[...]
    line = jnp.sum(
        jnp.where(lax.broadcasted_iota(jnp.int32, scales.shape, 0) == block, scales, 0.0),
        axis=0,
        keepdims=True,
    )
    square = (heads, heads)
    diagonal = lax.broadcasted_iota(jnp.int32, square, 0) == lax.broadcasted_iota(jnp.int32, square, 1)
    column = jnp.sum(jnp.where(diagonal, line, 0.0), axis=1, keepdims=True)
    lane_head = lax.broadcasted_iota(jnp.int32, (heads, rows), 1) % heads
    own_head = lax.broadcasted_iota(jnp.int32, (heads, rows), 0)
    return jnp.sum(jnp.where(lane_head == own_head, column, 0.0), axis=0, keepdims=True)


def kernel(
    n,
    groups,
    heads,
    drafts,
    q_hbm,
    qr_hbm,
    cache_hbm,
    rope_hbm,
    len_ref,
    kq_hbm,
    ks_ref,
    vq_hbm,
    vs_ref,
    w_hbm,
    out_ref,
    q,
    qr,
    cache,
    rope,
    kq,
    vq,
    w,
    cache_t,
    vq_t,
    base,
    lat_all,
    stats,
    out_send,
    out_recv,
    part_send,
    part_recv,
    share_all,
    flat,
    heads_out,
    final,
    in_sem,
    lat_send,
    lat_recv,
    pass_send,
    st_send,
    st_recv,
    o_send,
    o_recv,
    p_send,
    p_recv,
    s_send,
    s_recv,
    f_send,
    f_recv,
):
    me = lax.axis_index("seq")
    group = lax.axis_index("heads")
    rows = q.shape[0]
    cols = lat_all.shape[1]
    width = vq.shape[1]
    positions = cache.shape[0]
    factor = (q.shape[1] + qr.shape[1]) ** (-0.5)

    loads = []
    for i, (src, dst) in enumerate(
        ((kq_hbm, kq), (q_hbm, q), (qr_hbm, qr), (rope_hbm, rope), (cache_hbm, cache), (vq_hbm, vq), (w_hbm, w))
    ):
        copy = pltpu.make_async_copy(src, dst, in_sem.at[i])
        if dst is not w:
            copy.start()
        loads.append(copy)
    kq_load, q_load, qr_load, rope_load, cache_load, vq_load, w_load = loads

    barrier = pltpu.get_barrier_semaphore()

    def greet_seq(j, c):
        pl.semaphore_signal(barrier, inc=1, device_id=(group, lax.rem(me + j, n)), device_id_type=MESH)
        return c

    def greet_heads(j, c):
        pl.semaphore_signal(barrier, inc=1, device_id=(lax.rem(group + j, groups), me), device_id_type=MESH)
        return c

    lax.fori_loop(1, n, greet_seq, 0)
    lax.fori_loop(1, groups, greet_heads, 0)

    def spread(src_of, dst, send, recv):
        def make(j):
            peer = lax.rem(me + j, n)
            return pltpu.make_async_remote_copy(
                src_ref=src_of(peer),
                dst_ref=dst.at[me],
                send_sem=send.at[peer],
                recv_sem=recv.at[me],
                device_id=(group, peer),
                device_id_type=MESH,
            )

        def go(j, c):
            make(j).start()
            return c

        lax.fori_loop(1, n, go, 0)

    def arrive(src_of, dst, send, recv):
        def wait(j, c):
            peer = lax.rem(me + j, n)
            pltpu.make_async_remote_copy(
                src_ref=src_of(peer),
                dst_ref=dst.at[peer],
                send_sem=send.at[peer],
                recv_sem=recv.at[peer],
                device_id=(group, peer),
                device_id_type=MESH,
            ).wait_recv()
            return c

        lax.fori_loop(1, n, wait, 0)

    def drain(src_of, dst, send, recv):
        def wait(j, c):
            peer = lax.rem(me + j, n)
            pltpu.make_async_remote_copy(
                src_ref=src_of(peer),
                dst_ref=dst.at[me],
                send_sem=send.at[peer],
                recv_sem=recv.at[me],
                device_id=(group, peer),
                device_id_type=MESH,
            ).wait_send()
            return c

        lax.fori_loop(1, n, wait, 0)

    block = (me * cols) // QB
    lane_head = lax.broadcasted_iota(jnp.int32, (1, rows), 1) % heads
    key_row = scale_row(ks_ref, block, rows, heads)
    value_row = scale_row(vs_ref, block, rows, heads)

    kq_load.wait()
    q_load.wait()
    every = lax.dot_general(kq[...], q[...], (((1,), (1,)), ((), ())), preferred_element_type=F32)
    every = every.reshape(heads, cols, rows)
    own = lax.broadcasted_iota(jnp.int32, (heads, 1, rows), 0) == lane_head[None]
    piece = jnp.sum(jnp.where(own, every, 0.0), axis=0) * key_row
    lat_all[me] = piece.astype(BF16)

    pl.semaphore_wait(barrier, n - 1 + groups - 1)

    partner = me + 1 - 2 * lax.rem(me, 2)

    def lat_copy(slot, peer, send):
        return pltpu.make_async_remote_copy(
            src_ref=lat_all.at[slot],
            dst_ref=lat_all.at[slot],
            send_sem=send,
            recv_sem=lat_recv.at[slot],
            device_id=(group, peer),
            device_id_type=MESH,
        )

    def like(j):
        return lax.rem(me + 2 * j, n)

    def lat_go(j, c):
        lat_copy(me, like(j), lat_send.at[like(j)]).start()
        return c

    def lat_pass(j, c):
        lat_copy(like(j), partner, pass_send.at[like(j)]).wait_recv()
        lat_copy(like(j), partner, pass_send.at[like(j)]).start()
        return c

    def lat_rest(j, c):
        other = lax.rem(partner + 2 * j, n)
        lat_copy(other, partner, pass_send.at[other]).wait_recv()
        return c

    def lat_drain(j, c):
        lat_copy(me, like(j), lat_send.at[like(j)]).wait_send()
        lat_copy(like(j), partner, pass_send.at[like(j)]).wait_send()
        return c

    lax.fori_loop(1, n // 2, lat_go, 0)
    lat_copy(me, partner, lat_send.at[partner]).start()
    w_load.start()

    qr_load.wait()
    rope_load.wait()
    base[...] = lax.dot_general(
        rope[...].T, qr[...], (((1,), (1,)), ((), ())), preferred_element_type=F32
    )
    cache_load.wait()
    cache_t[...] = cache[...].T
    lax.fori_loop(1, n // 2, lat_pass, 0)
    position = me * positions + lax.broadcasted_iota(jnp.int32, (positions, rows), 0)
    horizon = len_ref[0] + lax.broadcasted_iota(jnp.int32, (positions, rows), 1) // heads
    visible = position < horizon

    lax.fori_loop(0, n // 2, lat_rest, 0)
    query_latent = lat_all[...].reshape(n * cols, rows)
    scores = (jnp.dot(cache[...], query_latent, preferred_element_type=F32) + base[...]) * factor
    block_max = jnp.max(jnp.where(visible, scores, neg_large), axis=0, keepdims=True)
    probs = jnp.where(visible, jnp.exp(scores - block_max), 0.0)
    block_sum = jnp.sum(probs, axis=0, keepdims=True)
    stats[me, 0:1, :] = block_max
    stats[me, 1:2, :] = block_sum
    st = (lambda peer: stats.at[me], stats, st_send, st_recv)
    spread(*st)
    block_out = jnp.dot(cache_t[...], probs.astype(BF16), preferred_element_type=F32)
    out_send[...] = block_out.astype(BF16).reshape(n, cols, rows)
    o = (lambda peer: out_send.at[peer], out_recv, o_send, o_recv)
    spread(*o)
    out_recv[me] = out_send[me]
    vq_load.wait()
    vq_t[...] = vq[...].T

    arrive(*st)
    all_max = stats[:, 0:1, :]
    top = jnp.max(all_max, axis=0, keepdims=True)
    weight = jnp.exp(all_max - top)
    total = jnp.sum(weight * stats[:, 1:2, :], axis=0)
    arrive(*o)
    merged = jnp.sum(out_recv[...].astype(F32) * weight, axis=0) / total
    latent = jnp.where(own, merged[None], 0.0).astype(BF16).reshape(heads * cols, rows)
    partial = jnp.dot(vq_t[...], latent, preferred_element_type=F32) * value_row
    step = width // n
    for d in range(n):
        part_send[d] = partial[d * step : (d + 1) * step].astype(part_send.dtype)
    p = (lambda peer: part_send.at[peer], part_recv, p_send, p_recv)
    spread(*p)
    part_recv[me] = part_send[me]
    arrive(*p)
    share_all[me] = jnp.sum(part_recv[...].astype(F32), axis=0).astype(BF16)
    s = (lambda peer: share_all.at[me], share_all, s_send, s_recv)
    spread(*s)
    arrive(*s)
    head_t = jnp.concatenate([share_all[d].astype(F32) for d in range(n)], axis=0)
    heads_out[...] = head_t.T.reshape(drafts, heads, width)
    for k in range(heads):
        flat[:, k * width : (k + 1) * width] = heads_out[:, k, :].astype(BF16)
    w_load.wait()
    final[group] = lax.dot_general(
        flat[...], w[...], (((1,), (1,)), ((), ())), preferred_element_type=F32
    )

    def pair(j, at):
        peer = lax.rem(group + j, groups)
        return pltpu.make_async_remote_copy(
            src_ref=final.at[group],
            dst_ref=final.at[group if at else peer],
            send_sem=f_send.at[peer],
            recv_sem=f_recv.at[group if at else peer],
            device_id=(peer, me),
            device_id_type=MESH,
        )

    for j in range(1, groups):
        pair(j, True).start()
    for j in range(1, groups):
        pair(j, False).wait_recv()
    out_ref[...] = jnp.sum(final[...], axis=0).astype(BF16)
    for each in (st, o, p, s):
        drain(*each)
    lax.fori_loop(1, n // 2, lat_drain, 0)
    lat_copy(me, partner, lat_send.at[partner]).wait_send()
    for j in range(1, groups):
        pair(j, True).wait_send()


def chip_peer(chip, chips, k):
    out = 0
    bit = 1
    while bit < chips:
        own = lax.rem(chip // bit, 2)
        out = out + bit * ((1 - own) if k & bit else own)
        bit *= 2
    return out


def pair_kernel(
    n,
    groups,
    heads,
    drafts,
    q_hbm,
    qr_hbm,
    cache_hbm,
    rope_hbm,
    len_hbm,
    kq_hbm,
    ks_hbm,
    vq_hbm,
    vs_hbm,
    w_hbm,
    out_ref,
    len_ref,
    ks_ref,
    vs_ref,
    q,
    qr,
    cache,
    rope,
    kq,
    vq,
    w,
    w_t,
    q_rows,
    qr_rows,
    cache_t,
    base,
    lat_send,
    lat_all,
    st_send,
    st_all,
    out_send,
    out_recv,
    part_send,
    part_recv,
    share_send,
    share_recv,
    fin_send,
    fin_recv,
    in_sem,
    swap_s,
    swap_r,
    lat_s,
    lat_r,
    st_s,
    st_r,
    o_s,
    o_r,
    p_s,
    p_r,
    s_s,
    s_r,
    f_s,
    f_r,
):
    me = lax.axis_index("seq")
    group = lax.axis_index("heads")
    core = lax.rem(me, 2)
    other = 1 - core
    chip = me // 2
    chips = n // 2
    half = heads // 2
    rows = half * drafts
    cols = lat_all.shape[1]
    wide = 2 * cols
    latent = cache.shape[2]
    positions = cache.shape[1]
    width = vq.shape[2]
    span = half * width
    share = rows // chips
    per = share // drafts
    factor = (q.shape[2] + qr.shape[2]) ** (-0.5)
    far_first = range(chips - 1, -1, -1)
    peers = [chip_peer(chip, chips, k) for k in range(chips)]
    partner = 2 * chip + other
    quarter = chips // 2
    near = chip // quarter

    def local(i, src, dst):
        copy = pltpu.make_async_copy(src, dst, in_sem.at[i])
        copy.start()
        return copy

    q_load = local(0, q_hbm, q)
    kq_loads = [local(1 + b, kq_hbm.at[pl.ds(b * half, half)], kq.at[pl.ds(b * half, half)]) for b in (1, 0)][::-1]

    barrier = pltpu.get_barrier_semaphore()
    for k in far_first:
        for b in range(2):
            if k:
                pl.semaphore_signal(barrier, inc=1, device_id=(group, 2 * peers[k] + b), device_id_type=MESH)
    pl.semaphore_signal(barrier, inc=1, device_id=(group, partner), device_id_type=MESH)
    for j in range(1, groups):
        for b in range(2):
            pl.semaphore_signal(
                barrier, inc=1, device_id=(lax.rem(group + j, groups), 2 * chip + b), device_id_type=MESH
            )

    ks_load = local(8, ks_hbm, ks_ref)
    qr_load = local(3, qr_hbm.at[:, pl.ds(core * half, half)], qr)
    rope_load = local(4, rope_hbm, rope.at[core])
    cache_load = local(5, cache_hbm, cache.at[core])
    vs_load = local(9, vs_hbm, vs_ref)
    len_load = local(10, len_hbm, len_ref)

    def remote(src, dst, send, recv, peer_group, peer):
        return pltpu.make_async_remote_copy(
            src_ref=src,
            dst_ref=dst,
            send_sem=send,
            recv_sem=recv,
            device_id=(peer_group, peer),
            device_id_type=MESH,
        )

    lane = lax.broadcasted_iota(jnp.int32, (1, rows), 1)
    block = (me * cols) // QB

    def scale_line(scale_ref, index):
        scales = scale_ref[...]
        at = lax.broadcasted_iota(jnp.int32, scales.shape, 0) == index
        return jnp.sum(jnp.where(at, scales, 0.0), axis=0, keepdims=True)

    def scale_column(line, count, first, step):
        shape = (count, heads)
        pick = lax.broadcasted_iota(jnp.int32, shape, 1) == lax.broadcasted_iota(jnp.int32, shape, 0) // step + first
        return jnp.sum(jnp.where(pick, line, 0.0), axis=1, keepdims=True)

    ks_load.wait()
    key_column = scale_column(scale_line(ks_ref, block), heads, 0, 1)
    own_head = lax.broadcasted_iota(jnp.int32, (half, rows), 0) == lane // drafts
    key_rows = [
        jnp.sum(jnp.where(own_head, key_column[b * half : (b + 1) * half], 0.0), axis=0, keepdims=True)
        for b in range(2)
    ]

    q_load.wait()
    for b in range(2):
        for t in range(drafts):
            q_rows[b, pl.ds(t, half, stride=drafts), :] = q[t, b * half : (b + 1) * half, :].astype(F32)

    own = lax.broadcasted_iota(jnp.int32, (half, 1, rows), 0) == lane[None] // drafts
    for b in (1, 0):
        kq_loads[b].wait()
        every = lax.dot_general(
            kq[b * half : (b + 1) * half].reshape(half * cols, kq.shape[2]),
            q_rows[b].astype(BF16),
            (((1,), (1,)), ((), ())),
            preferred_element_type=F32,
        ).reshape(half, cols, rows)
        lat_send[b] = (jnp.sum(jnp.where(own, every, 0.0), axis=0) * key_rows[b]).astype(BF16)
        if b == 1:
            pl.semaphore_wait(barrier, n - 1 + 2 * (groups - 1))
        for k in far_first:
            if k:
                remote(
                    lat_send.at[b], lat_all.at[me], lat_s, lat_r.at[k // quarter], group, 2 * peers[k] + b
                ).start()
    remote(lat_send.at[other], lat_all.at[me], lat_s, lat_r.at[0], group, partner).start()
    lat_all[me] = lat_send[core]

    swaps = [
        remote(src, dst, swap_s.at[i], swap_r.at[i], group, partner)
        for i, (src, dst) in enumerate(
            (
                (rope_hbm, rope.at[core]),
                (cache_hbm, cache.at[core]),
                (vq_hbm.at[pl.ds(core * half, half)], vq.at[:, pl.ds(core * cols, cols)]),
                (w_hbm.at[:, pl.ds(core * span, span)], w.at[core]),
            )
        )
    ]
    swap_arrive = [
        remote(src, dst, swap_s.at[i], swap_r.at[i], group, partner)
        for i, (src, dst) in enumerate(
            (
                (rope_hbm, rope.at[other]),
                (cache_hbm, cache.at[other]),
                (vq_hbm.at[pl.ds(core * half, half)], vq.at[:, pl.ds(other * cols, cols)]),
                (w_hbm.at[:, pl.ds(core * span, span)], w.at[other]),
            )
        )
    ]
    for each in swaps:
        each.start()
    vq_load = local(6, vq_hbm.at[pl.ds(other * half, half)], vq.at[:, pl.ds(core * cols, cols)])
    w_load = local(7, w_hbm.at[:, pl.ds(other * span, span)], w.at[core])

    qr_load.wait()
    for t in range(drafts):
        qr_rows[pl.ds(t, half, stride=drafts), :] = qr[t].astype(F32)
    query_rope = qr_rows[...].astype(BF16)

    def prepare(j):
        turned = lax.dot_general(
            rope[j].T, query_rope, (((1,), (1,)), ((), ())), preferred_element_type=F32
        )
        position = (2 * chip + j) * positions + lax.broadcasted_iota(jnp.int32, (positions, rows), 0)
        horizon = len_ref[0] + lax.rem(lax.broadcasted_iota(jnp.int32, (positions, rows), 1), drafts)
        base[j] = jnp.where(position < horizon, turned * factor, neg_large)
        cache_t[j] = cache[j].T

    vs_load.wait()
    value_column = scale_column(scale_line(vs_ref, block), rows, other * half, drafts)
    len_load.wait()
    rope_load.wait()
    cache_load.wait()
    prepare(core)
    swap_arrive[0].wait_recv()
    swap_arrive[1].wait_recv()
    prepare(other)

    def pieces(ref, count, send, recv):
        some = ref.at[pl.ds(0, count)]
        return remote(some, some, send, recv, group, partner)

    pieces(lat_all, 2 * quarter - 1, lat_s, lat_r.at[0]).wait_recv()

    def part_scores(side):
        begin = pl.multiple_of(side * (latent // 2), latent // 2)
        query = lat_all[pl.ds(side * chips, chips)].reshape(latent // 2, rows)
        return [
            jnp.dot(cache[j, :, pl.ds(begin, latent // 2)], query, preferred_element_type=F32) * factor + base[j]
            for j in range(2)
        ]

    for j, each in enumerate(part_scores(near)):
        base[j] = each
    pieces(lat_all, 2 * quarter, lat_s, lat_r.at[1]).wait_recv()
    scores = part_scores(1 - near)
    block_max = jnp.maximum(
        jnp.max(scores[0], axis=0, keepdims=True), jnp.max(scores[1], axis=0, keepdims=True)
    )
    probs = [jnp.exp(each - block_max) for each in scores]
    st_send[0:1, :] = block_max
    st_send[1:2, :] = jnp.sum(probs[0], axis=0, keepdims=True) + jnp.sum(probs[1], axis=0, keepdims=True)

    def exchange(src_of, dst, send, recv, ks):
        for k in ks:
            remote(src_of(k), dst.at[k], send, recv(k), group, 2 * peers[k] + other).start()

    st = (lambda k: st_send, st_all, st_s, lambda k: st_r)
    exchange(*st, far_first)
    probs = [each.astype(BF16) for each in probs]
    o = (lambda k: out_send.at[peers[k]], out_recv, o_s, lambda k: o_r.at[k // quarter])
    for side, ks in ((1 - near, range(chips - 1, quarter - 1, -1)), (near, range(quarter - 1, -1, -1))):
        begin = pl.multiple_of(side * (latent // 2), latent // 2)
        block_out = sum(
            jnp.dot(cache_t[j, pl.ds(begin, latent // 2), :], probs[j], preferred_element_type=F32)
            for j in range(2)
        )
        out_send[pl.ds(side * quarter, quarter)] = block_out.astype(BF16).reshape(quarter, wide, rows)
        exchange(*o, ks)

    def turn(j):
        step = per * width
        for k in range(chips):
            w_t[j, k * step : (k + 1) * step, :] = w[j, :, k * step : (k + 1) * step].T

    w_load.wait()
    turn(core)
    vq_load.wait()
    swap_arrive[2].wait_recv()

    pieces(st_all, chips, st_s, st_r).wait_recv()
    all_max = [st_all[k, 0:1, :] for k in range(chips)]
    top = functools.reduce(jnp.maximum, all_max)
    weight = [jnp.exp(each - top) for each in all_max]
    total = sum(weight[k] * st_all[k, 1:2, :] for k in range(chips))
    merged = jnp.zeros((wide, rows), F32)
    for k in range(chips):
        if k % quarter == 0:
            pieces(out_recv, quarter, o_s, o_r.at[k // quarter]).wait_recv()
        merged = merged + out_recv[k].astype(F32) * weight[k]
    merged = (merged / total).astype(BF16).astype(F32).T
    tile = per * wide
    spread = jnp.concatenate([merged] * per, axis=1)
    keep = (
        lax.broadcasted_iota(jnp.int32, (rows, tile), 1) // wide
        == lax.rem(lax.broadcasted_iota(jnp.int32, (rows, tile), 0) // drafts, per)
    )
    spread = jnp.where(keep, spread, 0.0).astype(BF16)
    for e in range(chips):
        part = jnp.dot(
            spread[e * share : (e + 1) * share],
            vq[e * per : (e + 1) * per].reshape(tile, width),
            preferred_element_type=F32,
        )
        part_send[e] = (part * value_column[e * share : (e + 1) * share]).astype(BF16)
    p = (lambda k: part_send.at[peers[k]], part_recv, p_s, lambda k: p_r)
    exchange(*p, far_first)
    swap_arrive[3].wait_recv()
    turn(other)
    summed = jnp.zeros((share, width), F32)
    pieces(part_recv, chips, p_s, p_r).wait_recv()
    for k in range(chips):
        summed = summed + part_recv[k].astype(F32)
    for h in range(per):
        share_send[:, h * width : (h + 1) * width] = summed[h * drafts : (h + 1) * drafts].astype(BF16)
    s = (lambda k: share_send, share_recv, s_s, lambda k: s_r.at[k])
    exchange(*s, far_first)

    model = w.shape[1]
    final = [jnp.zeros((drafts, model), F32) for j in range(2)]
    for k in range(chips):
        pieces(share_recv, 1, s_s, s_r.at[k]).wait_recv()
        begin = pl.multiple_of(peers[k] * (per * width), per * width)
        for j in range(2):
            final[j] = final[j] + jnp.dot(
                share_recv[k], w_t[j, pl.ds(begin, per * width), :], preferred_element_type=F32
            )
    for j in range(2):
        fin_send[j] = final[j]

    def last(i, j, b):
        peer_group = lax.rem(group + j, groups)
        side = core if b == 0 else other
        return remote(fin_send.at[side], fin_recv.at[i], f_s, f_r, peer_group, 2 * chip + side)

    lasts = [last(i, j, b) for i, (j, b) in enumerate((j, b) for j in range(groups) for b in range(2) if j or b)]
    for each in lasts[::-1]:
        each.start()
    result = fin_send[core]
    pieces(fin_recv, len(lasts), f_s, f_r).wait_recv()
    for i in range(len(lasts)):
        result = result + fin_recv[i]
    out_ref[...] = result.astype(BF16)

    pieces(lat_all, n - 1, lat_s, lat_r.at[0]).wait_send()
    for ref, send, recv in (
        (st_all, st_s, st_r),
        (out_send, o_s, o_r.at[0]),
        (part_send, p_s, p_r),
        (share_recv, s_s, s_r.at[0]),
        (fin_recv, f_s, f_r),
    ):
        pieces(ref, ref.shape[0], send, recv).wait_send()
    for each in swaps:
        each.wait_send()


def solution(mesh):
    n = mesh.shape["seq"]
    groups = mesh.shape["heads"]

    def paired(query_nope, query_rope, latent_cache, rope_keys, lengths, key_quant, key_scale, value_quant, value_scale, out_weight):
        drafts, heads, nope = query_nope.shape[1:]
        rope = query_rope.shape[-1]
        positions, latent = latent_cache.shape[1:]
        cols = key_quant.shape[1]
        width = value_quant.shape[2]
        model = out_weight.shape[1]
        chips = n // 2
        half = heads // 2
        rows = half * drafts
        share = rows // chips
        wide = 2 * cols
        hbm = pl.BlockSpec(memory_space=pltpu.HBM)
        vmem = pl.BlockSpec(memory_space=pltpu.VMEM)
        dma = pltpu.SemaphoreType.DMA
        lasts = 2 * groups - 1
        result = pl.pallas_call(
            functools.partial(pair_kernel, n, groups, heads, drafts),
            out_shape=pltpu.VMEM((drafts, model), BF16),
            in_specs=[hbm] * 10,
            out_specs=vmem,
            scratch_shapes=[
                pltpu.SMEM(lengths.shape, jnp.int32),
                pltpu.VMEM(key_scale.shape[::-1], F32),
                pltpu.VMEM(value_scale.shape[::-1], F32),
                pltpu.VMEM((drafts, heads, nope), BF16),
                pltpu.VMEM((drafts, half, rope), BF16),
                pltpu.VMEM((2, positions, latent), BF16),
                pltpu.VMEM((2, rope, positions), BF16),
                pltpu.VMEM((heads, cols, nope), BF16),
                pltpu.VMEM((half, wide, width), BF16),
                pltpu.VMEM((2, model, half * width), BF16),
                pltpu.VMEM((2, half * width, model), BF16),
                pltpu.VMEM((2, rows, nope), F32),
                pltpu.VMEM((rows, rope), F32),
                pltpu.VMEM((2, latent, positions), BF16),
                pltpu.VMEM((2, positions, rows), F32),
                pltpu.VMEM((2, cols, rows), BF16),
                pltpu.VMEM((n, cols, rows), BF16),
                pltpu.VMEM((2, rows), F32),
                pltpu.VMEM((chips, 2, rows), F32),
                pltpu.VMEM((chips, wide, rows), BF16),
                pltpu.VMEM((chips, wide, rows), BF16),
                pltpu.VMEM((chips, share, width), BF16),
                pltpu.VMEM((chips, share, width), BF16),
                pltpu.VMEM((drafts, share // drafts * width), BF16),
                pltpu.VMEM((chips, drafts, share // drafts * width), BF16),
                pltpu.VMEM((2, drafts, model), F32),
                pltpu.VMEM((lasts, drafts, model), F32),
                dma((11,)),
                dma((4,)),
                dma((4,)),
                dma,
                dma((2,)),
                dma,
                dma,
                dma,
                dma((2,)),
                dma,
                dma,
                dma,
                dma((chips,)),
                dma,
                dma,
            ],
            compiler_params=pltpu.CompilerParams(
                collective_id=0, has_side_effects=True, vmem_limit_bytes=VMEM_LIMIT
            ),
        )(
            query_nope.reshape(drafts, heads, nope),
            query_rope.reshape(drafts, heads, rope),
            latent_cache.reshape(positions, latent),
            rope_keys.reshape(rope, positions),
            lengths,
            key_quant,
            key_scale.T,
            value_quant,
            value_scale.T,
            out_weight.T,
        )
        return result.reshape(1, drafts, model)

    def per_device(*args):
        drafts, heads = args[0].shape[1:3]
        chips = n // 2
        rows = heads // 2 * drafts
        paired_fits = (
            n % 2 == 0
            and chips & (chips - 1) == 0
            and chips >= 2
            and heads % (2 * chips) == 0
            and rows % 128 == 0
            and args[5].shape[1] % 16 == 0
            and QB % (2 * args[5].shape[1]) == 0
        )
        return (paired if paired_fits else spread_out)(*args)

    def spread_out(
        query_nope,
        query_rope,
        latent_cache,
        rope_keys,
        lengths,
        key_quant,
        key_scale,
        value_quant,
        value_scale,
        out_weight,
    ):
        batch, drafts, heads, nope = query_nope.shape
        rows = batch * drafts * heads
        rope = query_rope.shape[-1]
        positions, latent = latent_cache.shape[1:]
        cols = key_quant.shape[1]
        width = value_quant.shape[2]
        model = out_weight.shape[1]
        hbm = pl.BlockSpec(memory_space=pltpu.HBM)
        vmem = pl.BlockSpec(memory_space=pltpu.VMEM)
        smem = pl.BlockSpec(memory_space=pltpu.SMEM)
        dma = pltpu.SemaphoreType.DMA
        result = pl.pallas_call(
            functools.partial(kernel, n, groups, heads, drafts),
            out_shape=jax.ShapeDtypeStruct((drafts, model), BF16),
            in_specs=[hbm, hbm, hbm, hbm, smem, hbm, vmem, hbm, vmem, hbm],
            out_specs=vmem,
            scratch_shapes=[
                pltpu.VMEM((rows, nope), BF16),
                pltpu.VMEM((rows, rope), BF16),
                pltpu.VMEM((positions, latent), BF16),
                pltpu.VMEM((rope, positions), BF16),
                pltpu.VMEM((heads * cols, nope), BF16),
                pltpu.VMEM((heads * cols, width), BF16),
                pltpu.VMEM(out_weight.shape[::-1], BF16),
                pltpu.VMEM((latent, positions), BF16),
                pltpu.VMEM((width, heads * cols), BF16),
                pltpu.VMEM((positions, rows), F32),
                pltpu.VMEM((n, cols, rows), BF16),
                pltpu.VMEM((n, 2, rows), F32),
                pltpu.VMEM((n, cols, rows), BF16),
                pltpu.VMEM((n, cols, rows), BF16),
                pltpu.VMEM((n, width // n, rows), BF16),
                pltpu.VMEM((n, width // n, rows), BF16),
                pltpu.VMEM((n, width // n, rows), BF16),
                pltpu.VMEM((drafts, heads * width), BF16),
                pltpu.VMEM((drafts, heads, width), F32),
                pltpu.VMEM((groups, drafts, model), F32),
                dma((7,)),
            ]
            + [dma((n,))] * 11
            + [dma((groups,))] * 2,
            compiler_params=pltpu.CompilerParams(
                collective_id=0, has_side_effects=True, vmem_limit_bytes=63 * 1024 * 1024
            ),
        )(
            query_nope.reshape(rows, nope),
            query_rope.reshape(rows, rope),
            latent_cache.reshape(positions, latent),
            rope_keys.reshape(rope, positions),
            lengths,
            key_quant.reshape(heads * cols, nope),
            key_scale.T,
            value_quant.reshape(heads * cols, width),
            value_scale.T,
            out_weight.T,
        )
        return result.reshape(batch, drafts, model)

    in_specs = (
        P(None, None, "heads", None),
        P(None, None, "heads", None),
        P(None, "seq", None),
        P(None, None, "seq"),
        P(),
        P("heads", "seq", None),
        P("heads", None),
        P("heads", "seq", None),
        P("heads", None),
        P("heads", "seq"),
    )
    return jax.shard_map(
        per_device, mesh=mesh, in_specs=in_specs, out_specs=P(None, None, "seq"), check_vma=False
    )
```

```python
import functools

import jax
import jax.numpy as jnp
from jax import lax
from jax.experimental import pallas as pl
from jax.experimental.pallas import tpu as pltpu
from jax.sharding import PartitionSpec as P

QB = 128
VMEM_LIMIT = 67043328 - 32768
MESH = pl.DeviceIdType.MESH
neg_large = -1e30
F32 = jnp.float32
BF16 = jnp.bfloat16


def scale_row(scale_ref, block, rows, heads):
    scales = scale_ref[...]
    line = jnp.sum(
        jnp.where(lax.broadcasted_iota(jnp.int32, scales.shape, 0) == block, scales, 0.0),
        axis=0,
        keepdims=True,
    )
    square = (heads, heads)
    diagonal = lax.broadcasted_iota(jnp.int32, square, 0) == lax.broadcasted_iota(jnp.int32, square, 1)
    column = jnp.sum(jnp.where(diagonal, line, 0.0), axis=1, keepdims=True)
    lane_head = lax.broadcasted_iota(jnp.int32, (heads, rows), 1) % heads
    own_head = lax.broadcasted_iota(jnp.int32, (heads, rows), 0)
    return jnp.sum(jnp.where(lane_head == own_head, column, 0.0), axis=0, keepdims=True)


def kernel(
    n,
    groups,
    heads,
    drafts,
    q_hbm,
    qr_hbm,
    cache_hbm,
    rope_hbm,
    len_ref,
    kq_hbm,
    ks_ref,
    vq_hbm,
    vs_ref,
    w_hbm,
    out_ref,
    q,
    qr,
    cache,
    rope,
    kq,
    vq,
    w,
    cache_t,
    vq_t,
    base,
    lat_all,
    stats,
    out_send,
    out_recv,
    part_send,
    part_recv,
    share_all,
    flat,
    heads_out,
    final,
    in_sem,
    lat_send,
    lat_recv,
    pass_send,
    st_send,
    st_recv,
    o_send,
    o_recv,
    p_send,
    p_recv,
    s_send,
    s_recv,
    f_send,
    f_recv,
):
    me = lax.axis_index("seq")
    group = lax.axis_index("heads")
    rows = q.shape[0]
    cols = lat_all.shape[1]
    width = vq.shape[1]
    positions = cache.shape[0]
    factor = (q.shape[1] + qr.shape[1]) ** (-0.5)

    loads = []
    for i, (src, dst) in enumerate(
        ((kq_hbm, kq), (q_hbm, q), (qr_hbm, qr), (rope_hbm, rope), (cache_hbm, cache), (vq_hbm, vq), (w_hbm, w))
    ):
        copy = pltpu.make_async_copy(src, dst, in_sem.at[i])
        if dst is not w:
            copy.start()
        loads.append(copy)
    kq_load, q_load, qr_load, rope_load, cache_load, vq_load, w_load = loads

    barrier = pltpu.get_barrier_semaphore()

    def greet_seq(j, c):
        pl.semaphore_signal(barrier, inc=1, device_id=(group, lax.rem(me + j, n)), device_id_type=MESH)
        return c

    def greet_heads(j, c):
        pl.semaphore_signal(barrier, inc=1, device_id=(lax.rem(group + j, groups), me), device_id_type=MESH)
        return c

    lax.fori_loop(1, n, greet_seq, 0)
    lax.fori_loop(1, groups, greet_heads, 0)

    def spread(src_of, dst, send, recv):
        def make(j):
            peer = lax.rem(me + j, n)
            return pltpu.make_async_remote_copy(
                src_ref=src_of(peer),
                dst_ref=dst.at[me],
                send_sem=send.at[peer],
                recv_sem=recv.at[me],
                device_id=(group, peer),
                device_id_type=MESH,
            )

        def go(j, c):
            make(j).start()
            return c

        lax.fori_loop(1, n, go, 0)

    def arrive(src_of, dst, send, recv):
        def wait(j, c):
            peer = lax.rem(me + j, n)
            pltpu.make_async_remote_copy(
                src_ref=src_of(peer),
                dst_ref=dst.at[peer],
                send_sem=send.at[peer],
                recv_sem=recv.at[peer],
                device_id=(group, peer),
                device_id_type=MESH,
            ).wait_recv()
            return c

        lax.fori_loop(1, n, wait, 0)

    def drain(src_of, dst, send, recv):
        def wait(j, c):
            peer = lax.rem(me + j, n)
            pltpu.make_async_remote_copy(
                src_ref=src_of(peer),
                dst_ref=dst.at[me],
                send_sem=send.at[peer],
                recv_sem=recv.at[me],
                device_id=(group, peer),
                device_id_type=MESH,
            ).wait_send()
            return c

        lax.fori_loop(1, n, wait, 0)

    block = (me * cols) // QB
    lane_head = lax.broadcasted_iota(jnp.int32, (1, rows), 1) % heads
    key_row = scale_row(ks_ref, block, rows, heads)
    value_row = scale_row(vs_ref, block, rows, heads)

    kq_load.wait()
    q_load.wait()
    every = lax.dot_general(kq[...], q[...], (((1,), (1,)), ((), ())), preferred_element_type=F32)
    every = every.reshape(heads, cols, rows)
    own = lax.broadcasted_iota(jnp.int32, (heads, 1, rows), 0) == lane_head[None]
    piece = jnp.sum(jnp.where(own, every, 0.0), axis=0) * key_row
    lat_all[me] = piece.astype(BF16)

    pl.semaphore_wait(barrier, n - 1 + groups - 1)

    partner = me + 1 - 2 * lax.rem(me, 2)

    def lat_copy(slot, peer, send):
        return pltpu.make_async_remote_copy(
            src_ref=lat_all.at[slot],
            dst_ref=lat_all.at[slot],
            send_sem=send,
            recv_sem=lat_recv.at[slot],
            device_id=(group, peer),
            device_id_type=MESH,
        )

    def like(j):
        return lax.rem(me + 2 * j, n)

    def lat_go(j, c):
        lat_copy(me, like(j), lat_send.at[like(j)]).start()
        return c

    def lat_pass(j, c):
        lat_copy(like(j), partner, pass_send.at[like(j)]).wait_recv()
        lat_copy(like(j), partner, pass_send.at[like(j)]).start()
        return c

    def lat_rest(j, c):
        other = lax.rem(partner + 2 * j, n)
        lat_copy(other, partner, pass_send.at[other]).wait_recv()
        return c

    def lat_drain(j, c):
        lat_copy(me, like(j), lat_send.at[like(j)]).wait_send()
        lat_copy(like(j), partner, pass_send.at[like(j)]).wait_send()
        return c

    lax.fori_loop(1, n // 2, lat_go, 0)
    lat_copy(me, partner, lat_send.at[partner]).start()
    w_load.start()

    qr_load.wait()
    rope_load.wait()
    base[...] = lax.dot_general(
        rope[...].T, qr[...], (((1,), (1,)), ((), ())), preferred_element_type=F32
    )
    cache_load.wait()
    cache_t[...] = cache[...].T
    lax.fori_loop(1, n // 2, lat_pass, 0)
    position = me * positions + lax.broadcasted_iota(jnp.int32, (positions, rows), 0)
    horizon = len_ref[0] + lax.broadcasted_iota(jnp.int32, (positions, rows), 1) // heads
    visible = position < horizon

    lax.fori_loop(0, n // 2, lat_rest, 0)
    query_latent = lat_all[...].reshape(n * cols, rows)
    scores = (jnp.dot(cache[...], query_latent, preferred_element_type=F32) + base[...]) * factor
    block_max = jnp.max(jnp.where(visible, scores, neg_large), axis=0, keepdims=True)
    probs = jnp.where(visible, jnp.exp(scores - block_max), 0.0)
    block_sum = jnp.sum(probs, axis=0, keepdims=True)
    stats[me, 0:1, :] = block_max
    stats[me, 1:2, :] = block_sum
    st = (lambda peer: stats.at[me], stats, st_send, st_recv)
    spread(*st)
    block_out = jnp.dot(cache_t[...], probs.astype(BF16), preferred_element_type=F32)
    out_send[...] = block_out.astype(BF16).reshape(n, cols, rows)
    o = (lambda peer: out_send.at[peer], out_recv, o_send, o_recv)
    spread(*o)
    out_recv[me] = out_send[me]
    vq_load.wait()
    vq_t[...] = vq[...].T

    arrive(*st)
    all_max = stats[:, 0:1, :]
    top = jnp.max(all_max, axis=0, keepdims=True)
    weight = jnp.exp(all_max - top)
    total = jnp.sum(weight * stats[:, 1:2, :], axis=0)
    arrive(*o)
    merged = jnp.sum(out_recv[...].astype(F32) * weight, axis=0) / total
    latent = jnp.where(own, merged[None], 0.0).astype(BF16).reshape(heads * cols, rows)
    partial = jnp.dot(vq_t[...], latent, preferred_element_type=F32) * value_row
    step = width // n
    for d in range(n):
        part_send[d] = partial[d * step : (d + 1) * step].astype(part_send.dtype)
    p = (lambda peer: part_send.at[peer], part_recv, p_send, p_recv)
    spread(*p)
    part_recv[me] = part_send[me]
    arrive(*p)
    share_all[me] = jnp.sum(part_recv[...].astype(F32), axis=0).astype(BF16)
    s = (lambda peer: share_all.at[me], share_all, s_send, s_recv)
    spread(*s)
    arrive(*s)
    head_t = jnp.concatenate([share_all[d].astype(F32) for d in range(n)], axis=0)
    heads_out[...] = head_t.T.reshape(drafts, heads, width)
    for k in range(heads):
        flat[:, k * width : (k + 1) * width] = heads_out[:, k, :].astype(BF16)
    w_load.wait()
    final[group] = lax.dot_general(
        flat[...], w[...], (((1,), (1,)), ((), ())), preferred_element_type=F32
    )

    def pair(j, at):
        peer = lax.rem(group + j, groups)
        return pltpu.make_async_remote_copy(
            src_ref=final.at[group],
            dst_ref=final.at[group if at else peer],
            send_sem=f_send.at[peer],
            recv_sem=f_recv.at[group if at else peer],
            device_id=(peer, me),
            device_id_type=MESH,
        )

    for j in range(1, groups):
        pair(j, True).start()
    for j in range(1, groups):
        pair(j, False).wait_recv()
    out_ref[...] = jnp.sum(final[...], axis=0).astype(BF16)
    for each in (st, o, p, s):
        drain(*each)
    lax.fori_loop(1, n // 2, lat_drain, 0)
    lat_copy(me, partner, lat_send.at[partner]).wait_send()
    for j in range(1, groups):
        pair(j, True).wait_send()


def chip_peer(chip, chips, k):
    out = 0
    bit = 1
    while bit < chips:
        own = lax.rem(chip // bit, 2)
        out = out + bit * ((1 - own) if k & bit else own)
        bit *= 2
    return out


def pair_kernel(
    n,
    groups,
    heads,
    drafts,
    q_hbm,
    qr_hbm,
    cache_hbm,
    rope_hbm,
    kq_hbm,
    ks_hbm,
    vq_hbm,
    vs_hbm,
    w_hbm,
    out_ref,
    ks_ref,
    vs_ref,
    q,
    qr,
    cache,
    rope,
    kq,
    vq,
    w,
    w_t,
    q_rows,
    qr_rows,
    cache_t,
    base,
    lat_send,
    lat_all,
    st_send,
    st_all,
    out_send,
    out_recv,
    part_send,
    part_recv,
    share_send,
    share_recv,
    fin_send,
    fin_recv,
    in_sem,
    swap_s,
    swap_r,
    lat_s,
    lat_r,
    st_s,
    st_r,
    o_s,
    o_r,
    p_s,
    p_r,
    s_s,
    s_r,
    f_s,
    f_r,
):
    me = lax.axis_index("seq")
    group = lax.axis_index("heads")
    core = lax.rem(me, 2)
    other = 1 - core
    chip = me // 2
    chips = n // 2
    half = heads // 2
    rows = half * drafts
    cols = lat_all.shape[1]
    wide = 2 * cols
    latent = cache.shape[2]
    positions = cache.shape[1]
    width = vq.shape[2]
    span = half * width
    share = rows // chips
    per = share // drafts
    factor = (q.shape[2] + qr.shape[2]) ** (-0.5)
    far_first = range(chips - 1, -1, -1)
    peers = [chip_peer(chip, chips, k) for k in range(chips)]
    partner = 2 * chip + other
    quarter = chips // 2
    near = chip // quarter

    def local(i, src, dst):
        copy = pltpu.make_async_copy(src, dst, in_sem.at[i])
        copy.start()
        return copy

    q_load = local(0, q_hbm, q)
    kq_loads = [local(1 + b, kq_hbm.at[pl.ds(b * half, half)], kq.at[pl.ds(b * half, half)]) for b in (1, 0)][::-1]

    barrier = pltpu.get_barrier_semaphore()
    for k in far_first:
        for b in range(2):
            if k:
                pl.semaphore_signal(barrier, inc=1, device_id=(group, 2 * peers[k] + b), device_id_type=MESH)
    pl.semaphore_signal(barrier, inc=1, device_id=(group, partner), device_id_type=MESH)
    for j in range(1, groups):
        for b in range(2):
            pl.semaphore_signal(
                barrier, inc=1, device_id=(lax.rem(group + j, groups), 2 * chip + b), device_id_type=MESH
            )

    ks_load = local(8, ks_hbm, ks_ref)
    qr_load = local(3, qr_hbm.at[:, pl.ds(core * half, half)], qr)
    rope_load = local(4, rope_hbm, rope.at[core])
    cache_load = local(5, cache_hbm, cache.at[core])
    vs_load = local(9, vs_hbm, vs_ref)

    def remote(src, dst, send, recv, peer_group, peer):
        return pltpu.make_async_remote_copy(
            src_ref=src,
            dst_ref=dst,
            send_sem=send,
            recv_sem=recv,
            device_id=(peer_group, peer),
            device_id_type=MESH,
        )

    lane = lax.broadcasted_iota(jnp.int32, (1, rows), 1)
    block = (me * cols) // QB

    def scale_line(scale_ref, index):
        scales = scale_ref[...]
        at = lax.broadcasted_iota(jnp.int32, scales.shape, 0) == index
        return jnp.sum(jnp.where(at, scales, 0.0), axis=0, keepdims=True)

    def scale_column(line, count, first, step):
        shape = (count, heads)
        pick = lax.broadcasted_iota(jnp.int32, shape, 1) == lax.broadcasted_iota(jnp.int32, shape, 0) // step + first
        return jnp.sum(jnp.where(pick, line, 0.0), axis=1, keepdims=True)

    ks_load.wait()
    key_column = scale_column(scale_line(ks_ref, block), heads, 0, 1)
    own_head = lax.broadcasted_iota(jnp.int32, (half, rows), 0) == lane // drafts
    key_rows = [
        jnp.sum(jnp.where(own_head, key_column[b * half : (b + 1) * half], 0.0), axis=0, keepdims=True)
        for b in range(2)
    ]

    q_load.wait()
    for b in range(2):
        for t in range(drafts):
            q_rows[b, pl.ds(t, half, stride=drafts), :] = q[t, b * half : (b + 1) * half, :].astype(F32)

    own = lax.broadcasted_iota(jnp.int32, (half, 1, rows), 0) == lane[None] // drafts
    for b in (1, 0):
        kq_loads[b].wait()
        every = lax.dot_general(
            kq[b * half : (b + 1) * half].reshape(half * cols, kq.shape[2]),
            q_rows[b].astype(BF16),
            (((1,), (1,)), ((), ())),
            preferred_element_type=F32,
        ).reshape(half, cols, rows)
        lat_send[b] = (jnp.sum(jnp.where(own, every, 0.0), axis=0) * key_rows[b]).astype(BF16)
        if b == 1:
            pl.semaphore_wait(barrier, n - 1 + 2 * (groups - 1))
        for k in far_first:
            if k:
                remote(
                    lat_send.at[b], lat_all.at[me], lat_s, lat_r.at[k // quarter], group, 2 * peers[k] + b
                ).start()
    remote(lat_send.at[other], lat_all.at[me], lat_s, lat_r.at[0], group, partner).start()
    lat_all[me] = lat_send[core]

    swaps = [
        remote(src, dst, swap_s.at[i], swap_r.at[i], group, partner)
        for i, (src, dst) in enumerate(
            (
                (rope_hbm, rope.at[core]),
                (cache_hbm, cache.at[core]),
                (vq_hbm.at[pl.ds(core * half, half)], vq.at[:, pl.ds(core * cols, cols)]),
                (w_hbm.at[:, pl.ds(core * span, span)], w.at[core]),
            )
        )
    ]
    swap_arrive = [
        remote(src, dst, swap_s.at[i], swap_r.at[i], group, partner)
        for i, (src, dst) in enumerate(
            (
                (rope_hbm, rope.at[other]),
                (cache_hbm, cache.at[other]),
                (vq_hbm.at[pl.ds(core * half, half)], vq.at[:, pl.ds(other * cols, cols)]),
                (w_hbm.at[:, pl.ds(core * span, span)], w.at[other]),
            )
        )
    ]
    for each in swaps:
        each.start()
    vq_load = local(6, vq_hbm.at[pl.ds(other * half, half)], vq.at[:, pl.ds(core * cols, cols)])
    w_load = local(7, w_hbm.at[:, pl.ds(other * span, span)], w.at[core])

    qr_load.wait()
    for t in range(drafts):
        qr_rows[pl.ds(t, half, stride=drafts), :] = qr[t].astype(F32)
    query_rope = qr_rows[...].astype(BF16)

    def prepare(j):
        turned = lax.dot_general(
            rope[j].T, query_rope, (((1,), (1,)), ((), ())), preferred_element_type=F32
        )
        position = (2 * chip + j) * positions + lax.broadcasted_iota(jnp.int32, (positions, rows), 0)
        horizon = n * positions - drafts + 1 + lax.rem(lax.broadcasted_iota(jnp.int32, (positions, rows), 1), drafts)
        base[j] = jnp.where(position < horizon, turned * factor, neg_large)
        cache_t[j] = cache[j].T

    vs_load.wait()
    value_column = scale_column(scale_line(vs_ref, block), rows, other * half, drafts)
    rope_load.wait()
    cache_load.wait()
    prepare(core)
    swap_arrive[0].wait_recv()
    swap_arrive[1].wait_recv()
    prepare(other)

    def pieces(ref, count, send, recv):
        some = ref.at[pl.ds(0, count)]
        return remote(some, some, send, recv, group, partner)

    pieces(lat_all, 2 * quarter - 1, lat_s, lat_r.at[0]).wait_recv()

    def part_scores(side):
        begin = pl.multiple_of(side * (latent // 2), latent // 2)
        query = lat_all[pl.ds(side * chips, chips)].reshape(latent // 2, rows)
        return [
            jnp.dot(cache[j, :, pl.ds(begin, latent // 2)], query, preferred_element_type=F32) * factor + base[j]
            for j in range(2)
        ]

    for j, each in enumerate(part_scores(near)):
        base[j] = each
    pieces(lat_all, 2 * quarter, lat_s, lat_r.at[1]).wait_recv()
    scores = part_scores(1 - near)
    block_max = jnp.maximum(
        jnp.max(scores[0], axis=0, keepdims=True), jnp.max(scores[1], axis=0, keepdims=True)
    )
    probs = [jnp.exp(each - block_max) for each in scores]
    st_send[0:1, :] = block_max
    st_send[1:2, :] = jnp.sum(probs[0], axis=0, keepdims=True) + jnp.sum(probs[1], axis=0, keepdims=True)

    def exchange(src_of, dst, send, recv, ks):
        for k in ks:
            remote(src_of(k), dst.at[k], send, recv(k), group, 2 * peers[k] + other).start()

    st = (lambda k: st_send, st_all, st_s, lambda k: st_r)
    exchange(*st, far_first)
    probs = [each.astype(BF16) for each in probs]
    o = (lambda k: out_send.at[peers[k]], out_recv, o_s, lambda k: o_r.at[k // quarter])
    for side, ks in ((1 - near, range(chips - 1, quarter - 1, -1)), (near, range(quarter - 1, -1, -1))):
        begin = pl.multiple_of(side * (latent // 2), latent // 2)
        block_out = sum(
            jnp.dot(cache_t[j, pl.ds(begin, latent // 2), :], probs[j], preferred_element_type=F32)
            for j in range(2)
        )
        out_send[pl.ds(side * quarter, quarter)] = block_out.astype(BF16).reshape(quarter, wide, rows)
        exchange(*o, ks)

    def turn(j):
        step = per * width
        for k in range(chips):
            w_t[j, k * step : (k + 1) * step, :] = w[j, :, k * step : (k + 1) * step].T

    w_load.wait()
    turn(core)
    vq_load.wait()
    swap_arrive[2].wait_recv()

    pieces(st_all, chips, st_s, st_r).wait_recv()
    all_max = [st_all[k, 0:1, :] for k in range(chips)]
    top = functools.reduce(jnp.maximum, all_max)
    weight = [jnp.exp(each - top) for each in all_max]
    total = sum(weight[k] * st_all[k, 1:2, :] for k in range(chips))
    merged = jnp.zeros((wide, rows), F32)
    for k in range(chips):
        if k % quarter == 0:
            pieces(out_recv, quarter, o_s, o_r.at[k // quarter]).wait_recv()
        merged = merged + out_recv[k].astype(F32) * weight[k]
    merged = (merged / total).astype(BF16).astype(F32).T
    tile = per * wide
    spread = jnp.concatenate([merged] * per, axis=1)
    keep = (
        lax.broadcasted_iota(jnp.int32, (rows, tile), 1) // wide
        == lax.rem(lax.broadcasted_iota(jnp.int32, (rows, tile), 0) // drafts, per)
    )
    spread = jnp.where(keep, spread, 0.0).astype(BF16)
    for e in range(chips):
        part = jnp.dot(
            spread[e * share : (e + 1) * share],
            vq[e * per : (e + 1) * per].reshape(tile, width),
            preferred_element_type=F32,
        )
        part_send[e] = (part * value_column[e * share : (e + 1) * share]).astype(BF16)
    p = (lambda k: part_send.at[peers[k]], part_recv, p_s, lambda k: p_r)
    exchange(*p, far_first)
    swap_arrive[3].wait_recv()
    turn(other)
    summed = jnp.zeros((share, width), F32)
    pieces(part_recv, chips, p_s, p_r).wait_recv()
    for k in range(chips):
        summed = summed + part_recv[k].astype(F32)
    for h in range(per):
        share_send[:, h * width : (h + 1) * width] = summed[h * drafts : (h + 1) * drafts].astype(BF16)
    s = (lambda k: share_send, share_recv, s_s, lambda k: s_r.at[k])
    exchange(*s, far_first)

    model = w.shape[1]
    final = [jnp.zeros((drafts, model), F32) for j in range(2)]
    for k in range(chips):
        pieces(share_recv, 1, s_s, s_r.at[k]).wait_recv()
        begin = pl.multiple_of(peers[k] * (per * width), per * width)
        for j in range(2):
            final[j] = final[j] + jnp.dot(
                share_recv[k], w_t[j, pl.ds(begin, per * width), :], preferred_element_type=F32
            )
    for j in range(2):
        fin_send[j] = final[j]

    def last(i, j, b):
        peer_group = lax.rem(group + j, groups)
        side = core if b == 0 else other
        return remote(fin_send.at[side], fin_recv.at[i], f_s, f_r, peer_group, 2 * chip + side)

    lasts = [last(i, j, b) for i, (j, b) in enumerate((j, b) for j in range(groups) for b in range(2) if j or b)]
    for each in lasts[::-1]:
        each.start()
    result = fin_send[core]
    pieces(fin_recv, len(lasts), f_s, f_r).wait_recv()
    for i in range(len(lasts)):
        result = result + fin_recv[i]
    out_ref[...] = result.astype(BF16)

    pieces(lat_all, n - 1, lat_s, lat_r.at[0]).wait_send()
    for ref, send, recv in (
        (st_all, st_s, st_r),
        (out_send, o_s, o_r.at[0]),
        (part_send, p_s, p_r),
        (share_recv, s_s, s_r.at[0]),
        (fin_recv, f_s, f_r),
    ):
        pieces(ref, ref.shape[0], send, recv).wait_send()
    for each in swaps:
        each.wait_send()


def solution(mesh):
    n = mesh.shape["seq"]
    groups = mesh.shape["heads"]

    def paired(query_nope, query_rope, latent_cache, rope_keys, lengths, key_quant, key_scale, value_quant, value_scale, out_weight):
        drafts, heads, nope = query_nope.shape[1:]
        rope = query_rope.shape[-1]
        positions, latent = latent_cache.shape[1:]
        cols = key_quant.shape[1]
        width = value_quant.shape[2]
        model = out_weight.shape[1]
        chips = n // 2
        half = heads // 2
        rows = half * drafts
        share = rows // chips
        wide = 2 * cols
        hbm = pl.BlockSpec(memory_space=pltpu.HBM)
        vmem = pl.BlockSpec(memory_space=pltpu.VMEM)
        dma = pltpu.SemaphoreType.DMA
        lasts = 2 * groups - 1
        result = pl.pallas_call(
            functools.partial(pair_kernel, n, groups, heads, drafts),
            out_shape=pltpu.VMEM((drafts, model), BF16),
            in_specs=[hbm] * 9,
            out_specs=vmem,
            scratch_shapes=[
                pltpu.VMEM(key_scale.shape[::-1], F32),
                pltpu.VMEM(value_scale.shape[::-1], F32),
                pltpu.VMEM((drafts, heads, nope), BF16),
                pltpu.VMEM((drafts, half, rope), BF16),
                pltpu.VMEM((2, positions, latent), BF16),
                pltpu.VMEM((2, rope, positions), BF16),
                pltpu.VMEM((heads, cols, nope), BF16),
                pltpu.VMEM((half, wide, width), BF16),
                pltpu.VMEM((2, model, half * width), BF16),
                pltpu.VMEM((2, half * width, model), BF16),
                pltpu.VMEM((2, rows, nope), F32),
                pltpu.VMEM((rows, rope), F32),
                pltpu.VMEM((2, latent, positions), BF16),
                pltpu.VMEM((2, positions, rows), F32),
                pltpu.VMEM((2, cols, rows), BF16),
                pltpu.VMEM((n, cols, rows), BF16),
                pltpu.VMEM((2, rows), F32),
                pltpu.VMEM((chips, 2, rows), F32),
                pltpu.VMEM((chips, wide, rows), BF16),
                pltpu.VMEM((chips, wide, rows), BF16),
                pltpu.VMEM((chips, share, width), BF16),
                pltpu.VMEM((chips, share, width), BF16),
                pltpu.VMEM((drafts, share // drafts * width), BF16),
                pltpu.VMEM((chips, drafts, share // drafts * width), BF16),
                pltpu.VMEM((2, drafts, model), F32),
                pltpu.VMEM((lasts, drafts, model), F32),
                dma((10,)),
                dma((4,)),
                dma((4,)),
                dma,
                dma((2,)),
                dma,
                dma,
                dma,
                dma((2,)),
                dma,
                dma,
                dma,
                dma((chips,)),
                dma,
                dma,
            ],
            compiler_params=pltpu.CompilerParams(
                collective_id=0, has_side_effects=True, vmem_limit_bytes=VMEM_LIMIT
            ),
        )(
            query_nope.reshape(drafts, heads, nope),
            query_rope.reshape(drafts, heads, rope),
            latent_cache.reshape(positions, latent),
            rope_keys.reshape(rope, positions),
            key_quant,
            key_scale.T,
            value_quant,
            value_scale.T,
            out_weight.T,
        )
        return result.reshape(1, drafts, model)

    def per_device(*args):
        drafts, heads = args[0].shape[1:3]
        chips = n // 2
        rows = heads // 2 * drafts
        paired_fits = (
            args[0].shape[0] == 1
            and n % 2 == 0
            and chips & (chips - 1) == 0
            and chips >= 2
            and heads % (2 * chips) == 0
            and rows % 128 == 0
            and args[5].shape[1] % 16 == 0
            and QB % (2 * args[5].shape[1]) == 0
        )
        return (paired if paired_fits else spread_out)(*args)

    def spread_out(
        query_nope,
        query_rope,
        latent_cache,
        rope_keys,
        lengths,
        key_quant,
        key_scale,
        value_quant,
        value_scale,
        out_weight,
    ):
        batch, drafts, heads, nope = query_nope.shape
        rows = batch * drafts * heads
        rope = query_rope.shape[-1]
        positions, latent = latent_cache.shape[1:]
        cols = key_quant.shape[1]
        width = value_quant.shape[2]
        model = out_weight.shape[1]
        hbm = pl.BlockSpec(memory_space=pltpu.HBM)
        vmem = pl.BlockSpec(memory_space=pltpu.VMEM)
        smem = pl.BlockSpec(memory_space=pltpu.SMEM)
        dma = pltpu.SemaphoreType.DMA
        result = pl.pallas_call(
            functools.partial(kernel, n, groups, heads, drafts),
            out_shape=jax.ShapeDtypeStruct((drafts, model), BF16),
            in_specs=[hbm, hbm, hbm, hbm, smem, hbm, vmem, hbm, vmem, hbm],
            out_specs=vmem,
            scratch_shapes=[
                pltpu.VMEM((rows, nope), BF16),
                pltpu.VMEM((rows, rope), BF16),
                pltpu.VMEM((positions, latent), BF16),
                pltpu.VMEM((rope, positions), BF16),
                pltpu.VMEM((heads * cols, nope), BF16),
                pltpu.VMEM((heads * cols, width), BF16),
                pltpu.VMEM(out_weight.shape[::-1], BF16),
                pltpu.VMEM((latent, positions), BF16),
                pltpu.VMEM((width, heads * cols), BF16),
                pltpu.VMEM((positions, rows), F32),
                pltpu.VMEM((n, cols, rows), BF16),
                pltpu.VMEM((n, 2, rows), F32),
                pltpu.VMEM((n, cols, rows), BF16),
                pltpu.VMEM((n, cols, rows), BF16),
                pltpu.VMEM((n, width // n, rows), BF16),
                pltpu.VMEM((n, width // n, rows), BF16),
                pltpu.VMEM((n, width // n, rows), BF16),
                pltpu.VMEM((drafts, heads * width), BF16),
                pltpu.VMEM((drafts, heads, width), F32),
                pltpu.VMEM((groups, drafts, model), F32),
                dma((7,)),
            ]
            + [dma((n,))] * 11
            + [dma((groups,))] * 2,
            compiler_params=pltpu.CompilerParams(
                collective_id=0, has_side_effects=True, vmem_limit_bytes=63 * 1024 * 1024
            ),
        )(
            query_nope.reshape(rows, nope),
            query_rope.reshape(rows, rope),
            latent_cache.reshape(positions, latent),
            rope_keys.reshape(rope, positions),
            lengths,
            key_quant.reshape(heads * cols, nope),
            key_scale.T,
            value_quant.reshape(heads * cols, width),
            value_scale.T,
            out_weight.T,
        )
        return result.reshape(batch, drafts, model)

    in_specs = (
        P(None, None, "heads", None),
        P(None, None, "heads", None),
        P(None, "seq", None),
        P(None, None, "seq"),
        P(),
        P("heads", "seq", None),
        P("heads", None),
        P("heads", "seq", None),
        P("heads", None),
        P("heads", "seq"),
    )
    return jax.shard_map(
        per_device, mesh=mesh, in_specs=in_specs, out_specs=P(None, None, "seq"), check_vma=False
    )
```

```python
import functools

import jax
import jax.numpy as jnp
from jax import lax
from jax.experimental import pallas as pl
from jax.experimental.pallas import tpu as pltpu
from jax.sharding import PartitionSpec as P

QB = 128
VMEM_LIMIT = 67043328 - 32768
MESH = pl.DeviceIdType.MESH
neg_large = -1e30
F32 = jnp.float32
BF16 = jnp.bfloat16


def scale_row(scale_ref, block, rows, heads):
    scales = scale_ref[...]
    line = jnp.sum(
        jnp.where(lax.broadcasted_iota(jnp.int32, scales.shape, 0) == block, scales, 0.0),
        axis=0,
        keepdims=True,
    )
    square = (heads, heads)
    diagonal = lax.broadcasted_iota(jnp.int32, square, 0) == lax.broadcasted_iota(jnp.int32, square, 1)
    column = jnp.sum(jnp.where(diagonal, line, 0.0), axis=1, keepdims=True)
    lane_head = lax.broadcasted_iota(jnp.int32, (heads, rows), 1) % heads
    own_head = lax.broadcasted_iota(jnp.int32, (heads, rows), 0)
    return jnp.sum(jnp.where(lane_head == own_head, column, 0.0), axis=0, keepdims=True)


def kernel(
    n,
    groups,
    heads,
    drafts,
    q_hbm,
    qr_hbm,
    cache_hbm,
    rope_hbm,
    len_ref,
    kq_hbm,
    ks_ref,
    vq_hbm,
    vs_ref,
    w_hbm,
    out_ref,
    q,
    qr,
    cache,
    rope,
    kq,
    vq,
    w,
    cache_t,
    vq_t,
    base,
    lat_all,
    stats,
    out_send,
    out_recv,
    part_send,
    part_recv,
    share_all,
    flat,
    heads_out,
    final,
    in_sem,
    lat_send,
    lat_recv,
    pass_send,
    st_send,
    st_recv,
    o_send,
    o_recv,
    p_send,
    p_recv,
    s_send,
    s_recv,
    f_send,
    f_recv,
):
    me = lax.axis_index("seq")
    group = lax.axis_index("heads")
    rows = q.shape[0]
    cols = lat_all.shape[1]
    width = vq.shape[1]
    positions = cache.shape[0]
    factor = (q.shape[1] + qr.shape[1]) ** (-0.5)

    loads = []
    for i, (src, dst) in enumerate(
        ((kq_hbm, kq), (q_hbm, q), (qr_hbm, qr), (rope_hbm, rope), (cache_hbm, cache), (vq_hbm, vq), (w_hbm, w))
    ):
        copy = pltpu.make_async_copy(src, dst, in_sem.at[i])
        if dst is not w:
            copy.start()
        loads.append(copy)
    kq_load, q_load, qr_load, rope_load, cache_load, vq_load, w_load = loads

    barrier = pltpu.get_barrier_semaphore()

    def greet_seq(j, c):
        pl.semaphore_signal(barrier, inc=1, device_id=(group, lax.rem(me + j, n)), device_id_type=MESH)
        return c

    def greet_heads(j, c):
        pl.semaphore_signal(barrier, inc=1, device_id=(lax.rem(group + j, groups), me), device_id_type=MESH)
        return c

    lax.fori_loop(1, n, greet_seq, 0)
    lax.fori_loop(1, groups, greet_heads, 0)

    def spread(src_of, dst, send, recv):
        def make(j):
            peer = lax.rem(me + j, n)
            return pltpu.make_async_remote_copy(
                src_ref=src_of(peer),
                dst_ref=dst.at[me],
                send_sem=send.at[peer],
                recv_sem=recv.at[me],
                device_id=(group, peer),
                device_id_type=MESH,
            )

        def go(j, c):
            make(j).start()
            return c

        lax.fori_loop(1, n, go, 0)

    def arrive(src_of, dst, send, recv):
        def wait(j, c):
            peer = lax.rem(me + j, n)
            pltpu.make_async_remote_copy(
                src_ref=src_of(peer),
                dst_ref=dst.at[peer],
                send_sem=send.at[peer],
                recv_sem=recv.at[peer],
                device_id=(group, peer),
                device_id_type=MESH,
            ).wait_recv()
            return c

        lax.fori_loop(1, n, wait, 0)

    def drain(src_of, dst, send, recv):
        def wait(j, c):
            peer = lax.rem(me + j, n)
            pltpu.make_async_remote_copy(
                src_ref=src_of(peer),
                dst_ref=dst.at[me],
                send_sem=send.at[peer],
                recv_sem=recv.at[me],
                device_id=(group, peer),
                device_id_type=MESH,
            ).wait_send()
            return c

        lax.fori_loop(1, n, wait, 0)

    block = (me * cols) // QB
    lane_head = lax.broadcasted_iota(jnp.int32, (1, rows), 1) % heads
    key_row = scale_row(ks_ref, block, rows, heads)
    value_row = scale_row(vs_ref, block, rows, heads)

    kq_load.wait()
    q_load.wait()
    every = lax.dot_general(kq[...], q[...], (((1,), (1,)), ((), ())), preferred_element_type=F32)
    every = every.reshape(heads, cols, rows)
    own = lax.broadcasted_iota(jnp.int32, (heads, 1, rows), 0) == lane_head[None]
    piece = jnp.sum(jnp.where(own, every, 0.0), axis=0) * key_row
    lat_all[me] = piece.astype(BF16)

    pl.semaphore_wait(barrier, n - 1 + groups - 1)

    partner = me + 1 - 2 * lax.rem(me, 2)

    def lat_copy(slot, peer, send):
        return pltpu.make_async_remote_copy(
            src_ref=lat_all.at[slot],
            dst_ref=lat_all.at[slot],
            send_sem=send,
            recv_sem=lat_recv.at[slot],
            device_id=(group, peer),
            device_id_type=MESH,
        )

    def like(j):
        return lax.rem(me + 2 * j, n)

    def lat_go(j, c):
        lat_copy(me, like(j), lat_send.at[like(j)]).start()
        return c

    def lat_pass(j, c):
        lat_copy(like(j), partner, pass_send.at[like(j)]).wait_recv()
        lat_copy(like(j), partner, pass_send.at[like(j)]).start()
        return c

    def lat_rest(j, c):
        other = lax.rem(partner + 2 * j, n)
        lat_copy(other, partner, pass_send.at[other]).wait_recv()
        return c

    def lat_drain(j, c):
        lat_copy(me, like(j), lat_send.at[like(j)]).wait_send()
        lat_copy(like(j), partner, pass_send.at[like(j)]).wait_send()
        return c

    lax.fori_loop(1, n // 2, lat_go, 0)
    lat_copy(me, partner, lat_send.at[partner]).start()
    w_load.start()

    qr_load.wait()
    rope_load.wait()
    base[...] = lax.dot_general(
        rope[...].T, qr[...], (((1,), (1,)), ((), ())), preferred_element_type=F32
    )
    cache_load.wait()
    cache_t[...] = cache[...].T
    lax.fori_loop(1, n // 2, lat_pass, 0)
    position = me * positions + lax.broadcasted_iota(jnp.int32, (positions, rows), 0)
    horizon = len_ref[0] + lax.broadcasted_iota(jnp.int32, (positions, rows), 1) // heads
    visible = position < horizon

    lax.fori_loop(0, n // 2, lat_rest, 0)
    query_latent = lat_all[...].reshape(n * cols, rows)
    scores = (jnp.dot(cache[...], query_latent, preferred_element_type=F32) + base[...]) * factor
    block_max = jnp.max(jnp.where(visible, scores, neg_large), axis=0, keepdims=True)
    probs = jnp.where(visible, jnp.exp(scores - block_max), 0.0)
    block_sum = jnp.sum(probs, axis=0, keepdims=True)
    stats[me, 0:1, :] = block_max
    stats[me, 1:2, :] = block_sum
    st = (lambda peer: stats.at[me], stats, st_send, st_recv)
    spread(*st)
    block_out = jnp.dot(cache_t[...], probs.astype(BF16), preferred_element_type=F32)
    out_send[...] = block_out.astype(BF16).reshape(n, cols, rows)
    o = (lambda peer: out_send.at[peer], out_recv, o_send, o_recv)
    spread(*o)
    out_recv[me] = out_send[me]
    vq_load.wait()
    vq_t[...] = vq[...].T

    arrive(*st)
    all_max = stats[:, 0:1, :]
    top = jnp.max(all_max, axis=0, keepdims=True)
    weight = jnp.exp(all_max - top)
    total = jnp.sum(weight * stats[:, 1:2, :], axis=0)
    arrive(*o)
    merged = jnp.sum(out_recv[...].astype(F32) * weight, axis=0) / total
    latent = jnp.where(own, merged[None], 0.0).astype(BF16).reshape(heads * cols, rows)
    partial = jnp.dot(vq_t[...], latent, preferred_element_type=F32) * value_row
    step = width // n
    for d in range(n):
        part_send[d] = partial[d * step : (d + 1) * step].astype(part_send.dtype)
    p = (lambda peer: part_send.at[peer], part_recv, p_send, p_recv)
    spread(*p)
    part_recv[me] = part_send[me]
    arrive(*p)
    share_all[me] = jnp.sum(part_recv[...].astype(F32), axis=0).astype(BF16)
    s = (lambda peer: share_all.at[me], share_all, s_send, s_recv)
    spread(*s)
    arrive(*s)
    head_t = jnp.concatenate([share_all[d].astype(F32) for d in range(n)], axis=0)
    heads_out[...] = head_t.T.reshape(drafts, heads, width)
    for k in range(heads):
        flat[:, k * width : (k + 1) * width] = heads_out[:, k, :].astype(BF16)
    w_load.wait()
    final[group] = lax.dot_general(
        flat[...], w[...], (((1,), (1,)), ((), ())), preferred_element_type=F32
    )

    def pair(j, at):
        peer = lax.rem(group + j, groups)
        return pltpu.make_async_remote_copy(
            src_ref=final.at[group],
            dst_ref=final.at[group if at else peer],
            send_sem=f_send.at[peer],
            recv_sem=f_recv.at[group if at else peer],
            device_id=(peer, me),
            device_id_type=MESH,
        )

    for j in range(1, groups):
        pair(j, True).start()
    for j in range(1, groups):
        pair(j, False).wait_recv()
    out_ref[...] = jnp.sum(final[...], axis=0).astype(BF16)
    for each in (st, o, p, s):
        drain(*each)
    lax.fori_loop(1, n // 2, lat_drain, 0)
    lat_copy(me, partner, lat_send.at[partner]).wait_send()
    for j in range(1, groups):
        pair(j, True).wait_send()


def chip_peer(chip, chips, k):
    out = 0
    bit = 1
    while bit < chips:
        own = lax.rem(chip // bit, 2)
        out = out + bit * ((1 - own) if k & bit else own)
        bit *= 2
    return out


def pair_kernel(
    n,
    groups,
    heads,
    drafts,
    q_hbm,
    qr_hbm,
    cache_hbm,
    rope_hbm,
    kq_hbm,
    ks_hbm,
    vq_hbm,
    vs_hbm,
    w_hbm,
    out_ref,
    ks_ref,
    vs_ref,
    q,
    qr,
    cache,
    rope,
    kq,
    vq,
    w,
    w_t,
    q_rows,
    qr_rows,
    cache_t,
    base,
    lat_send,
    lat_all,
    st_send,
    st_all,
    out_send,
    out_recv,
    part_send,
    part_recv,
    share_send,
    share_recv,
    fin_send,
    fin_recv,
    in_sem,
    swap_s,
    swap_r,
    lat_s,
    lat_r,
    st_s,
    st_r,
    o_s,
    o_r,
    p_s,
    p_r,
    s_s,
    s_r,
    f_s,
    f_r,
):
    me = lax.axis_index("seq")
    group = lax.axis_index("heads")
    core = lax.rem(me, 2)
    other = 1 - core
    chip = me // 2
    chips = n // 2
    half = heads // 2
    rows = half * drafts
    cols = lat_all.shape[1]
    wide = 2 * cols
    latent = cache.shape[2]
    positions = cache.shape[1]
    width = vq.shape[2]
    span = half * width
    share = rows // chips
    per = share // drafts
    factor = (q.shape[2] + qr.shape[2]) ** (-0.5)
    far_first = range(chips - 1, -1, -1)
    peers = [chip_peer(chip, chips, k) for k in range(chips)]
    partner = 2 * chip + other
    quarter = chips // 2
    near = chip // quarter

    def local(i, src, dst):
        copy = pltpu.make_async_copy(src, dst, in_sem.at[i])
        copy.start()
        return copy

    q_load = local(0, q_hbm, q)
    kq_loads = [local(1 + b, kq_hbm.at[pl.ds(b * half, half)], kq.at[pl.ds(b * half, half)]) for b in (1, 0)][::-1]

    barrier = pltpu.get_barrier_semaphore()
    for k in far_first:
        for b in range(2):
            if k:
                pl.semaphore_signal(barrier, inc=1, device_id=(group, 2 * peers[k] + b), device_id_type=MESH)
    pl.semaphore_signal(barrier, inc=1, device_id=(group, partner), device_id_type=MESH)
    for j in range(1, groups):
        for b in range(2):
            pl.semaphore_signal(
                barrier, inc=1, device_id=(lax.rem(group + j, groups), 2 * chip + b), device_id_type=MESH
            )

    ks_load = local(8, ks_hbm, ks_ref)
    qr_load = local(3, qr_hbm.at[:, pl.ds(core * half, half)], qr)
    rope_load = local(4, rope_hbm, rope.at[core])
    cache_load = local(5, cache_hbm, cache.at[core])
    vs_load = local(9, vs_hbm, vs_ref)

    def remote(src, dst, send, recv, peer_group, peer):
        return pltpu.make_async_remote_copy(
            src_ref=src,
            dst_ref=dst,
            send_sem=send,
            recv_sem=recv,
            device_id=(peer_group, peer),
            device_id_type=MESH,
        )

    lane = lax.broadcasted_iota(jnp.int32, (1, rows), 1)
    block = (me * cols) // QB

    def scale_line(scale_ref, index):
        scales = scale_ref[...]
        at = lax.broadcasted_iota(jnp.int32, scales.shape, 0) == index
        return jnp.sum(jnp.where(at, scales, 0.0), axis=0, keepdims=True)

    def scale_column(line, count, first, step):
        shape = (count, heads)
        pick = lax.broadcasted_iota(jnp.int32, shape, 1) == lax.broadcasted_iota(jnp.int32, shape, 0) // step + first
        return jnp.sum(jnp.where(pick, line, 0.0), axis=1, keepdims=True)

    ks_load.wait()
    key_column = scale_column(scale_line(ks_ref, block), heads, 0, 1)
    own_head = lax.broadcasted_iota(jnp.int32, (half, rows), 0) == lane // drafts
    key_rows = [
        jnp.sum(jnp.where(own_head, key_column[b * half : (b + 1) * half], 0.0), axis=0, keepdims=True)
        for b in range(2)
    ]

    q_load.wait()
    for b in range(2):
        for t in range(drafts):
            q_rows[b, pl.ds(t, half, stride=drafts), :] = q[t, b * half : (b + 1) * half, :].astype(F32)

    own = lax.broadcasted_iota(jnp.int32, (half, 1, rows), 0) == lane[None] // drafts
    for b in (1, 0):
        kq_loads[b].wait()
        every = lax.dot_general(
            kq[b * half : (b + 1) * half].reshape(half * cols, kq.shape[2]),
            q_rows[b].astype(BF16),
            (((1,), (1,)), ((), ())),
            preferred_element_type=F32,
        ).reshape(half, cols, rows)
        lat_send[b] = (jnp.sum(jnp.where(own, every, 0.0), axis=0) * key_rows[b]).astype(BF16)
        if b == 1:
            pl.semaphore_wait(barrier, n - 1 + 2 * (groups - 1))
        for k in far_first:
            if k:
                remote(
                    lat_send.at[b], lat_all.at[me], lat_s, lat_r.at[k // quarter], group, 2 * peers[k] + b
                ).start()
    remote(lat_send.at[other], lat_all.at[me], lat_s, lat_r.at[0], group, partner).start()
    lat_all[me] = lat_send[core]

    swaps = [
        remote(src, dst, swap_s.at[i], swap_r.at[i], group, partner)
        for i, (src, dst) in enumerate(
            (
                (rope_hbm, rope.at[core]),
                (cache_hbm, cache.at[core]),
                (vq_hbm.at[pl.ds(core * half, half)], vq.at[:, pl.ds(core * cols, cols)]),
                (w_hbm.at[:, pl.ds(core * span, span)], w.at[core]),
            )
        )
    ]
    swap_arrive = [
        remote(src, dst, swap_s.at[i], swap_r.at[i], group, partner)
        for i, (src, dst) in enumerate(
            (
                (rope_hbm, rope.at[other]),
                (cache_hbm, cache.at[other]),
                (vq_hbm.at[pl.ds(core * half, half)], vq.at[:, pl.ds(other * cols, cols)]),
                (w_hbm.at[:, pl.ds(core * span, span)], w.at[other]),
            )
        )
    ]
    for each in swaps:
        each.start()
    vq_load = local(6, vq_hbm.at[pl.ds(other * half, half)], vq.at[:, pl.ds(core * cols, cols)])
    w_load = local(7, w_hbm.at[:, pl.ds(other * span, span)], w.at[core])

    qr_load.wait()
    for t in range(drafts):
        qr_rows[pl.ds(t, half, stride=drafts), :] = qr[t].astype(F32)
    query_rope = qr_rows[...].astype(BF16)

    def prepare(j):
        turned = lax.dot_general(
            rope[j].T, query_rope, (((1,), (1,)), ((), ())), preferred_element_type=F32
        )
        position = (2 * chip + j) * positions + lax.broadcasted_iota(jnp.int32, (positions, rows), 0)
        horizon = n * positions - drafts + 1 + lax.rem(lax.broadcasted_iota(jnp.int32, (positions, rows), 1), drafts)
        base[j] = jnp.where(position < horizon, turned * factor, neg_large)
        cache_t[j] = cache[j].T

    vs_load.wait()
    value_column = scale_column(scale_line(vs_ref, block), rows, other * half, drafts)
    rope_load.wait()
    cache_load.wait()
    prepare(core)
    swap_arrive[0].wait_recv()
    swap_arrive[1].wait_recv()
    prepare(other)

    def pieces(ref, count, send, recv):
        some = ref.at[pl.ds(0, count)]
        return remote(some, some, send, recv, group, partner)

    pieces(lat_all, 2 * quarter - 1, lat_s, lat_r.at[0]).wait_recv()

    def part_scores(side):
        begin = pl.multiple_of(side * (latent // 2), latent // 2)
        query = lat_all[pl.ds(side * chips, chips)].reshape(latent // 2, rows)
        return [
            jnp.dot(cache[j, :, pl.ds(begin, latent // 2)], query, preferred_element_type=F32) * factor + base[j]
            for j in range(2)
        ]

    for j, each in enumerate(part_scores(near)):
        base[j] = each
    pieces(lat_all, 2 * quarter, lat_s, lat_r.at[1]).wait_recv()
    scores = part_scores(1 - near)
    block_max = jnp.maximum(
        jnp.max(scores[0], axis=0, keepdims=True), jnp.max(scores[1], axis=0, keepdims=True)
    )
    probs = [jnp.exp(each - block_max) for each in scores]
    st_send[0:1, :] = block_max
    st_send[1:2, :] = jnp.sum(probs[0], axis=0, keepdims=True) + jnp.sum(probs[1], axis=0, keepdims=True)

    def exchange(src_of, dst, send, recv, ks):
        for k in ks:
            remote(src_of(k), dst.at[k], send, recv(k), group, 2 * peers[k] + other).start()

    st = (lambda k: st_send, st_all, st_s, lambda k: st_r)
    exchange(*st, far_first)
    probs = [each.astype(BF16) for each in probs]
    o = (lambda k: out_send.at[peers[k]], out_recv, o_s, lambda k: o_r.at[k // quarter])
    middle = quarter + quarter // 2
    for ks in (range(middle - 1, quarter - 1, -1), range(chips - 1, middle - 1, -1), range(quarter - 1, -1, -1)):
        count = len(ks)
        first = count * (peers[ks[0]] // count)
        begin = pl.multiple_of(first * wide, count * wide)
        block_out = sum(
            jnp.dot(cache_t[j, pl.ds(begin, count * wide), :], probs[j], preferred_element_type=F32)
            for j in range(2)
        )
        out_send[pl.ds(first, count)] = block_out.astype(BF16).reshape(count, wide, rows)
        exchange(*o, ks)

    def turn(j):
        step = per * width
        for k in range(chips):
            w_t[j, k * step : (k + 1) * step, :] = w[j, :, k * step : (k + 1) * step].T

    w_load.wait()
    turn(core)
    vq_load.wait()
    swap_arrive[2].wait_recv()

    pieces(st_all, chips, st_s, st_r).wait_recv()
    all_max = [st_all[k, 0:1, :] for k in range(chips)]
    top = functools.reduce(jnp.maximum, all_max)
    weight = [jnp.exp(each - top) for each in all_max]
    total = sum(weight[k] * st_all[k, 1:2, :] for k in range(chips))
    merged = jnp.zeros((wide, rows), F32)
    for k in range(chips):
        if k % quarter == 0:
            pieces(out_recv, quarter, o_s, o_r.at[k // quarter]).wait_recv()
        merged = merged + out_recv[k].astype(F32) * weight[k]
    merged = (merged / total).astype(BF16).astype(F32).T
    tile = per * wide
    spread = jnp.concatenate([merged] * per, axis=1)
    keep = (
        lax.broadcasted_iota(jnp.int32, (rows, tile), 1) // wide
        == lax.rem(lax.broadcasted_iota(jnp.int32, (rows, tile), 0) // drafts, per)
    )
    spread = jnp.where(keep, spread, 0.0).astype(BF16)
    for e in range(chips):
        part = jnp.dot(
            spread[e * share : (e + 1) * share],
            vq[e * per : (e + 1) * per].reshape(tile, width),
            preferred_element_type=F32,
        )
        part_send[e] = (part * value_column[e * share : (e + 1) * share]).astype(BF16)
    p = (lambda k: part_send.at[peers[k]], part_recv, p_s, lambda k: p_r)
    exchange(*p, far_first)
    swap_arrive[3].wait_recv()
    turn(other)
    summed = jnp.zeros((share, width), F32)
    pieces(part_recv, chips, p_s, p_r).wait_recv()
    for k in range(chips):
        summed = summed + part_recv[k].astype(F32)
    for h in range(per):
        share_send[:, h * width : (h + 1) * width] = summed[h * drafts : (h + 1) * drafts].astype(BF16)
    s = (lambda k: share_send, share_recv, s_s, lambda k: s_r.at[k])
    exchange(*s, far_first)

    model = w.shape[1]
    final = [jnp.zeros((drafts, model), F32) for j in range(2)]
    for k in range(chips):
        pieces(share_recv, 1, s_s, s_r.at[k]).wait_recv()
        begin = pl.multiple_of(peers[k] * (per * width), per * width)
        for j in range(2):
            final[j] = final[j] + jnp.dot(
                share_recv[k], w_t[j, pl.ds(begin, per * width), :], preferred_element_type=F32
            )
    for j in range(2):
        fin_send[j] = final[j]

    def last(i, j, b):
        peer_group = lax.rem(group + j, groups)
        side = core if b == 0 else other
        return remote(fin_send.at[side], fin_recv.at[i], f_s, f_r, peer_group, 2 * chip + side)

    lasts = [last(i, j, b) for i, (j, b) in enumerate((j, b) for j in range(groups) for b in range(2) if j or b)]
    for each in lasts[::-1]:
        each.start()
    result = fin_send[core]
    pieces(fin_recv, len(lasts), f_s, f_r).wait_recv()
    for i in range(len(lasts)):
        result = result + fin_recv[i]
    out_ref[...] = result.astype(BF16)

    pieces(lat_all, n - 1, lat_s, lat_r.at[0]).wait_send()
    for ref, send, recv in (
        (st_all, st_s, st_r),
        (out_send, o_s, o_r.at[0]),
        (part_send, p_s, p_r),
        (share_recv, s_s, s_r.at[0]),
        (fin_recv, f_s, f_r),
    ):
        pieces(ref, ref.shape[0], send, recv).wait_send()
    for each in swaps:
        each.wait_send()


def solution(mesh):
    n = mesh.shape["seq"]
    groups = mesh.shape["heads"]

    def paired(query_nope, query_rope, latent_cache, rope_keys, lengths, key_quant, key_scale, value_quant, value_scale, out_weight):
        drafts, heads, nope = query_nope.shape[1:]
        rope = query_rope.shape[-1]
        positions, latent = latent_cache.shape[1:]
        cols = key_quant.shape[1]
        width = value_quant.shape[2]
        model = out_weight.shape[1]
        chips = n // 2
        half = heads // 2
        rows = half * drafts
        share = rows // chips
        wide = 2 * cols
        hbm = pl.BlockSpec(memory_space=pltpu.HBM)
        vmem = pl.BlockSpec(memory_space=pltpu.VMEM)
        dma = pltpu.SemaphoreType.DMA
        lasts = 2 * groups - 1
        result = pl.pallas_call(
            functools.partial(pair_kernel, n, groups, heads, drafts),
            out_shape=pltpu.VMEM((drafts, model), BF16),
            in_specs=[hbm] * 9,
            out_specs=vmem,
            scratch_shapes=[
                pltpu.VMEM(key_scale.shape[::-1], F32),
                pltpu.VMEM(value_scale.shape[::-1], F32),
                pltpu.VMEM((drafts, heads, nope), BF16),
                pltpu.VMEM((drafts, half, rope), BF16),
                pltpu.VMEM((2, positions, latent), BF16),
                pltpu.VMEM((2, rope, positions), BF16),
                pltpu.VMEM((heads, cols, nope), BF16),
                pltpu.VMEM((half, wide, width), BF16),
                pltpu.VMEM((2, model, half * width), BF16),
                pltpu.VMEM((2, half * width, model), BF16),
                pltpu.VMEM((2, rows, nope), F32),
                pltpu.VMEM((rows, rope), F32),
                pltpu.VMEM((2, latent, positions), BF16),
                pltpu.VMEM((2, positions, rows), F32),
                pltpu.VMEM((2, cols, rows), BF16),
                pltpu.VMEM((n, cols, rows), BF16),
                pltpu.VMEM((2, rows), F32),
                pltpu.VMEM((chips, 2, rows), F32),
                pltpu.VMEM((chips, wide, rows), BF16),
                pltpu.VMEM((chips, wide, rows), BF16),
                pltpu.VMEM((chips, share, width), BF16),
                pltpu.VMEM((chips, share, width), BF16),
                pltpu.VMEM((drafts, share // drafts * width), BF16),
                pltpu.VMEM((chips, drafts, share // drafts * width), BF16),
                pltpu.VMEM((2, drafts, model), F32),
                pltpu.VMEM((lasts, drafts, model), F32),
                dma((10,)),
                dma((4,)),
                dma((4,)),
                dma,
                dma((2,)),
                dma,
                dma,
                dma,
                dma((2,)),
                dma,
                dma,
                dma,
                dma((chips,)),
                dma,
                dma,
            ],
            compiler_params=pltpu.CompilerParams(
                collective_id=0, has_side_effects=True, vmem_limit_bytes=VMEM_LIMIT
            ),
        )(
            query_nope.reshape(drafts, heads, nope),
            query_rope.reshape(drafts, heads, rope),
            latent_cache.reshape(positions, latent),
            rope_keys.reshape(rope, positions),
            key_quant,
            key_scale.T,
            value_quant,
            value_scale.T,
            out_weight.T,
        )
        return result.reshape(1, drafts, model)

    def per_device(*args):
        drafts, heads = args[0].shape[1:3]
        chips = n // 2
        rows = heads // 2 * drafts
        paired_fits = (
            args[0].shape[0] == 1
            and n % 2 == 0
            and chips & (chips - 1) == 0
            and chips >= 4
            and heads % (2 * chips) == 0
            and rows % 128 == 0
            and args[5].shape[1] % 16 == 0
            and QB % (2 * args[5].shape[1]) == 0
        )
        return (paired if paired_fits else spread_out)(*args)

    def spread_out(
        query_nope,
        query_rope,
        latent_cache,
        rope_keys,
        lengths,
        key_quant,
        key_scale,
        value_quant,
        value_scale,
        out_weight,
    ):
        batch, drafts, heads, nope = query_nope.shape
        rows = batch * drafts * heads
        rope = query_rope.shape[-1]
        positions, latent = latent_cache.shape[1:]
        cols = key_quant.shape[1]
        width = value_quant.shape[2]
        model = out_weight.shape[1]
        hbm = pl.BlockSpec(memory_space=pltpu.HBM)
        vmem = pl.BlockSpec(memory_space=pltpu.VMEM)
        smem = pl.BlockSpec(memory_space=pltpu.SMEM)
        dma = pltpu.SemaphoreType.DMA
        result = pl.pallas_call(
            functools.partial(kernel, n, groups, heads, drafts),
            out_shape=jax.ShapeDtypeStruct((drafts, model), BF16),
            in_specs=[hbm, hbm, hbm, hbm, smem, hbm, vmem, hbm, vmem, hbm],
            out_specs=vmem,
            scratch_shapes=[
                pltpu.VMEM((rows, nope), BF16),
                pltpu.VMEM((rows, rope), BF16),
                pltpu.VMEM((positions, latent), BF16),
                pltpu.VMEM((rope, positions), BF16),
                pltpu.VMEM((heads * cols, nope), BF16),
                pltpu.VMEM((heads * cols, width), BF16),
                pltpu.VMEM(out_weight.shape[::-1], BF16),
                pltpu.VMEM((latent, positions), BF16),
                pltpu.VMEM((width, heads * cols), BF16),
                pltpu.VMEM((positions, rows), F32),
                pltpu.VMEM((n, cols, rows), BF16),
                pltpu.VMEM((n, 2, rows), F32),
                pltpu.VMEM((n, cols, rows), BF16),
                pltpu.VMEM((n, cols, rows), BF16),
                pltpu.VMEM((n, width // n, rows), BF16),
                pltpu.VMEM((n, width // n, rows), BF16),
                pltpu.VMEM((n, width // n, rows), BF16),
                pltpu.VMEM((drafts, heads * width), BF16),
                pltpu.VMEM((drafts, heads, width), F32),
                pltpu.VMEM((groups, drafts, model), F32),
                dma((7,)),
            ]
            + [dma((n,))] * 11
            + [dma((groups,))] * 2,
            compiler_params=pltpu.CompilerParams(
                collective_id=0, has_side_effects=True, vmem_limit_bytes=63 * 1024 * 1024
            ),
        )(
            query_nope.reshape(rows, nope),
            query_rope.reshape(rows, rope),
            latent_cache.reshape(positions, latent),
            rope_keys.reshape(rope, positions),
            lengths,
            key_quant.reshape(heads * cols, nope),
            key_scale.T,
            value_quant.reshape(heads * cols, width),
            value_scale.T,
            out_weight.T,
        )
        return result.reshape(batch, drafts, model)

    in_specs = (
        P(None, None, "heads", None),
        P(None, None, "heads", None),
        P(None, "seq", None),
        P(None, None, "seq"),
        P(),
        P("heads", "seq", None),
        P("heads", None),
        P("heads", "seq", None),
        P("heads", None),
        P("heads", "seq"),
    )
    return jax.shard_map(
        per_device, mesh=mesh, in_specs=in_specs, out_specs=P(None, None, "seq"), check_vma=False
    )
```

```python
import functools

import jax
import jax.numpy as jnp
from jax import lax
from jax.experimental import pallas as pl
from jax.experimental.pallas import tpu as pltpu
from jax.sharding import PartitionSpec as P

QB = 128
VMEM_LIMIT = 67043328 - 32768
MESH = pl.DeviceIdType.MESH
neg_large = -1e30
F32 = jnp.float32
BF16 = jnp.bfloat16


def scale_row(scale_ref, block, rows, heads):
    scales = scale_ref[...]
    line = jnp.sum(
        jnp.where(lax.broadcasted_iota(jnp.int32, scales.shape, 0) == block, scales, 0.0),
        axis=0,
        keepdims=True,
    )
    square = (heads, heads)
    diagonal = lax.broadcasted_iota(jnp.int32, square, 0) == lax.broadcasted_iota(jnp.int32, square, 1)
    column = jnp.sum(jnp.where(diagonal, line, 0.0), axis=1, keepdims=True)
    lane_head = lax.broadcasted_iota(jnp.int32, (heads, rows), 1) % heads
    own_head = lax.broadcasted_iota(jnp.int32, (heads, rows), 0)
    return jnp.sum(jnp.where(lane_head == own_head, column, 0.0), axis=0, keepdims=True)


def kernel(
    n,
    groups,
    heads,
    drafts,
    q_hbm,
    qr_hbm,
    cache_hbm,
    rope_hbm,
    len_ref,
    kq_hbm,
    ks_ref,
    vq_hbm,
    vs_ref,
    w_hbm,
    out_ref,
    q,
    qr,
    cache,
    rope,
    kq,
    vq,
    w,
    cache_t,
    vq_t,
    base,
    lat_all,
    stats,
    out_send,
    out_recv,
    part_send,
    part_recv,
    share_all,
    flat,
    heads_out,
    final,
    in_sem,
    lat_send,
    lat_recv,
    pass_send,
    st_send,
    st_recv,
    o_send,
    o_recv,
    p_send,
    p_recv,
    s_send,
    s_recv,
    f_send,
    f_recv,
):
    me = lax.axis_index("seq")
    group = lax.axis_index("heads")
    rows = q.shape[0]
    cols = lat_all.shape[1]
    width = vq.shape[1]
    positions = cache.shape[0]
    factor = (q.shape[1] + qr.shape[1]) ** (-0.5)

    loads = []
    for i, (src, dst) in enumerate(
        ((kq_hbm, kq), (q_hbm, q), (qr_hbm, qr), (rope_hbm, rope), (cache_hbm, cache), (vq_hbm, vq), (w_hbm, w))
    ):
        copy = pltpu.make_async_copy(src, dst, in_sem.at[i])
        if dst is not w:
            copy.start()
        loads.append(copy)
    kq_load, q_load, qr_load, rope_load, cache_load, vq_load, w_load = loads

    barrier = pltpu.get_barrier_semaphore()

    def greet_seq(j, c):
        pl.semaphore_signal(barrier, inc=1, device_id=(group, lax.rem(me + j, n)), device_id_type=MESH)
        return c

    def greet_heads(j, c):
        pl.semaphore_signal(barrier, inc=1, device_id=(lax.rem(group + j, groups), me), device_id_type=MESH)
        return c

    lax.fori_loop(1, n, greet_seq, 0)
    lax.fori_loop(1, groups, greet_heads, 0)

    def spread(src_of, dst, send, recv):
        def make(j):
            peer = lax.rem(me + j, n)
            return pltpu.make_async_remote_copy(
                src_ref=src_of(peer),
                dst_ref=dst.at[me],
                send_sem=send.at[peer],
                recv_sem=recv.at[me],
                device_id=(group, peer),
                device_id_type=MESH,
            )

        def go(j, c):
            make(j).start()
            return c

        lax.fori_loop(1, n, go, 0)

    def arrive(src_of, dst, send, recv):
        def wait(j, c):
            peer = lax.rem(me + j, n)
            pltpu.make_async_remote_copy(
                src_ref=src_of(peer),
                dst_ref=dst.at[peer],
                send_sem=send.at[peer],
                recv_sem=recv.at[peer],
                device_id=(group, peer),
                device_id_type=MESH,
            ).wait_recv()
            return c

        lax.fori_loop(1, n, wait, 0)

    def drain(src_of, dst, send, recv):
        def wait(j, c):
            peer = lax.rem(me + j, n)
            pltpu.make_async_remote_copy(
                src_ref=src_of(peer),
                dst_ref=dst.at[me],
                send_sem=send.at[peer],
                recv_sem=recv.at[me],
                device_id=(group, peer),
                device_id_type=MESH,
            ).wait_send()
            return c

        lax.fori_loop(1, n, wait, 0)

    block = (me * cols) // QB
    lane_head = lax.broadcasted_iota(jnp.int32, (1, rows), 1) % heads
    key_row = scale_row(ks_ref, block, rows, heads)
    value_row = scale_row(vs_ref, block, rows, heads)

    kq_load.wait()
    q_load.wait()
    every = lax.dot_general(kq[...], q[...], (((1,), (1,)), ((), ())), preferred_element_type=F32)
    every = every.reshape(heads, cols, rows)
    own = lax.broadcasted_iota(jnp.int32, (heads, 1, rows), 0) == lane_head[None]
    piece = jnp.sum(jnp.where(own, every, 0.0), axis=0) * key_row
    lat_all[me] = piece.astype(BF16)

    pl.semaphore_wait(barrier, n - 1 + groups - 1)

    partner = me + 1 - 2 * lax.rem(me, 2)

    def lat_copy(slot, peer, send):
        return pltpu.make_async_remote_copy(
            src_ref=lat_all.at[slot],
            dst_ref=lat_all.at[slot],
            send_sem=send,
            recv_sem=lat_recv.at[slot],
            device_id=(group, peer),
            device_id_type=MESH,
        )

    def like(j):
        return lax.rem(me + 2 * j, n)

    def lat_go(j, c):
        lat_copy(me, like(j), lat_send.at[like(j)]).start()
        return c

    def lat_pass(j, c):
        lat_copy(like(j), partner, pass_send.at[like(j)]).wait_recv()
        lat_copy(like(j), partner, pass_send.at[like(j)]).start()
        return c

    def lat_rest(j, c):
        other = lax.rem(partner + 2 * j, n)
        lat_copy(other, partner, pass_send.at[other]).wait_recv()
        return c

    def lat_drain(j, c):
        lat_copy(me, like(j), lat_send.at[like(j)]).wait_send()
        lat_copy(like(j), partner, pass_send.at[like(j)]).wait_send()
        return c

    lax.fori_loop(1, n // 2, lat_go, 0)
    lat_copy(me, partner, lat_send.at[partner]).start()
    w_load.start()

    qr_load.wait()
    rope_load.wait()
    base[...] = lax.dot_general(
        rope[...].T, qr[...], (((1,), (1,)), ((), ())), preferred_element_type=F32
    )
    cache_load.wait()
    cache_t[...] = cache[...].T
    lax.fori_loop(1, n // 2, lat_pass, 0)
    position = me * positions + lax.broadcasted_iota(jnp.int32, (positions, rows), 0)
    horizon = len_ref[0] + lax.broadcasted_iota(jnp.int32, (positions, rows), 1) // heads
    visible = position < horizon

    lax.fori_loop(0, n // 2, lat_rest, 0)
    query_latent = lat_all[...].reshape(n * cols, rows)
    scores = (jnp.dot(cache[...], query_latent, preferred_element_type=F32) + base[...]) * factor
    block_max = jnp.max(jnp.where(visible, scores, neg_large), axis=0, keepdims=True)
    probs = jnp.where(visible, jnp.exp(scores - block_max), 0.0)
    block_sum = jnp.sum(probs, axis=0, keepdims=True)
    stats[me, 0:1, :] = block_max
    stats[me, 1:2, :] = block_sum
    st = (lambda peer: stats.at[me], stats, st_send, st_recv)
    spread(*st)
    block_out = jnp.dot(cache_t[...], probs.astype(BF16), preferred_element_type=F32)
    out_send[...] = block_out.astype(BF16).reshape(n, cols, rows)
    o = (lambda peer: out_send.at[peer], out_recv, o_send, o_recv)
    spread(*o)
    out_recv[me] = out_send[me]
    vq_load.wait()
    vq_t[...] = vq[...].T

    arrive(*st)
    all_max = stats[:, 0:1, :]
    top = jnp.max(all_max, axis=0, keepdims=True)
    weight = jnp.exp(all_max - top)
    total = jnp.sum(weight * stats[:, 1:2, :], axis=0)
    arrive(*o)
    merged = jnp.sum(out_recv[...].astype(F32) * weight, axis=0) / total
    latent = jnp.where(own, merged[None], 0.0).astype(BF16).reshape(heads * cols, rows)
    partial = jnp.dot(vq_t[...], latent, preferred_element_type=F32) * value_row
    step = width // n
    for d in range(n):
        part_send[d] = partial[d * step : (d + 1) * step].astype(part_send.dtype)
    p = (lambda peer: part_send.at[peer], part_recv, p_send, p_recv)
    spread(*p)
    part_recv[me] = part_send[me]
    arrive(*p)
    share_all[me] = jnp.sum(part_recv[...].astype(F32), axis=0).astype(BF16)
    s = (lambda peer: share_all.at[me], share_all, s_send, s_recv)
    spread(*s)
    arrive(*s)
    head_t = jnp.concatenate([share_all[d].astype(F32) for d in range(n)], axis=0)
    heads_out[...] = head_t.T.reshape(drafts, heads, width)
    for k in range(heads):
        flat[:, k * width : (k + 1) * width] = heads_out[:, k, :].astype(BF16)
    w_load.wait()
    final[group] = lax.dot_general(
        flat[...], w[...], (((1,), (1,)), ((), ())), preferred_element_type=F32
    )

    def pair(j, at):
        peer = lax.rem(group + j, groups)
        return pltpu.make_async_remote_copy(
            src_ref=final.at[group],
            dst_ref=final.at[group if at else peer],
            send_sem=f_send.at[peer],
            recv_sem=f_recv.at[group if at else peer],
            device_id=(peer, me),
            device_id_type=MESH,
        )

    for j in range(1, groups):
        pair(j, True).start()
    for j in range(1, groups):
        pair(j, False).wait_recv()
    out_ref[...] = jnp.sum(final[...], axis=0).astype(BF16)
    for each in (st, o, p, s):
        drain(*each)
    lax.fori_loop(1, n // 2, lat_drain, 0)
    lat_copy(me, partner, lat_send.at[partner]).wait_send()
    for j in range(1, groups):
        pair(j, True).wait_send()


def chip_peer(chip, chips, k):
    out = 0
    bit = 1
    while bit < chips:
        own = lax.rem(chip // bit, 2)
        out = out + bit * ((1 - own) if k & bit else own)
        bit *= 2
    return out


def pair_kernel(
    n,
    groups,
    heads,
    drafts,
    q_hbm,
    qr_hbm,
    cache_hbm,
    rope_hbm,
    kq_hbm,
    ks_hbm,
    vq_hbm,
    vs_hbm,
    w_hbm,
    out_ref,
    ks_ref,
    vs_ref,
    q,
    qr,
    cache,
    rope,
    kq,
    vq,
    w,
    w_t,
    q_rows,
    qr_rows,
    cache_t,
    base,
    lat_send,
    lat_all,
    st_send,
    st_all,
    out_send,
    out_recv,
    part_send,
    part_recv,
    share_send,
    share_recv,
    fin_send,
    fin_recv,
    in_sem,
    swap_s,
    swap_r,
    lat_s,
    lat_r,
    st_s,
    st_r,
    o_s,
    o_r,
    p_s,
    p_r,
    s_s,
    s_r,
    f_s,
    f_r,
):
    me = lax.axis_index("seq")
    group = lax.axis_index("heads")
    core = lax.rem(me, 2)
    other = 1 - core
    chip = me // 2
    chips = n // 2
    half = heads // 2
    rows = half * drafts
    cols = lat_all.shape[1]
    wide = 2 * cols
    latent = cache.shape[2]
    positions = cache.shape[1]
    width = vq.shape[2]
    span = half * width
    share = rows // chips
    per = share // drafts
    factor = (q.shape[2] + qr.shape[2]) ** (-0.5)
    far_first = range(chips - 1, -1, -1)
    peers = [chip_peer(chip, chips, k) for k in range(chips)]
    partner = 2 * chip + other
    quarter = chips // 2
    near = chip // quarter

    def local(i, src, dst):
        copy = pltpu.make_async_copy(src, dst, in_sem.at[i])
        copy.start()
        return copy

    q_load = local(0, q_hbm, q)
    kq_loads = [local(1 + b, kq_hbm.at[pl.ds(b * half, half)], kq.at[pl.ds(b * half, half)]) for b in (1, 0)][::-1]

    barrier = pltpu.get_barrier_semaphore()
    for k in far_first:
        for b in range(2):
            if k:
                pl.semaphore_signal(barrier, inc=1, device_id=(group, 2 * peers[k] + b), device_id_type=MESH)
    pl.semaphore_signal(barrier, inc=1, device_id=(group, partner), device_id_type=MESH)
    for j in range(1, groups):
        for b in range(2):
            pl.semaphore_signal(
                barrier, inc=1, device_id=(lax.rem(group + j, groups), 2 * chip + b), device_id_type=MESH
            )

    ks_load = local(8, ks_hbm, ks_ref)
    qr_load = local(3, qr_hbm.at[:, pl.ds(core * half, half)], qr)
    rope_load = local(4, rope_hbm, rope.at[core])
    cache_load = local(5, cache_hbm, cache.at[core])
    vs_load = local(9, vs_hbm, vs_ref)

    def remote(src, dst, send, recv, peer_group, peer):
        return pltpu.make_async_remote_copy(
            src_ref=src,
            dst_ref=dst,
            send_sem=send,
            recv_sem=recv,
            device_id=(peer_group, peer),
            device_id_type=MESH,
        )

    lane = lax.broadcasted_iota(jnp.int32, (1, rows), 1)
    block = (me * cols) // QB

    def scale_line(scale_ref, index):
        scales = scale_ref[...]
        at = lax.broadcasted_iota(jnp.int32, scales.shape, 0) == index
        return jnp.sum(jnp.where(at, scales, 0.0), axis=0, keepdims=True)

    def scale_column(line, count, first, step):
        shape = (count, heads)
        pick = lax.broadcasted_iota(jnp.int32, shape, 1) == lax.broadcasted_iota(jnp.int32, shape, 0) // step + first
        return jnp.sum(jnp.where(pick, line, 0.0), axis=1, keepdims=True)

    ks_load.wait()
    key_column = scale_column(scale_line(ks_ref, block), heads, 0, 1)
    own_head = lax.broadcasted_iota(jnp.int32, (half, rows), 0) == lane // drafts
    key_rows = [
        jnp.sum(jnp.where(own_head, key_column[b * half : (b + 1) * half], 0.0), axis=0, keepdims=True)
        for b in range(2)
    ]

    q_load.wait()
    for b in range(2):
        for t in range(drafts):
            q_rows[b, pl.ds(t, half, stride=drafts), :] = q[t, b * half : (b + 1) * half, :].astype(F32)

    own = lax.broadcasted_iota(jnp.int32, (half, 1, rows), 0) == lane[None] // drafts
    for b in (1, 0):
        kq_loads[b].wait()
        every = lax.dot_general(
            kq[b * half : (b + 1) * half].reshape(half * cols, kq.shape[2]),
            q_rows[b].astype(BF16),
            (((1,), (1,)), ((), ())),
            preferred_element_type=F32,
        ).reshape(half, cols, rows)
        lat_send[b] = (jnp.sum(jnp.where(own, every, 0.0), axis=0) * key_rows[b]).astype(BF16)
        if b == 1:
            pl.semaphore_wait(barrier, n - 1 + 2 * (groups - 1))
        for k in far_first:
            if k:
                remote(
                    lat_send.at[b], lat_all.at[me], lat_s, lat_r.at[k // quarter], group, 2 * peers[k] + b
                ).start()
    remote(lat_send.at[other], lat_all.at[me], lat_s, lat_r.at[0], group, partner).start()
    lat_all[me] = lat_send[core]

    swaps = [
        remote(src, dst, swap_s.at[i], swap_r.at[i], group, partner)
        for i, (src, dst) in enumerate(
            (
                (rope_hbm, rope.at[core]),
                (cache_hbm, cache.at[core]),
                (vq_hbm.at[pl.ds(core * half, half)], vq.at[:, pl.ds(core * cols, cols)]),
                (w_hbm.at[:, pl.ds(core * span, span)], w.at[core]),
            )
        )
    ]
    swap_arrive = [
        remote(src, dst, swap_s.at[i], swap_r.at[i], group, partner)
        for i, (src, dst) in enumerate(
            (
                (rope_hbm, rope.at[other]),
                (cache_hbm, cache.at[other]),
                (vq_hbm.at[pl.ds(core * half, half)], vq.at[:, pl.ds(other * cols, cols)]),
                (w_hbm.at[:, pl.ds(core * span, span)], w.at[other]),
            )
        )
    ]
    for each in swaps:
        each.start()
    vq_load = local(6, vq_hbm.at[pl.ds(other * half, half)], vq.at[:, pl.ds(core * cols, cols)])
    w_load = local(7, w_hbm.at[:, pl.ds(other * span, span)], w.at[core])

    qr_load.wait()
    for t in range(drafts):
        qr_rows[pl.ds(t, half, stride=drafts), :] = qr[t].astype(F32)
    query_rope = qr_rows[...].astype(BF16)

    def prepare(j):
        turned = lax.dot_general(
            rope[j].T, query_rope, (((1,), (1,)), ((), ())), preferred_element_type=F32
        )
        position = (2 * chip + j) * positions + lax.broadcasted_iota(jnp.int32, (positions, rows), 0)
        horizon = n * positions - drafts + 1 + lax.rem(lax.broadcasted_iota(jnp.int32, (positions, rows), 1), drafts)
        base[j] = jnp.where(position < horizon, turned * factor, neg_large)
        cache_t[j] = cache[j].T

    vs_load.wait()
    value_column = scale_column(scale_line(vs_ref, block), rows, other * half, drafts)
    rope_load.wait()
    cache_load.wait()
    prepare(core)
    swap_arrive[0].wait_recv()
    swap_arrive[1].wait_recv()
    prepare(other)

    def pieces(ref, count, send, recv):
        some = ref.at[pl.ds(0, count)]
        return remote(some, some, send, recv, group, partner)

    pieces(lat_all, 2 * quarter - 1, lat_s, lat_r.at[0]).wait_recv()

    def part_scores(side):
        begin = pl.multiple_of(side * (latent // 2), latent // 2)
        query = lat_all[pl.ds(side * chips, chips)].reshape(latent // 2, rows)
        return [
            jnp.dot(cache[j, :, pl.ds(begin, latent // 2)], query, preferred_element_type=F32) * factor + base[j]
            for j in range(2)
        ]

    for j, each in enumerate(part_scores(near)):
        base[j] = each
    pieces(lat_all, 2 * quarter, lat_s, lat_r.at[1]).wait_recv()
    scores = part_scores(1 - near)
    block_max = jnp.maximum(
        jnp.max(scores[0], axis=0, keepdims=True), jnp.max(scores[1], axis=0, keepdims=True)
    )
    probs = [jnp.exp(each - block_max) for each in scores]
    st_send[0:1, :] = block_max
    st_send[1:2, :] = jnp.sum(probs[0], axis=0, keepdims=True) + jnp.sum(probs[1], axis=0, keepdims=True)

    def exchange(src_of, dst, send, recv, ks):
        for k in ks:
            remote(src_of(k), dst.at[k], send, recv(k), group, 2 * peers[k] + other).start()

    st = (lambda k: st_send, st_all, st_s, lambda k: st_r)
    probs = [each.astype(BF16) for each in probs]
    o = (lambda k: out_send.at[peers[k]], out_recv, o_s, lambda k: o_r.at[k // quarter])
    middle = quarter + quarter // 2
    for ks in (range(middle - 1, quarter - 1, -1), range(chips - 1, middle - 1, -1), range(quarter - 1, -1, -1)):
        count = len(ks)
        first = count * (peers[ks[0]] // count)
        begin = pl.multiple_of(first * wide, count * wide)
        block_out = sum(
            jnp.dot(cache_t[j, pl.ds(begin, count * wide), :], probs[j], preferred_element_type=F32)
            for j in range(2)
        )
        out_send[pl.ds(first, count)] = block_out.astype(BF16).reshape(count, wide, rows)
        exchange(*o, ks)
        if ks[-1] == quarter:
            exchange(*st, far_first)

    def turn(j):
        step = per * width
        for k in range(chips):
            w_t[j, k * step : (k + 1) * step, :] = w[j, :, k * step : (k + 1) * step].T

    w_load.wait()
    turn(core)
    vq_load.wait()
    swap_arrive[2].wait_recv()

    pieces(st_all, chips, st_s, st_r).wait_recv()
    all_max = [st_all[k, 0:1, :] for k in range(chips)]
    top = functools.reduce(jnp.maximum, all_max)
    weight = [jnp.exp(each - top) for each in all_max]
    total = sum(weight[k] * st_all[k, 1:2, :] for k in range(chips))
    merged = jnp.zeros((wide, rows), F32)
    for k in range(chips):
        if k % quarter == 0:
            pieces(out_recv, quarter, o_s, o_r.at[k // quarter]).wait_recv()
        merged = merged + out_recv[k].astype(F32) * weight[k]
    merged = (merged / total).astype(BF16).astype(F32).T
    tile = per * wide
    spread = jnp.concatenate([merged] * per, axis=1)
    keep = (
        lax.broadcasted_iota(jnp.int32, (rows, tile), 1) // wide
        == lax.rem(lax.broadcasted_iota(jnp.int32, (rows, tile), 0) // drafts, per)
    )
    spread = jnp.where(keep, spread, 0.0).astype(BF16)
    for e in range(chips):
        part = jnp.dot(
            spread[e * share : (e + 1) * share],
            vq[e * per : (e + 1) * per].reshape(tile, width),
            preferred_element_type=F32,
        )
        part_send[e] = (part * value_column[e * share : (e + 1) * share]).astype(BF16)
    p = (lambda k: part_send.at[peers[k]], part_recv, p_s, lambda k: p_r)
    exchange(*p, far_first)
    swap_arrive[3].wait_recv()
    turn(other)
    summed = jnp.zeros((share, width), F32)
    pieces(part_recv, chips, p_s, p_r).wait_recv()
    for k in range(chips):
        summed = summed + part_recv[k].astype(F32)
    for h in range(per):
        share_send[:, h * width : (h + 1) * width] = summed[h * drafts : (h + 1) * drafts].astype(BF16)
    s = (lambda k: share_send, share_recv, s_s, lambda k: s_r.at[k])
    exchange(*s, far_first)

    model = w.shape[1]
    final = [jnp.zeros((drafts, model), F32) for j in range(2)]
    for k in range(chips):
        pieces(share_recv, 1, s_s, s_r.at[k]).wait_recv()
        begin = pl.multiple_of(peers[k] * (per * width), per * width)
        for j in range(2):
            final[j] = final[j] + jnp.dot(
                share_recv[k], w_t[j, pl.ds(begin, per * width), :], preferred_element_type=F32
            )
    for j in range(2):
        fin_send[j] = final[j]

    def last(i, j, b):
        peer_group = lax.rem(group + j, groups)
        side = core if b == 0 else other
        return remote(fin_send.at[side], fin_recv.at[i], f_s, f_r, peer_group, 2 * chip + side)

    lasts = [last(i, j, b) for i, (j, b) in enumerate((j, b) for j in range(groups) for b in range(2) if j or b)]
    for each in lasts[::-1]:
        each.start()
    result = fin_send[core]
    pieces(fin_recv, len(lasts), f_s, f_r).wait_recv()
    for i in range(len(lasts)):
        result = result + fin_recv[i]
    out_ref[...] = result.astype(BF16)

    pieces(lat_all, n - 1, lat_s, lat_r.at[0]).wait_send()
    for ref, send, recv in (
        (st_all, st_s, st_r),
        (out_send, o_s, o_r.at[0]),
        (part_send, p_s, p_r),
        (share_recv, s_s, s_r.at[0]),
        (fin_recv, f_s, f_r),
    ):
        pieces(ref, ref.shape[0], send, recv).wait_send()
    for each in swaps:
        each.wait_send()


def solution(mesh):
    n = mesh.shape["seq"]
    groups = mesh.shape["heads"]

    def paired(query_nope, query_rope, latent_cache, rope_keys, lengths, key_quant, key_scale, value_quant, value_scale, out_weight):
        drafts, heads, nope = query_nope.shape[1:]
        rope = query_rope.shape[-1]
        positions, latent = latent_cache.shape[1:]
        cols = key_quant.shape[1]
        width = value_quant.shape[2]
        model = out_weight.shape[1]
        chips = n // 2
        half = heads // 2
        rows = half * drafts
        share = rows // chips
        wide = 2 * cols
        hbm = pl.BlockSpec(memory_space=pltpu.HBM)
        vmem = pl.BlockSpec(memory_space=pltpu.VMEM)
        dma = pltpu.SemaphoreType.DMA
        lasts = 2 * groups - 1
        result = pl.pallas_call(
            functools.partial(pair_kernel, n, groups, heads, drafts),
            out_shape=pltpu.VMEM((drafts, model), BF16),
            in_specs=[hbm] * 9,
            out_specs=vmem,
            scratch_shapes=[
                pltpu.VMEM(key_scale.shape[::-1], F32),
                pltpu.VMEM(value_scale.shape[::-1], F32),
                pltpu.VMEM((drafts, heads, nope), BF16),
                pltpu.VMEM((drafts, half, rope), BF16),
                pltpu.VMEM((2, positions, latent), BF16),
                pltpu.VMEM((2, rope, positions), BF16),
                pltpu.VMEM((heads, cols, nope), BF16),
                pltpu.VMEM((half, wide, width), BF16),
                pltpu.VMEM((2, model, half * width), BF16),
                pltpu.VMEM((2, half * width, model), BF16),
                pltpu.VMEM((2, rows, nope), F32),
                pltpu.VMEM((rows, rope), F32),
                pltpu.VMEM((2, latent, positions), BF16),
                pltpu.VMEM((2, positions, rows), F32),
                pltpu.VMEM((2, cols, rows), BF16),
                pltpu.VMEM((n, cols, rows), BF16),
                pltpu.VMEM((2, rows), F32),
                pltpu.VMEM((chips, 2, rows), F32),
                pltpu.VMEM((chips, wide, rows), BF16),
                pltpu.VMEM((chips, wide, rows), BF16),
                pltpu.VMEM((chips, share, width), BF16),
                pltpu.VMEM((chips, share, width), BF16),
                pltpu.VMEM((drafts, share // drafts * width), BF16),
                pltpu.VMEM((chips, drafts, share // drafts * width), BF16),
                pltpu.VMEM((2, drafts, model), F32),
                pltpu.VMEM((lasts, drafts, model), F32),
                dma((10,)),
                dma((4,)),
                dma((4,)),
                dma,
                dma((2,)),
                dma,
                dma,
                dma,
                dma((2,)),
                dma,
                dma,
                dma,
                dma((chips,)),
                dma,
                dma,
            ],
            compiler_params=pltpu.CompilerParams(
                collective_id=0, has_side_effects=True, vmem_limit_bytes=VMEM_LIMIT
            ),
        )(
            query_nope.reshape(drafts, heads, nope),
            query_rope.reshape(drafts, heads, rope),
            latent_cache.reshape(positions, latent),
            rope_keys.reshape(rope, positions),
            key_quant,
            key_scale.T,
            value_quant,
            value_scale.T,
            out_weight.T,
        )
        return result.reshape(1, drafts, model)

    def per_device(*args):
        drafts, heads = args[0].shape[1:3]
        chips = n // 2
        rows = heads // 2 * drafts
        paired_fits = (
            args[0].shape[0] == 1
            and n % 2 == 0
            and chips & (chips - 1) == 0
            and chips >= 4
            and heads % (2 * chips) == 0
            and rows % 128 == 0
            and args[5].shape[1] % 16 == 0
            and QB % (2 * args[5].shape[1]) == 0
        )
        return (paired if paired_fits else spread_out)(*args)

    def spread_out(
        query_nope,
        query_rope,
        latent_cache,
        rope_keys,
        lengths,
        key_quant,
        key_scale,
        value_quant,
        value_scale,
        out_weight,
    ):
        batch, drafts, heads, nope = query_nope.shape
        rows = batch * drafts * heads
        rope = query_rope.shape[-1]
        positions, latent = latent_cache.shape[1:]
        cols = key_quant.shape[1]
        width = value_quant.shape[2]
        model = out_weight.shape[1]
        hbm = pl.BlockSpec(memory_space=pltpu.HBM)
        vmem = pl.BlockSpec(memory_space=pltpu.VMEM)
        smem = pl.BlockSpec(memory_space=pltpu.SMEM)
        dma = pltpu.SemaphoreType.DMA
        result = pl.pallas_call(
            functools.partial(kernel, n, groups, heads, drafts),
            out_shape=jax.ShapeDtypeStruct((drafts, model), BF16),
            in_specs=[hbm, hbm, hbm, hbm, smem, hbm, vmem, hbm, vmem, hbm],
            out_specs=vmem,
            scratch_shapes=[
                pltpu.VMEM((rows, nope), BF16),
                pltpu.VMEM((rows, rope), BF16),
                pltpu.VMEM((positions, latent), BF16),
                pltpu.VMEM((rope, positions), BF16),
                pltpu.VMEM((heads * cols, nope), BF16),
                pltpu.VMEM((heads * cols, width), BF16),
                pltpu.VMEM(out_weight.shape[::-1], BF16),
                pltpu.VMEM((latent, positions), BF16),
                pltpu.VMEM((width, heads * cols), BF16),
                pltpu.VMEM((positions, rows), F32),
                pltpu.VMEM((n, cols, rows), BF16),
                pltpu.VMEM((n, 2, rows), F32),
                pltpu.VMEM((n, cols, rows), BF16),
                pltpu.VMEM((n, cols, rows), BF16),
                pltpu.VMEM((n, width // n, rows), BF16),
                pltpu.VMEM((n, width // n, rows), BF16),
                pltpu.VMEM((n, width // n, rows), BF16),
                pltpu.VMEM((drafts, heads * width), BF16),
                pltpu.VMEM((drafts, heads, width), F32),
                pltpu.VMEM((groups, drafts, model), F32),
                dma((7,)),
            ]
            + [dma((n,))] * 11
            + [dma((groups,))] * 2,
            compiler_params=pltpu.CompilerParams(
                collective_id=0, has_side_effects=True, vmem_limit_bytes=63 * 1024 * 1024
            ),
        )(
            query_nope.reshape(rows, nope),
            query_rope.reshape(rows, rope),
            latent_cache.reshape(positions, latent),
            rope_keys.reshape(rope, positions),
            lengths,
            key_quant.reshape(heads * cols, nope),
            key_scale.T,
            value_quant.reshape(heads * cols, width),
            value_scale.T,
            out_weight.T,
        )
        return result.reshape(batch, drafts, model)

    in_specs = (
        P(None, None, "heads", None),
        P(None, None, "heads", None),
        P(None, "seq", None),
        P(None, None, "seq"),
        P(),
        P("heads", "seq", None),
        P("heads", None),
        P("heads", "seq", None),
        P("heads", None),
        P("heads", "seq"),
    )
    return jax.shard_map(
        per_device, mesh=mesh, in_specs=in_specs, out_specs=P(None, None, "seq"), check_vma=False
    )
```
